128 devices in a mesh: dp: 8 (over z, core), mp: 16 (over x, y).
Axes of the slice: x: 4, y: 4, z: 4, core: 2. Of those that a mesh axis runs over, the one named last changes fastest.
Arguments:
- features: bfloat16 [8192, 2048], P('dp'), may hold values from -21 to 21
- rewards: float32 [32, 256], P('dp'), may hold values from -6 to 6
- old_values: float32 [32, 256], P('dp'), may hold values from -6 to 6
- dones: int32 [32, 256], P('dp'), may hold values 0 or 1
- lengths: int32 [32], P('dp'), may hold values from 128 to 256
- proj_weights: bfloat16 [2048, 2, 8192], P(None, None, 'mp'), may hold values from -0.125 to 0.125
- down_weight: bfloat16 [8192, 2048], P('mp'), may hold values from -0.0625 to 0.0625
- value_head: float32 [2048], replicated, may hold values from -0.0078125 to 0.0078125
- master: float32 [2048, 2, 8192], P('dp', None, 'mp'), may hold values from -0.125 to 0.125
- moment: float32 [2048, 2, 8192], P('dp', None, 'mp'), may hold values from -1.035801e-05 to 1.035801e-05
- second: float32 [2048, 2, 8192], P('dp', None, 'mp'), may hold values from 2.9802322e-13 to 2.9802322e-12
Outputs:
- master_new: float32 [2048, 2, 8192], P('dp', None, 'mp')
- moment_new: float32 [2048, 2, 8192], P('dp', None, 'mp')
- second_new: float32 [2048, 2, 8192], P('dp', None, 'mp')
- working: bfloat16 [2048, 2, 8192], P(None, None, 'mp')
- total_loss: float32 [], replicated
The draws below stay inside these ranges and needn't reach their ends.
All inputs are finite; a program needn't handle non-finite values. No bound on the sum of `dones` on one device may be relied on, other than what follows from the above.
Results may differ from the reference program's by a relative error of at most 0.0011.
Values may be sent and summed in bfloat16 or wider, within the bound.
A program may use at most 128 MiB of HBM per device.

```python
import math
import jax
import jax.numpy as jnp
from jax import lax

D = 2048
FF = 8192
SEQ_LEN = 256
TOK_DEV = 1024
SEQS = 32
TOKENS = 8192


def common_direction(key):
    return jnp.clip(jax.random.normal(jax.random.fold_in(key, 101), (D,), jnp.float32), -2.5, 2.5)


def draw_features(key, part):
    direction = common_direction(key)
    magnitude = jax.random.uniform(jax.random.fold_in(key, 102), (TOKENS,), jnp.float32, 0.5, 1.5)
    polarity = (2 * jax.random.randint(jax.random.fold_in(key, 103), (TOKENS,), 0, 2) - 1).astype(jnp.float32)
    jitter = jnp.clip(jax.random.normal(jax.random.fold_in(key, 104), (TOKENS, D), jnp.float32), -3.0, 3.0)
    values = jitter + (magnitude * polarity)[:, None] * direction[None, :]
    blocks = TOKENS // TOK_DEV
    block_width = D // blocks
    pairing = jax.random.permutation(jax.random.fold_in(key, 105), blocks)
    token_block = jnp.arange(TOKENS, dtype=jnp.int32) // TOK_DEV
    column_block = jnp.arange(D, dtype=jnp.int32) // block_width
    spiked = pairing[token_block][:, None] == column_block[None, :]
    values = jnp.where(spiked, 3.0 * values, values)
    return values.astype(jnp.bfloat16)


def draw_value_head(key, part):
    direction = common_direction(key)
    jitter = 0.5 * jnp.clip(jax.random.normal(jax.random.fold_in(key, 106), (D,), jnp.float32), -3.0, 3.0)
    return (4.0 / D * (direction + jitter)).astype(jnp.float32)


def set_ends(drawn, own_key, smallest, largest):
    dims = drawn.shape
    spot = [jax.random.randint(jax.random.fold_in(own_key, axis), (), 0, dims[axis]) for axis in range(len(dims))]
    drawn = drawn.at[tuple(spot)].set(smallest)
    longest = dims.index(max(dims))
    spot[longest] = (spot[longest] + 1) % dims[longest]
    return drawn.at[tuple(spot)].set(largest)


def level_of(stream_key, shape, shards, smallest, largest):
    loudness, own = 1.0, jax.random.fold_in(stream_key, 6)
    for axis_at, parts in shards:
        steps = jnp.exp(jax.random.uniform(jax.random.fold_in(own, axis_at), (parts,), jnp.float32, smallest / len(shards), largest / len(shards)))
        loudness = loudness * jnp.repeat(steps, shape[axis_at] // parts).reshape([-1 if axis == axis_at else 1 for axis in range(len(shape))])
    return loudness


def scatter_about(stream_key, extent, deviation, limit, split=(), kind=jnp.bfloat16):
    drawn = jax.random.normal(stream_key, extent, jnp.float32) * deviation
    if len(split) > 0:
        drawn = level_of(stream_key, extent, split, -0.22, 0.18) * drawn
    return jnp.clip(drawn, min=-limit, max=limit).astype(kind)


def setup_inputs(seed: int = 0) -> dict:
    key_list = jax.random.split(jax.random.key(seed), 12)
    return {
        "features": draw_features(jax.random.fold_in(key_list[11], 71), 0),
        "rewards": scatter_about(key_list[1], (SEQS, SEQ_LEN), 1.0, 6.0, ((0, 8),), jnp.float32),
        "old_values": scatter_about(key_list[2], (SEQS, SEQ_LEN), 1.0, 6.0, ((0, 8),), jnp.float32),
        "dones": set_ends((jax.random.randint(key_list[3], (SEQS, SEQ_LEN), 0, 32) < 1).astype(jnp.int32), jax.random.fold_in(key_list[3], 1), 0, 1),
        "lengths": set_ends(jax.random.randint(key_list[4], (SEQS,), SEQ_LEN // 2, SEQ_LEN + 1), jax.random.fold_in(key_list[4], 1), SEQ_LEN // 2, SEQ_LEN).astype(jnp.int32),
        "proj_weights": scatter_about(key_list[5], (D, 2, FF), D ** -0.5, 0.125, ((2, 16),)),
        "down_weight": scatter_about(key_list[6], (FF, D), FF ** -0.5, 0.0625, ((0, 16),)),
        "value_head": draw_value_head(jax.random.fold_in(key_list[11], 71), 0),
        "master": scatter_about(key_list[8], (D, 2, FF), D ** -0.5, 0.125, ((0, 8), (2, 16)), jnp.float32),
        "moment": scatter_about(key_list[9], (D, 2, FF), (0.01 / (2 * D * FF) ** 0.5), 1.035800960380584e-05, ((0, 8), (2, 16)), jnp.float32),
        "second": jnp.clip(jnp.exp(math.log(2.9802321634825324e-12) - 2.3025851 * jax.random.uniform(key_list[10], (D, 2, FF), jnp.float32) ** level_of(key_list[10], (D, 2, FF), ((0, 8), (2, 16)), -0.2, 0.2)), 2.9802321634825324e-13, 2.9802321634825324e-12),
    }


GAMMA = 0.99
LAMBDA = 0.95
MAX_NORM = 0.05

def gae_targets(rewards, old_values, dones, lengths):
    seq_len = rewards.shape[1]
    keeps = 1.0 - dones.astype(jnp.float32)
    following = jnp.concatenate([old_values[:, 1:], jnp.zeros_like(old_values[:, :1])], axis=1)
    deltas = rewards + GAMMA * following * keeps - old_values
    counted = jnp.cumsum(dones, axis=1).astype(jnp.int32) - dones
    places = jnp.arange(seq_len, dtype=jnp.int32)
    spans = places[None, :] - places[:, None]
    linked = (counted[:, :, None] == counted[:, None, :]) & (spans[None] >= 0)
    powers = jnp.exp(jnp.maximum(spans, 0).astype(jnp.float32) * math.log(GAMMA * LAMBDA))
    kernel = jnp.where(linked, powers[None], jnp.zeros((), jnp.float32))
    advantage = jnp.einsum('ats,as->at', kernel, deltas, precision=lax.Precision.HIGHEST)
    targets = (advantage + old_values).reshape(-1)
    mask = (places[None, :] < lengths[:, None]).astype(jnp.float32).reshape(-1)
    return (targets, mask)

def reference(features, rewards, old_values, dones, lengths, proj_weights, down_weight, value_head, master, moment, second):
    targets, mask = gae_targets(rewards, old_values, dones, lengths)
    both = jnp.dot(features, proj_weights.reshape(D, 2 * FF), preferred_element_type=jnp.float32).reshape(-1, 2, FF)
    gate_values = both[:, 0, :]
    up_values = both[:, 1, :]
    hidden = (jax.nn.silu(gate_values) * up_values).astype(jnp.bfloat16)
    stream = features.astype(jnp.float32) + jnp.dot(hidden, down_weight, preferred_element_type=jnp.float32)
    norm_factor = lax.rsqrt(lax.optimization_barrier(jnp.mean(stream * stream, axis=-1)) + 1e-05)
    normed = stream * norm_factor[:, None]
    estimate = jnp.dot(normed, value_head, precision=lax.Precision.HIGHEST)
    errors = estimate - targets
    total_loss = jnp.sum(mask * errors * errors) / TOKENS
    coeff = 2.0 * mask * errors / TOKENS
    head_grad = coeff[:, None] * value_head[None, :]
    out_grad = (norm_factor[:, None] * (head_grad - normed * lax.optimization_barrier(jnp.mean(head_grad * normed, axis=-1, keepdims=True)))).astype(jnp.bfloat16)
    hidden_grad = jnp.dot(out_grad, down_weight.T, preferred_element_type=jnp.float32)
    gate_sigmoid = jax.nn.sigmoid(gate_values)
    gate_grad = (hidden_grad * up_values * gate_sigmoid * (1.0 + gate_values * (1.0 - gate_sigmoid))).astype(jnp.bfloat16)
    up_grad = (hidden_grad * gate_values * gate_sigmoid).astype(jnp.bfloat16)
    grads = jnp.stack([jnp.dot(features.T, gate_grad, preferred_element_type=jnp.float32), jnp.dot(features.T, up_grad, preferred_element_type=jnp.float32)], axis=1)
    grad_norm = jnp.sqrt(jnp.sum(grads * grads))
    clip = jnp.minimum(1.0, MAX_NORM / (grad_norm + 1e-06))
    clipped = clip * grads
    moment_new = 0.9 * moment + 0.1 * clipped
    second_new = 0.999 * second + 0.001 * clipped * clipped
    first_hat = moment_new / (1.0 - 0.9 ** 10)
    second_hat = second_new / (1.0 - 0.999 ** 10)
    master_new = master - 0.001 * (first_hat / (jnp.sqrt(second_hat) + 1e-08) + 0.1 * master)
    working = master_new.astype(jnp.bfloat16)
    return (master_new, moment_new, second_new, working, total_loss)
```

```python
import math

import jax
import jax.numpy as jnp
from jax import lax
from jax.experimental import pallas as pl
from jax.experimental.pallas import tpu as pltpu
from jax.sharding import Mesh
from jax.sharding import PartitionSpec as P

Z, CORE, X, Y = "dp_0", "dp_1", "mp_0", "mp_1"
DP = (Z, CORE)
MP = (X, Y)
GAMMA = 0.99
LAMBDA = 0.95
MAX_NORM = 0.05
D = 2048
TOK = 1024
FFL = 512
ROWS = 256
BF = jnp.bfloat16
LEVELS = 32000.0
F32 = jnp.float32
VMEM_LIMIT = 62 * 1024 * 1024


def mul_of(v, n):
    return pl.multiple_of(v, n)


def ring(v, d):
    return lax.rem(v + (d + 4), 4)


def remote(src, dst, send, recv, device):
    return pltpu.make_async_remote_copy(
        src_ref=src, dst_ref=dst, send_sem=send, recv_sem=recv,
        device_id=device, device_id_type=pl.DeviceIdType.MESH,
    )


def greet(devices):
    barrier = pltpu.get_barrier_semaphore()
    for device in devices:
        pl.semaphore_signal(barrier, inc=1, device_id=device, device_id_type=pl.DeviceIdType.MESH)
    pl.semaphore_wait(barrier, len(devices))


def own_targets(x, y, rew, old, dones, lengths):
    dn = jnp.broadcast_to(dones[pl.ds(y, 1), :].astype(F32), (8, 256))
    ov = jnp.broadcast_to(old[pl.ds(y, 1), :], (8, 256))
    rw = jnp.broadcast_to(rew[pl.ds(y, 1), :], (8, 256))
    lane = lax.broadcasted_iota(jnp.int32, (8, 256), 1)
    following = jnp.where(lane == 255, 0.0, pltpu.roll(ov, 255, axis=1))
    deltas = (rw + GAMMA * following * (1.0 - dn) - ov)[0:1]
    before = lax.broadcasted_iota(jnp.int32, (256, 256), 0) < lax.broadcasted_iota(jnp.int32, (256, 256), 1)
    counted_s = jnp.dot(dn.astype(BF), before.astype(F32).astype(BF), preferred_element_type=F32)[0:1]
    t = x * 64 + lax.broadcasted_iota(jnp.int32, (64, 256), 0)
    s = lax.broadcasted_iota(jnp.int32, (64, 256), 1)
    counted_t = jnp.sum(jnp.where(s < t, dn[0:1], 0.0), axis=1, keepdims=True)
    linked = (counted_t == counted_s) & (s >= t)
    powers = jnp.exp(jnp.maximum(s - t, 0).astype(F32) * math.log(GAMMA * LAMBDA))
    advantage = jnp.sum(jnp.where(linked, powers, 0.0) * deltas, axis=1, keepdims=True)
    own_old = jnp.sum(jnp.where(s == t, ov[0:1], 0.0), axis=1, keepdims=True)
    mask = jnp.where(t[:, 0:1] < lengths[y], 1.0, 0.0)
    return advantage + own_old, mask


STREAMS = ((True, 1), (True, -1), (False, 1), (False, -1))


def forward_kernel(feat, w4, down, head, rew, old, dones, lengths, bg, loss,
                   both, hid, part, rv1, rv2, og, mix,
                   s1, r1, s2, r2, gs1, gr1, gs2, gr2):
    x, y = lax.axis_index(X), lax.axis_index(Y)
    greet([{X: ring(x, 1)}, {X: ring(x, -1)}, {Y: ring(y, 1)}, {Y: ring(y, -1)}])

    def peer(first, h, delta):
        along_x = STREAMS[h][0] == first
        return {X: ring(x, delta)} if along_x else {Y: ring(y, delta)}

    def tok(h, da, db):
        dx, dy = (da, db) if STREAMS[h][0] else (db, da)
        return pl.ds(mul_of(ring(y, dy) * 256 + ring(x, dx) * 64, 64), 64)

    def offsets(h):
        s = STREAMS[h][1]
        return (2, s, -s, 0)

    one = {}
    two = {}
    for h in range(4):
        s = STREAMS[h][1]
        for j, db in enumerate(offsets(h)):
            for kind, (da, to) in enumerate(((2, s), (s, s), (-s, -s))):
                one[h, kind, j] = remote(part.at[h, tok(h, da, db)], rv1.at[h, kind, j],
                                         s1.at[h, kind, j], r1.at[h, kind, j], peer(True, h, to))
        for kind, (db, to) in enumerate(((2, s), (s, s), (-s, -s))):
            two[h, kind] = remote(part.at[h, tok(h, 0, db)], rv2.at[h, kind],
                                  s2.at[h, kind], r2.at[h, kind], peer(False, h, to))

    def chunk(dy):
        rows = pl.ds(mul_of(ring(y, dy) * 256, 256), 256)
        f = feat[rows, :]
        for c in range(4):
            gu = jnp.dot(f, w4[c], preferred_element_type=F32)
            both[c, rows, :] = gu
            gate, up = gu[:, :128], gu[:, 128:]
            hid[rows, c * 128:(c + 1) * 128] = (gate * jax.nn.sigmoid(gate) * up).astype(BF)
        v = hid[rows, :]
        for h in range(4):
            part[h, rows, :] = jnp.dot(
                v, down[:, h * 512:(h + 1) * 512], preferred_element_type=F32).astype(BF)

    def index(h, db):
        return offsets(h).index(db)

    def send_raw(dy):
        for h in (0, 1):
            one[h, 0, index(h, dy)].start()
            one[h, 2, index(h, dy)].start()
        for h in (2, 3):
            s = STREAMS[h][1]
            if dy == 2:
                for j in range(4):
                    one[h, 0, j].start()
            elif dy == -s:
                for j in range(4):
                    one[h, 2, j].start()

    def pass_on(h, j):
        s = STREAMS[h][1]
        one[h, 0, j].wait_recv()
        t = tok(h, s, offsets(h)[j])
        part[h, t, :] = (part[h, t, :].astype(F32) + rv1[h, 0, j].astype(F32)).astype(BF)
        one[h, 1, j].start()

    def finish(h, j):
        one[h, 1, j].wait_recv()
        one[h, 2, j].wait_recv()
        t = tok(h, 0, offsets(h)[j])
        total = part[h, t, :].astype(F32) + rv1[h, 1, j].astype(F32) + rv1[h, 2, j].astype(F32)
        if j == 3:
            two[h, 1].wait_recv()
            two[h, 2].wait_recv()
            mix[:, h * 512:(h + 1) * 512] = total + rv2[h, 1].astype(F32) + rv2[h, 2].astype(F32)
            return
        if j == 1:
            two[h, 0].wait_recv()
            total = total + rv2[h, 0].astype(F32)
        part[h, t, :] = total.astype(BF)
        two[h, j].start()

    chunk(2)
    send_raw(2)
    chunk(1)
    send_raw(1)
    for h in (0, 1):
        pass_on(h, index(h, 2))
    for j in range(4):
        pass_on(2, j)
    chunk(-1)
    send_raw(-1)
    for h in (0, 1):
        pass_on(h, index(h, 1))
    for j in range(4):
        pass_on(3, j)
    chunk(0)
    send_raw(0)
    for h in (0, 1):
        pass_on(h, index(h, -1))
    targets, mask = own_targets(x, y, rew, old, dones, lengths)
    for h in range(4):
        finish(h, 0)
    for h in (0, 1):
        pass_on(h, index(h, 0))
    for j in (1, 2, 3):
        for h in range(4):
            finish(h, j)

    mine = pl.ds(mul_of(y * 256 + x * 64, 64), 64)
    stream = feat[mine, :].astype(F32) + mix[...]
    vh = head[...]
    norm = lax.rsqrt(jnp.sum(stream * stream, axis=1, keepdims=True) / D + 1e-05)
    estimate = norm * jnp.sum(stream * vh, axis=1, keepdims=True)
    errors = estimate - targets
    total_tokens = TOK * 8
    loss[...] = jnp.broadcast_to(jnp.sum(mask * errors * errors, axis=0, keepdims=True) / total_tokens, (8, 128))
    coeff = 2.0 * mask * errors / total_tokens
    inner = coeff * estimate / D
    a = norm * coeff
    b = norm * norm * inner
    for h in range(4):
        cols = slice(h * 512, (h + 1) * 512)
        st = feat[mine, cols].astype(F32) + mix[:, cols]
        og[h, mine, :] = (a * vh[:, cols] - b * st).astype(BF)

    g1 = {}
    g2 = {}
    for h in range(4):
        s = STREAMS[h][1]
        for kind, (db, to) in enumerate(((0, 1), (0, -1), (-s, s))):
            t = og.at[h, tok(h, 0, db)]
            g1[h, kind] = remote(t, t, gs1.at[h, kind], gr1.at[h, kind], peer(False, h, to))
        for k, db in enumerate((0, -s, s, 2)):
            for kind, (da, to) in enumerate(((0, 1), (0, -1), (-s, s))):
                t = og.at[h, tok(h, da, db)]
                g2[h, k, kind] = remote(t, t, gs2.at[h, k, kind], gr2.at[h, k, kind], peer(True, h, to))

    waited = set()

    def arrive(table, key):
        if (id(table), key) not in waited:
            waited.add((id(table), key))
            table[key].wait_recv()

    def spread(h, k):
        g2[h, k, 0].start()
        g2[h, k, 1].start()

    def relay(h, k):
        kind = 0 if STREAMS[h][1] == 1 else 1
        arrive(g2, (h, k, kind))
        g2[h, k, 2].start()

    def backward(dy):
        rows = pl.ds(mul_of(ring(y, dy) * 256, 256), 256)
        hg = None
        for h in range(4):
            term = lax.dot_general(og[h, rows, :], down[:, h * 512:(h + 1) * 512],
                                   (((1,), (1,)), ((), ())), preferred_element_type=F32)
            hg = term if hg is None else hg + term
        for c in range(4):
            gate, up = both[c, rows, :128], both[c, rows, 128:]
            d = hg[:, c * 128:(c + 1) * 128]
            sig = jax.nn.sigmoid(gate)
            bg[rows, c * 256:c * 256 + 128] = (d * up * sig * (1.0 + gate * (1.0 - sig))).astype(BF)
            bg[rows, c * 256 + 128:(c + 1) * 256] = (d * gate * sig).astype(BF)

    for h in range(4):
        g1[h, 0].start()
        g1[h, 1].start()
    for h in range(4):
        spread(h, 0)
    for h in range(4):
        with_relay, against = (0, 1) if STREAMS[h][1] == 1 else (1, 0)
        arrive(g1, (h, with_relay))
        g1[h, 2].start()
    for h in range(4):
        spread(h, 1)
    for h in range(4):
        relay(h, 0)
        arrive(g1, (h, 1 if STREAMS[h][1] == 1 else 0))
        spread(h, 2)
    for h in range(4):
        arrive(g1, (h, 2))
        spread(h, 3)
    for h in range(4):
        relay(h, 1)
    for h in (0, 1):
        for kind in range(3):
            arrive(g2, (h, 0, kind))
    backward(0)
    for h in range(4):
        relay(h, 2)
    for dy in (-1, 1):
        for h in (0, 1):
            k = (0, -STREAMS[h][1], STREAMS[h][1], 2).index(dy)
            for kind in range(3):
                arrive(g2, (h, k, kind))
        for h in (2, 3):
            for k in range(4):
                arrive(g2, (h, k, 0 if dy == -1 else 1))
        if dy == -1:
            for h in range(4):
                relay(h, 3)
        backward(dy)
    for h in range(4):
        for k in range(4):
            for kind in range(3):
                arrive(g2, (h, k, kind))
    backward(2)

    for table in (one, two, g1, g2):
        for key in table:
            table[key].wait_send()


def update_kernel(feat, bg, loss_in, master, moment, second, work, master_new, moment_new, second_new, loss,
                  gsend, gown, grecv, qs, qr, gv, wk, mo, vo, so, n1, n2,
                  ds, dr, zs, zr, ns, nr, ms, mr, ws, wr, cs, cr, ls):
    z, core, x, y = (lax.axis_index(a) for a in (Z, CORE, X, Y))
    other = 1 - core
    me = z * 2 + core
    plane = x * 4 + y
    dp_peers = [{Z: ring(z, i // 2), CORE: lax.rem(core + i % 2, 2)} for i in range(1, 8)]
    mp_peers = [{X: ring(x, i // 4), Y: ring(y, i % 4)} for i in range(1, 16)]
    greet(dp_peers + mp_peers)

    order = (2, 1, -1, 0)
    swap = [remote(gsend.at[i], grecv.at[i], ds.at[i], dr.at[i], {CORE: other}) for i in range(4)]

    def grad_rows(dz, c):
        cols = pl.ds(mul_of((ring(z, dz) * 2 + c) * ROWS, ROWS), ROWS)
        return lax.dot_general(feat[:, cols], bg[...], (((0,), (0,)), ((), ())), preferred_element_type=F32)

    hop = {}
    for h, s in enumerate((1, -1)):
        for kind, to in enumerate((s, s, -s)):
            for j in range(4):
                rows = pl.ds(0, 80) if j == 0 else pl.ds(16 + 64 * j, 64)
                hop[h, kind, j] = remote(qs.at[h, kind, rows], qr.at[h, kind, rows],
                                         zs.at[h, kind, j], zr.at[h, kind, j], {Z: ring(z, to)})

    def exponent_of(bound):
        return jnp.ceil(4.0 * jnp.log2(jnp.maximum(bound, 1e-30)) + 0.02)

    def power(exponent):
        return jnp.exp(exponent * (math.log(2.0) / 4.0))

    def received(h, kind):
        exponent = qr[h, kind, 0:16, :].astype(jnp.int32).astype(F32)[0:1]
        return power(exponent)

    def head_of(h, kind, bound):
        exponent = exponent_of(bound)
        qs[h, kind, 0:16, :] = jnp.broadcast_to(exponent, (16, 512)).astype(jnp.int32).astype(jnp.int16)
        return LEVELS * power(-exponent)

    def both_cores(i, h):
        cols = slice(512 * h, 512 * (h + 1))
        size = jnp.zeros((8, 512), F32)
        for j in range(4):
            rows = slice(64 * j, 64 * (j + 1))
            t = gown[i, rows, cols] + grecv[i, rows, cols]
            gown[i, rows, cols] = t
            size = jnp.maximum(size, jnp.max(jnp.abs(t).reshape(8, 8, 512), axis=0))
        return jnp.max(size, axis=0, keepdims=True)

    def own(i, h, j):
        return gown[i, 64 * j:64 * (j + 1), 512 * h:512 * (h + 1)]

    def code(value, scale):
        return jnp.round(value * scale).astype(jnp.int32).astype(jnp.int16)

    def value_of(h, kind, j, unit):
        return qr[h, kind, 16 + 64 * j:80 + 64 * j, :].astype(jnp.int32).astype(F32) * unit

    def straight(i, h, kind):
        scale = head_of(h, kind, both_cores(i, h))
        for j in range(4):
            qs[h, kind, 16 + 64 * j:80 + 64 * j, :] = code(own(i, h, j), scale)
            hop[h, kind, j].start()

    def pass_on(i, h):
        size = both_cores(i, h)
        hop[h, 0, 0].wait_recv()
        far_size = received(h, 0)
        scale = head_of(h, 1, size + far_size)
        for j in range(4):
            if j > 0:
                hop[h, 0, j].wait_recv()
            qs[h, 1, 16 + 64 * j:80 + 64 * j, :] = code(own(i, h, j) + value_of(h, 0, j, far_size / LEVELS), scale)
            hop[h, 1, j].start()

    for i, dz in enumerate(order):
        gsend[i] = grad_rows(dz, other)
        swap[i].start()
        gown[i] = grad_rows(dz, core)
        if i == 1:
            swap[0].wait_recv()
            straight(0, 0, 0)
            straight(0, 1, 0)
        if i == 2:
            swap[1].wait_recv()
            straight(1, 1, 2)
        if i == 3:
            swap[2].wait_recv()
            straight(2, 0, 2)
    pass_on(1, 0)
    pass_on(2, 1)
    swap[3].wait_recv()
    squares = jnp.zeros((8, 128), F32)
    units = {}
    for j in range(4):
        for h in range(2):
            hop[h, 2, j].wait_recv()
            hop[h, 1, j].wait_recv()
            if j == 0:
                units[h] = [received(h, kind) / LEVELS for kind in (1, 2)]
            part = gown[3, 64 * j:64 * (j + 1), 512 * h:512 * (h + 1)] + grecv[3, 64 * j:64 * (j + 1), 512 * h:512 * (h + 1)]
            g = part + value_of(h, 1, j, units[h][0]) + value_of(h, 2, j, units[h][1])
            for c in range(4):
                piece = g[:, c * 128:(c + 1) * 128]
                gv[pl.ds(64 * j * 8 + 4 * h + c, 64, stride=8), :] = piece
                squares = squares + jnp.sum((piece * piece).reshape(8, 8, 128), axis=0)

    n1[me, 0:8, :] = squares
    n1[me, 8:16, :] = loss_in[...]
    near = [remote(n1.at[me], n1.at[me], ns.at[i], nr.at[i], p) for i, p in enumerate(dp_peers)]
    for c in near:
        c.start()
    for c in near:
        c.wait_recv()
    sums = n1[0]
    for i in range(1, 8):
        sums = sums + n1[i]
    n2[plane] = sums
    far = [remote(n2.at[plane], n2.at[plane], ms.at[i], mr.at[i], p) for i, p in enumerate(mp_peers)]
    for c in far:
        c.start()
    for c in far:
        c.wait_recv()
    sums = n2[0]
    for i in range(1, 16):
        sums = sums + n2[i]
    loss[...] = sums[8:16]
    squared = jnp.sum(jnp.sum(sums[0:8], axis=1, keepdims=True), axis=0, keepdims=True)
    clip = jnp.minimum(1.0, MAX_NORM / (jnp.sqrt(squared) + 1e-06))

    def place(device, q):
        return pl.ds(mul_of(device * 2048 + q * 256, 256), 256)

    def block(device, q):
        return wk.at[place(device, q)]

    spread = {}
    for q in range(8):
        s = 1 if q % 2 == 0 else -1
        src = {0: (me, {Z: ring(z, 1)}), 1: (me, {Z: ring(z, -1)}),
               2: (ring(z, -s) * 2 + core, {Z: ring(z, s)}),
               3: (me, {CORE: other}), 4: (ring(z, -1) * 2 + core, {CORE: other}),
               5: (ring(z, 1) * 2 + core, {CORE: other}), 6: (ring(z, 2) * 2 + core, {CORE: other})}
        for kind, (device, to) in src.items():
            b = block(device, q)
            spread[q, kind] = remote(b, b, ws.at[q, kind], wr.at[q, kind], to)
    for q in range(8):
        rows = pl.ds(256 * q, 256)
        g = gv[rows, :] * clip
        m = 0.9 * moment[rows, :] + 0.1 * g
        v = 0.999 * second[rows, :] + 0.001 * g * g
        old = master[rows, :]
        first_hat = m * (1.0 / (1.0 - 0.9 ** 10))
        second_hat = v * (1.0 / (1.0 - 0.999 ** 10))
        new = old - 0.001 * (first_hat / (jnp.sqrt(second_hat) + 1e-08) + 0.1 * old)
        mo[rows, :] = new
        vo[rows, :] = m
        so[rows, :] = v
        wk[place(me, q), :] = new.astype(BF)
        for kind in (0, 1, 3):
            spread[q, kind].start()
    local = [pltpu.make_async_copy(a, b, ls.at[i])
             for i, (a, b) in enumerate(((mo, master_new), (vo, moment_new), (so, second_new)))]
    for c in local:
        c.start()
    for q in range(8):
        with_relay, against = (0, 1) if q % 2 == 0 else (1, 0)
        spread[q, with_relay].wait_recv()
        spread[q, 2].start()
        spread[q, 4 + with_relay].start()
        spread[q, against].wait_recv()
        spread[q, 4 + against].start()
    out = {}

    def store(i, device):
        rows = pl.ds(mul_of(device * 2048, 2048), 2048)
        out[i] = pltpu.make_async_copy(wk.at[rows], work.at[rows], cs.at[i])
        out[i].start()

    store(0, me)
    store(1, ring(z, 1) * 2 + core)
    store(2, ring(z, -1) * 2 + core)
    for q in range(8):
        spread[q, 2].wait_recv()
        spread[q, 6].start()
    store(3, ring(z, 2) * 2 + core)
    for i, kind in enumerate((3, 4, 5, 6)):
        for q in range(8):
            spread[q, kind].wait_recv()
        store(4 + i, ring(z, (0, -1, 1, 2)[i]) * 2 + other)
    for c in local:
        c.wait()
    for i in out:
        out[i].wait()
    for c in swap + near + far:
        c.wait_send()
    for table in (hop, spread):
        for key in table:
            table[key].wait_send()


def rows_of(value):
    r = value.shape[0]
    return value.reshape(r, 2, 4, 128).transpose(0, 2, 1, 3).reshape(r * 8, 128)


def from_rows(value):
    r = value.shape[0] // 8
    return value.reshape(r, 4, 2, 128).transpose(0, 2, 1, 3).reshape(r, 2, 512)


def per_device(features, rewards, old_values, dones, lengths, proj_weights, down_weight, value_head,
               master, moment, second):
    dma = pltpu.SemaphoreType.DMA
    vm = pl.BlockSpec(memory_space=pltpu.VMEM)
    sm = pl.BlockSpec(memory_space=pltpu.SMEM)
    anyspace = pl.BlockSpec(memory_space=pl.ANY)
    w4 = proj_weights.reshape(D, 2, 4, 128).transpose(2, 0, 1, 3).reshape(4, D, 256)
    bg, loss_part = pl.pallas_call(
        forward_kernel,
        name="forward_and_backward",
        out_shape=(jax.ShapeDtypeStruct((TOK, 2 * FFL), BF), jax.ShapeDtypeStruct((8, 128), F32)),
        in_specs=[vm] * 7 + [sm],
        out_specs=(vm, vm),
        scratch_shapes=[
            pltpu.VMEM((4, TOK, 256), F32), pltpu.VMEM((TOK, FFL), BF), pltpu.VMEM((4, TOK, 512), BF),
            pltpu.VMEM((4, 3, 4, 64, 512), BF), pltpu.VMEM((4, 3, 64, 512), BF), pltpu.VMEM((4, TOK, 512), BF),
            pltpu.VMEM((64, D), F32),
            dma((4, 3, 4)), dma((4, 3, 4)), dma((4, 3)), dma((4, 3)),
            dma((4, 3)), dma((4, 3)), dma((4, 4, 3)), dma((4, 4, 3)),
        ],
        compiler_params=pltpu.CompilerParams(collective_id=0, has_side_effects=True, vmem_limit_bytes=VMEM_LIMIT),
    )(features, w4, down_weight, value_head.reshape(1, D), rewards, old_values, dones, lengths)
    rows = jax.ShapeDtypeStruct((8 * ROWS, 128), F32)
    work, master_new, moment_new, second_new, loss = pl.pallas_call(
        update_kernel,
        name="gradients_and_update",
        out_shape=(jax.ShapeDtypeStruct((8 * D, 128), BF), rows, rows, rows, jax.ShapeDtypeStruct((8, 128), F32)),
        in_specs=[vm] * 6,
        out_specs=(anyspace, anyspace, anyspace, anyspace, vm),
        scratch_shapes=[
            pltpu.VMEM((4, ROWS, 1024), F32), pltpu.VMEM((4, ROWS, 1024), F32), pltpu.VMEM((4, ROWS, 1024), F32),
            pltpu.VMEM((2, 3, 16 + ROWS, 512), jnp.int16), pltpu.VMEM((2, 3, 16 + ROWS, 512), jnp.int16),
            pltpu.VMEM((8 * ROWS, 128), F32), pltpu.VMEM((8 * D, 128), BF),
            pltpu.VMEM((8 * ROWS, 128), F32), pltpu.VMEM((8 * ROWS, 128), F32), pltpu.VMEM((8 * ROWS, 128), F32),
            pltpu.VMEM((8, 16, 128), F32), pltpu.VMEM((16, 16, 128), F32),
            dma((4,)), dma((4,)), dma((2, 3, 4)), dma((2, 3, 4)), dma((7,)), dma((7,)), dma((15,)), dma((15,)),
            dma((8, 7)), dma((8, 7)), dma((8,)), dma((8,)), dma((3,)),
        ],
        compiler_params=pltpu.CompilerParams(collective_id=1, has_side_effects=True, vmem_limit_bytes=VMEM_LIMIT),
    )(features, bg, loss_part, rows_of(master), rows_of(moment), rows_of(second))
    return (from_rows(master_new), from_rows(moment_new), from_rows(second_new), from_rows(work), loss[0, 0])


def solution(mesh):
    finer = Mesh(mesh.devices.reshape(4, 2, 4, 4), (Z, CORE, X, Y))
    return jax.shard_map(
        per_device,
        mesh=finer,
        in_specs=(
            P(DP, None), P(DP, None), P(DP, None), P(DP, None), P(DP),
            P(None, None, MP), P(MP, None), P(),
            P(DP, None, MP), P(DP, None, MP), P(DP, None, MP),
        ),
        out_specs=(P(DP, None, MP), P(DP, None, MP), P(DP, None, MP), P(None, None, MP), P()),
        check_vma=False,
    )
```

```python
import math

import jax
import jax.numpy as jnp
from jax import lax
from jax.experimental import pallas as pl
from jax.experimental.pallas import tpu as pltpu
from jax.sharding import Mesh
from jax.sharding import PartitionSpec as P

Z, CORE, X, Y = "dp_0", "dp_1", "mp_0", "mp_1"
DP = (Z, CORE)
MP = (X, Y)
GAMMA = 0.99
LAMBDA = 0.95
MAX_NORM = 0.05
D = 2048
TOK = 1024
FFL = 512
ROWS = 256
BF = jnp.bfloat16
LEVELS = 32000.0
F32 = jnp.float32
VMEM_LIMIT = 62 * 1024 * 1024


def mul_of(v, n):
    return pl.multiple_of(v, n)


def ring(v, d):
    return lax.rem(v + (d + 4), 4)


def remote(src, dst, send, recv, device):
    return pltpu.make_async_remote_copy(
        src_ref=src, dst_ref=dst, send_sem=send, recv_sem=recv,
        device_id=device, device_id_type=pl.DeviceIdType.MESH,
    )


def greet(devices):
    barrier = pltpu.get_barrier_semaphore()
    for device in devices:
        pl.semaphore_signal(barrier, inc=1, device_id=device, device_id_type=pl.DeviceIdType.MESH)
    pl.semaphore_wait(barrier, len(devices))


def own_targets(row, start, rew, old, dones, lengths):
    dn = jnp.broadcast_to(dones[pl.ds(row, 1), :].astype(F32), (8, 256))
    ov = jnp.broadcast_to(old[pl.ds(row, 1), :], (8, 256))
    rw = jnp.broadcast_to(rew[pl.ds(row, 1), :], (8, 256))
    lane = lax.broadcasted_iota(jnp.int32, (8, 256), 1)
    following = jnp.where(lane == 255, 0.0, pltpu.roll(ov, 255, axis=1))
    deltas = (rw + GAMMA * following * (1.0 - dn) - ov)[0:1]
    before = lax.broadcasted_iota(jnp.int32, (256, 256), 0) < lax.broadcasted_iota(jnp.int32, (256, 256), 1)
    counted_s = jnp.dot(dn.astype(BF), before.astype(F32).astype(BF), preferred_element_type=F32)[0:1]
    t = start + lax.broadcasted_iota(jnp.int32, (WT, 256), 0)
    s = lax.broadcasted_iota(jnp.int32, (WT, 256), 1)
    counted_t = jnp.sum(jnp.where(s < t, dn[0:1], 0.0), axis=1, keepdims=True)
    linked = (counted_t == counted_s) & (s >= t)
    powers = jnp.exp(jnp.maximum(s - t, 0).astype(F32) * math.log(GAMMA * LAMBDA))
    advantage = jnp.sum(jnp.where(linked, powers, 0.0) * deltas, axis=1, keepdims=True)
    own_old = jnp.sum(jnp.where(s == t, ov[0:1], 0.0), axis=1, keepdims=True)
    mask = jnp.where(t[:, 0:1] < lengths[row], 1.0, 0.0)
    return advantage + own_old, mask


STREAMS = ((True, 1), (True, -1), (False, 1), (False, -1))
WT = 32
WAVE = 512


def step_kernel(feat_hbm, w_hbm, down_hbm, master_hbm, moment_hbm, second_hbm, head, rew, old, dones, lengths,
                work, grad_out, sums_out,
                feat, w4, down, both, hid, part, rv1, rv2, og, mix, bg,
                master, moment, second, gsend, gown, grecv, qs, qr, gv, wk, n1, n2,
                fs, rs, os, s1, r1, s2, r2, gs1, gr1, gs2, gr2,
                ds, dr, zs, zr, ns, nr, ms, mr, ws, wr, cs, ls):
    z, core, x, y = (lax.axis_index(a) for a in (Z, CORE, X, Y))
    other = 1 - core
    me = z * 2 + core
    plane = x * 4 + y
    dp_peers = [{Z: ring(z, i // 2), CORE: lax.rem(core + i % 2, 2)} for i in range(1, 8)]
    mp_peers = [{X: ring(x, i // 4), Y: ring(y, i % 4)} for i in range(1, 16)]

    load_w = []
    for p in range(4):
        rows = pl.ds(4096 * p, 4096)
        load_w.append(pltpu.make_async_copy(w_hbm.at[rows], wk.at[rows], rs.at[p]))
        load_w[p].start()
    load_f = {}
    for w in range(2):
        for i, dy in enumerate((2, 1, -1, 0)):
            rows = pl.ds(mul_of(ring(y, dy) * 128 + WAVE * w, 128), 128)
            load_f[w, dy] = pltpu.make_async_copy(feat_hbm.at[rows], feat.at[rows], fs.at[w, i])
    load_d = pltpu.make_async_copy(down_hbm, down, os.at[0])
    load_f[0, 2].start()
    load_d.start()
    for key in load_f:
        if key != (0, 2):
            load_f[key].start()
    state = [pltpu.make_async_copy(a, b, os.at[i]) for i, a, b in
             ((1, master_hbm, master), (2, moment_hbm, moment), (3, second_hbm, second))]
    for c in state:
        c.start()
    greet(dp_peers + mp_peers)

    out_row = lax.broadcasted_iota(jnp.int32, (256, 256), 0)
    in_row = lax.broadcasted_iota(jnp.int32, (256, 256), 1)
    select = jnp.where(in_row == (out_row % 32) * 8 + out_row // 32, 1.0, 0.0).astype(BF)
    for p in range(4):
        load_w[p].wait()
        for u in range(8):
            base = 4096 * p + 512 * u
            pair = jnp.concatenate([wk[base:base + 256, :], wk[base + 256:base + 512, :]], axis=1)
            moved = jnp.dot(select, pair, preferred_element_type=F32).astype(BF)
            k = 512 * p + 64 * u
            for i in range(8):
                c, g = i // 2, i % 2
                for half in range(2):
                    w4[c, k + 32 * half:k + 32 * half + 32, 128 * g:128 * (g + 1)] = \
                        moved[32 * i:32 * (i + 1), 128 * half:128 * (half + 1)]
    load_d.wait()

    def peer(first, h, delta):
        along_x = STREAMS[h][0] == first
        return {X: ring(x, delta)} if along_x else {Y: ring(y, delta)}

    def tok(w, h, da, db):
        dx, dy = (da, db) if STREAMS[h][0] else (db, da)
        return pl.ds(mul_of(WAVE * w + ring(y, dy) * 128 + ring(x, dx) * WT, WT), WT)

    def offsets(h):
        s = STREAMS[h][1]
        return (2, s, -s, 0)

    def index(h, db):
        return offsets(h).index(db)

    one, two, g1, g2 = {}, {}, {}, {}
    for w in range(2):
        for h in range(4):
            s = STREAMS[h][1]
            for j, db in enumerate(offsets(h)):
                for kind, (da, to) in enumerate(((2, s), (s, s), (-s, -s))):
                    one[w, h, kind, j] = remote(part.at[h, tok(w, h, da, db)], rv1.at[w, h, kind, j],
                                                s1.at[w, h, kind, j], r1.at[w, h, kind, j], peer(True, h, to))
            for kind, (db, to) in enumerate(((2, s), (s, s), (-s, -s))):
                two[w, h, kind] = remote(part.at[h, tok(w, h, 0, db)], rv2.at[w, h, kind],
                                         s2.at[w, h, kind], r2.at[w, h, kind], peer(False, h, to))
            for kind, (db, to) in enumerate(((0, 1), (0, -1), (-s, s))):
                t = og.at[h, tok(w, h, 0, db)]
                g1[w, h, kind] = remote(t, t, gs1.at[w, h, kind], gr1.at[w, h, kind], peer(False, h, to))
            for k, db in enumerate((0, -s, s, 2)):
                for kind, (da, to) in enumerate(((0, 1), (0, -1), (-s, s))):
                    t = og.at[h, tok(w, h, da, db)]
                    g2[w, h, k, kind] = remote(t, t, gs2.at[w, h, k, kind], gr2.at[w, h, k, kind], peer(True, h, to))

    def chunk(w, dy):
        load_f[w, dy].wait()
        rows = pl.ds(mul_of(ring(y, dy) * 128 + WAVE * w, 128), 128)
        f = feat[rows, :]
        for c in range(4):
            gu = jnp.dot(f, w4[c], preferred_element_type=F32)
            both[c, rows, :] = gu
            gate, up = gu[:, :128], gu[:, 128:]
            hid[rows, c * 128:(c + 1) * 128] = (gate * jax.nn.sigmoid(gate) * up).astype(BF)
        v = hid[rows, :]
        for h in range(4):
            part[h, rows, :] = jnp.dot(
                v, down[:, h * 512:(h + 1) * 512], preferred_element_type=F32).astype(BF)
        for h in (0, 1):
            one[w, h, 0, index(h, dy)].start()
            one[w, h, 2, index(h, dy)].start()
        for h in (2, 3):
            s = STREAMS[h][1]
            if dy == 2:
                for j in range(4):
                    one[w, h, 0, j].start()
            elif dy == -s:
                for j in range(4):
                    one[w, h, 2, j].start()

    def pass_on(w, h, j):
        s = STREAMS[h][1]
        one[w, h, 0, j].wait_recv()
        t = tok(w, h, s, offsets(h)[j])
        part[h, t, :] = (part[h, t, :].astype(F32) + rv1[w, h, 0, j].astype(F32)).astype(BF)
        one[w, h, 1, j].start()

    def pass_x(w, dy):
        for h in (0, 1):
            pass_on(w, h, index(h, dy))

    def pass_y(w, h):
        for j in range(4):
            pass_on(w, h, j)

    def finish_one(w, h, j):
        one[w, h, 1, j].wait_recv()
        one[w, h, 2, j].wait_recv()
        t = tok(w, h, 0, offsets(h)[j])
        total = part[h, t, :].astype(F32) + rv1[w, h, 1, j].astype(F32) + rv1[w, h, 2, j].astype(F32)
        if j == 3:
            two[w, h, 1].wait_recv()
            two[w, h, 2].wait_recv()
            mix[w, :, h * 512:(h + 1) * 512] = total + rv2[w, h, 1].astype(F32) + rv2[w, h, 2].astype(F32)
            return
        if j == 1:
            two[w, h, 0].wait_recv()
            total = total + rv2[w, h, 0].astype(F32)
        part[h, t, :] = total.astype(BF)
        two[w, h, j].start()

    def finish(w, j):
        for h in range(4):
            finish_one(w, h, j)

    def own_loss(w, targets, mask):
        mine = pl.ds(mul_of(WAVE * w + y * 128 + x * WT, WT), WT)
        stream = feat[mine, :].astype(F32) + mix[w]
        vh = head[...]
        norm = lax.rsqrt(jnp.sum(stream * stream, axis=1, keepdims=True) / D + 1e-05)
        estimate = norm * jnp.sum(stream * vh, axis=1, keepdims=True)
        errors = estimate - targets
        total_tokens = TOK * 8
        coeff = 2.0 * mask * errors / total_tokens
        inner = coeff * estimate / D
        a = norm * coeff
        b = norm * norm * inner
        for h in range(4):
            cols = slice(h * 512, (h + 1) * 512)
            og[h, mine, :] = (a * vh[:, cols] - b * stream[:, cols]).astype(BF)
        return jnp.sum(mask * errors * errors, axis=0, keepdims=True) / total_tokens

    waited = set()

    def arrive(name, key):
        if (name, key) not in waited:
            waited.add((name, key))
            {"g1": g1, "g2": g2}[name][key].wait_recv()

    def ahead(h):
        return 0 if STREAMS[h][1] == 1 else 1

    def spread(w, h, k):
        g2[w, h, k, 0].start()
        g2[w, h, k, 1].start()

    def relay(w, k):
        for h in range(4):
            arrive("g2", (w, h, k, ahead(h)))
            g2[w, h, k, 2].start()

    def gather_0(w):
        for h in range(4):
            g1[w, h, 0].start()
            g1[w, h, 1].start()
        for h in range(4):
            spread(w, h, 0)

    def gather_1(w):
        for h in range(4):
            arrive("g1", (w, h, ahead(h)))
            g1[w, h, 2].start()
            spread(w, h, 1)

    def gather_2(w):
        relay(w, 0)
        for h in range(4):
            arrive("g1", (w, h, 1 - ahead(h)))
            spread(w, h, 2)

    def gather_3(w):
        for h in range(4):
            arrive("g1", (w, h, 2))
            spread(w, h, 3)

    def backward(w, dy):
        for h in (0, 1):
            k = (0, -STREAMS[h][1], STREAMS[h][1], 2).index(dy)
            for kind in range(3):
                arrive("g2", (w, h, k, kind))
        if dy != 0:
            for h in (2, 3):
                for k in range(4):
                    arrive("g2", (w, h, k, {-1: 0, 1: 1, 2: 2}[dy]))
        rows = pl.ds(mul_of(ring(y, dy) * 128 + WAVE * w, 128), 128)
        hg = None
        for h in range(4):
            term = lax.dot_general(og[h, rows, :], down[:, h * 512:(h + 1) * 512],
                                   (((1,), (1,)), ((), ())), preferred_element_type=F32)
            hg = term if hg is None else hg + term
        for c in range(4):
            gate, up = both[c, rows, :128], both[c, rows, 128:]
            d = hg[:, c * 128:(c + 1) * 128]
            sig = jax.nn.sigmoid(gate)
            bg[rows, c * 256:c * 256 + 128] = (d * up * sig * (1.0 + gate * (1.0 - sig))).astype(BF)
            bg[rows, c * 256 + 128:(c + 1) * 256] = (d * gate * sig).astype(BF)

    chunk(0, 2)
    chunk(0, 1)
    pass_x(0, 2)
    pass_y(0, 2)
    chunk(0, -1)
    pass_x(0, 1)
    pass_y(0, 3)
    chunk(0, 0)
    pass_x(0, -1)
    chunk(1, 2)
    own = [own_targets(2 * w + y // 2, (y % 2) * 128 + x * WT, rew, old, dones, lengths) for w in range(2)]
    finish(0, 0)
    pass_x(0, 0)
    chunk(1, 1)
    finish(0, 1)
    pass_x(1, 2)
    pass_y(1, 2)
    chunk(1, -1)
    finish(0, 2)
    pass_x(1, 1)
    finish(0, 3)
    loss = own_loss(0, *own[0])
    gather_0(0)
    pass_y(1, 3)
    chunk(1, 0)
    pass_x(1, -1)
    finish(1, 0)
    pass_x(1, 0)
    gather_1(0)
    finish(1, 1)
    gather_2(0)
    finish(1, 2)
    finish(1, 3)
    loss = loss + own_loss(1, *own[1])
    gather_0(1)
    gather_3(0)
    relay(0, 1)
    gather_1(1)
    relay(0, 2)
    relay(0, 3)
    gather_2(1)
    backward(0, 0)
    gather_3(1)
    backward(0, -1)
    relay(1, 1)
    backward(0, 1)
    relay(1, 2)
    backward(0, 2)
    relay(1, 3)
    for dy in (0, -1, 1, 2):
        backward(1, dy)

    order = (2, 1, -1, 0)
    swap = [remote(gsend.at[i], grecv.at[i], ds.at[i], dr.at[i], {CORE: other}) for i in range(4)]

    def grad_rows(dz, c):
        cols = pl.ds(mul_of((ring(z, dz) * 2 + c) * ROWS, ROWS), ROWS)
        return lax.dot_general(feat[:, cols], bg[...], (((0,), (0,)), ((), ())), preferred_element_type=F32)

    hop = {}
    for h, s in enumerate((1, -1)):
        for kind, to in enumerate((s, s, -s)):
            for j in range(4):
                rows = pl.ds(0, 80) if j == 0 else pl.ds(16 + 64 * j, 64)
                hop[h, kind, j] = remote(qs.at[h, kind, rows], qr.at[h, kind, rows],
                                         zs.at[h, kind, j], zr.at[h, kind, j], {Z: ring(z, to)})

    def exponent_of(bound):
        return jnp.ceil(4.0 * jnp.log2(jnp.maximum(bound, 1e-30)) + 0.02)

    def power(exponent):
        return jnp.exp(exponent * (math.log(2.0) / 4.0))

    def received(h, kind):
        exponent = qr[h, kind, 0:16, :].astype(jnp.int32).astype(F32)[0:1]
        return power(exponent)

    def head_of(h, kind, bound):
        exponent = exponent_of(bound)
        qs[h, kind, 0:16, :] = jnp.broadcast_to(exponent, (16, 512)).astype(jnp.int32).astype(jnp.int16)
        return LEVELS * power(-exponent)

    def both_cores(i, h):
        cols = slice(512 * h, 512 * (h + 1))
        size = jnp.zeros((8, 512), F32)
        for j in range(4):
            rows = slice(64 * j, 64 * (j + 1))
            t = gown[i, rows, cols] + grecv[i, rows, cols]
            gown[i, rows, cols] = t
            size = jnp.maximum(size, jnp.max(jnp.abs(t).reshape(8, 8, 512), axis=0))
        return jnp.max(size, axis=0, keepdims=True)

    def mine_of(i, h, j):
        return gown[i, 64 * j:64 * (j + 1), 512 * h:512 * (h + 1)]

    def code(value, scale):
        return jnp.round(value * scale).astype(jnp.int32).astype(jnp.int16)

    def value_of(h, kind, j, unit):
        return qr[h, kind, 16 + 64 * j:80 + 64 * j, :].astype(jnp.int32).astype(F32) * unit

    def straight(i, h, kind):
        scale = head_of(h, kind, both_cores(i, h))
        for j in range(4):
            qs[h, kind, 16 + 64 * j:80 + 64 * j, :] = code(mine_of(i, h, j), scale)
            hop[h, kind, j].start()

    def pass_sum(i, h):
        size = both_cores(i, h)
        hop[h, 0, 0].wait_recv()
        far_size = received(h, 0)
        scale = head_of(h, 1, size + far_size)
        for j in range(4):
            if j > 0:
                hop[h, 0, j].wait_recv()
            qs[h, 1, 16 + 64 * j:80 + 64 * j, :] = code(mine_of(i, h, j) + value_of(h, 0, j, far_size / LEVELS), scale)
            hop[h, 1, j].start()

    for i, dz in enumerate(order):
        gsend[i] = grad_rows(dz, other)
        swap[i].start()
        gown[i] = grad_rows(dz, core)
        if i == 1:
            swap[0].wait_recv()
            straight(0, 0, 0)
            straight(0, 1, 0)
        if i == 2:
            swap[1].wait_recv()
            straight(1, 1, 2)
        if i == 3:
            swap[2].wait_recv()
            straight(2, 0, 2)
    pass_sum(1, 0)
    pass_sum(2, 1)
    swap[3].wait_recv()
    squares = jnp.zeros((8, 128), F32)
    units = {}
    for j in range(4):
        for h in range(2):
            hop[h, 2, j].wait_recv()
            hop[h, 1, j].wait_recv()
            if j == 0:
                units[h] = [received(h, kind) / LEVELS for kind in (1, 2)]
            owned = gown[3, 64 * j:64 * (j + 1), 512 * h:512 * (h + 1)] + grecv[3, 64 * j:64 * (j + 1), 512 * h:512 * (h + 1)]
            g = owned + value_of(h, 1, j, units[h][0]) + value_of(h, 2, j, units[h][1])
            for c in range(4):
                piece = g[:, c * 128:(c + 1) * 128]
                gv[pl.ds(64 * j * 8 + 4 * h + c, 64, stride=8), :] = piece
                squares = squares + jnp.sum((piece * piece).reshape(8, 8, 128), axis=0)

    give = pltpu.make_async_copy(gv, grad_out, ls.at[0])
    give.start()

    n1[me, 0:8, :] = squares
    n1[me, 8:16, :] = jnp.broadcast_to(loss, (8, 128))
    near = [remote(n1.at[me], n1.at[me], ns.at[i], nr.at[i], p) for i, p in enumerate(dp_peers)]
    for c in near:
        c.start()
    for c in near:
        c.wait_recv()
    sums = n1[0]
    for i in range(1, 8):
        sums = sums + n1[i]
    n2[plane] = sums
    far = [remote(n2.at[plane], n2.at[plane], ms.at[i], mr.at[i], p) for i, p in enumerate(mp_peers)]
    for c in far:
        c.start()
    for c in far:
        c.wait_recv()
    sums = n2[0]
    for i in range(1, 16):
        sums = sums + n2[i]
    sums_out[...] = sums
    squared = jnp.sum(jnp.sum(sums[0:8], axis=1, keepdims=True), axis=0, keepdims=True)
    clip = jnp.minimum(1.0, MAX_NORM / (jnp.sqrt(squared) + 1e-06))

    def place(device, q):
        return pl.ds(mul_of(device * 2048 + q * 256, 256), 256)

    def block(device, q):
        return wk.at[place(device, q)]

    spread_dp = {}
    for q in range(8):
        s = 1 if q % 2 == 0 else -1
        src = {0: (me, {Z: ring(z, 1)}), 1: (me, {Z: ring(z, -1)}),
               2: (ring(z, -s) * 2 + core, {Z: ring(z, s)}),
               3: (me, {CORE: other}), 4: (ring(z, -1) * 2 + core, {CORE: other}),
               5: (ring(z, 1) * 2 + core, {CORE: other}), 6: (ring(z, 2) * 2 + core, {CORE: other})}
        for kind, (device, to) in src.items():
            b = block(device, q)
            spread_dp[q, kind] = remote(b, b, ws.at[q, kind], wr.at[q, kind], to)
    for c in state:
        c.wait()
    for q in range(8):
        rows = pl.ds(256 * q, 256)
        g = gv[rows, :] * clip
        new, _, _ = updated(g, master[rows, :], moment[rows, :], second[rows, :])
        wk[place(me, q), :] = new.astype(BF)
        for kind in (0, 1, 3):
            spread_dp[q, kind].start()
    for q in range(8):
        with_relay, against = (0, 1) if q % 2 == 0 else (1, 0)
        spread_dp[q, with_relay].wait_recv()
        spread_dp[q, 2].start()
        spread_dp[q, 4 + with_relay].start()
        spread_dp[q, against].wait_recv()
        spread_dp[q, 4 + against].start()
    out = {}

    def store(i, device):
        rows = pl.ds(mul_of(device * 2048, 2048), 2048)
        out[i] = pltpu.make_async_copy(wk.at[rows], work.at[rows], cs.at[i])
        out[i].start()

    store(0, me)
    store(1, ring(z, 1) * 2 + core)
    store(2, ring(z, -1) * 2 + core)
    for q in range(8):
        spread_dp[q, 2].wait_recv()
        spread_dp[q, 6].start()
    store(3, ring(z, 2) * 2 + core)
    for i, kind in enumerate((3, 4, 5, 6)):
        for q in range(8):
            spread_dp[q, kind].wait_recv()
        store(4 + i, ring(z, (0, -1, 1, 2)[i]) * 2 + other)
    give.wait()
    for i in out:
        out[i].wait()
    for c in swap + near + far:
        c.wait_send()
    for table in (one, two, g1, g2, hop, spread_dp):
        for key in table:
            table[key].wait_send()


def tail_kernel(grad, sums, master, moment, second, master_new, moment_new, second_new, loss):
    squared = jnp.sum(jnp.sum(sums[0:8, :], axis=1, keepdims=True), axis=0, keepdims=True)
    clip = jnp.minimum(1.0, MAX_NORM / (jnp.sqrt(squared) + 1e-06))
    new, m, v = updated(grad[...] * clip, master[...], moment[...], second[...])
    master_new[...] = new
    moment_new[...] = m
    second_new[...] = v
    loss[...] = sums[8:9, 0:1]


def updated(g, old, moment, second):
    m = 0.9 * moment + 0.1 * g
    v = 0.999 * second + 0.001 * g * g
    first_hat = m * (1.0 / (1.0 - 0.9 ** 10))
    second_hat = v * (1.0 / (1.0 - 0.999 ** 10))
    return old - 0.001 * (first_hat / (jnp.sqrt(second_hat) + 1e-08) + 0.1 * old), m, v


def rows_of(value):
    r = value.shape[0]
    return value.reshape(r, 2, 4, 128).transpose(0, 2, 1, 3).reshape(r * 8, 128)


def from_rows(value):
    r = value.shape[0] // 8
    return value.reshape(r, 4, 2, 128).transpose(0, 2, 1, 3).reshape(r, 2, 512)


def per_device(features, rewards, old_values, dones, lengths, proj_weights, down_weight, value_head,
               master, moment, second):
    dma = pltpu.SemaphoreType.DMA
    vm = pl.BlockSpec(memory_space=pltpu.VMEM)
    sm = pl.BlockSpec(memory_space=pltpu.SMEM)
    hbm = pl.BlockSpec(memory_space=pl.ANY)
    state = (rows_of(master), rows_of(moment), rows_of(second))
    rows = jax.ShapeDtypeStruct((8 * ROWS, 128), F32)
    row_scratch = pltpu.VMEM((8 * ROWS, 128), F32)
    block_scratch = pltpu.VMEM((4, ROWS, 1024), F32)
    link_scratch = pltpu.VMEM((2, 3, 16 + ROWS, 512), jnp.int16)
    work, grad, sums = pl.pallas_call(
        step_kernel,
        name="critic_step",
        out_shape=(jax.ShapeDtypeStruct((8 * D, 128), BF), rows, jax.ShapeDtypeStruct((16, 128), F32)),
        in_specs=[hbm] * 6 + [vm] * 4 + [sm],
        out_specs=(hbm, hbm, vm),
        scratch_shapes=[
            pltpu.VMEM((TOK, D), BF), pltpu.VMEM((4, D, 256), BF), pltpu.VMEM((FFL, D), BF),
            pltpu.VMEM((4, TOK, 256), F32), pltpu.VMEM((TOK, FFL), BF), pltpu.VMEM((4, TOK, 512), BF),
            pltpu.VMEM((2, 4, 3, 4, WT, 512), BF), pltpu.VMEM((2, 4, 3, WT, 512), BF), pltpu.VMEM((4, TOK, 512), BF),
            pltpu.VMEM((2, WT, D), F32), pltpu.VMEM((TOK, 2 * FFL), BF),
            row_scratch, row_scratch, row_scratch, block_scratch, block_scratch, block_scratch,
            link_scratch, link_scratch, row_scratch, pltpu.VMEM((8 * D, 128), BF),
            pltpu.VMEM((8, 16, 128), F32), pltpu.VMEM((16, 16, 128), F32),
            dma((2, 4)), dma((4,)), dma((4,)),
            dma((2, 4, 3, 4)), dma((2, 4, 3, 4)), dma((2, 4, 3)), dma((2, 4, 3)),
            dma((2, 4, 3)), dma((2, 4, 3)), dma((2, 4, 4, 3)), dma((2, 4, 4, 3)),
            dma((4,)), dma((4,)), dma((2, 3, 4)), dma((2, 3, 4)), dma((7,)), dma((7,)), dma((15,)), dma((15,)),
            dma((8, 7)), dma((8, 7)), dma((8,)), dma((1,)),
        ],
        compiler_params=pltpu.CompilerParams(collective_id=0, has_side_effects=True, vmem_limit_bytes=VMEM_LIMIT),
    )(features, rows_of(proj_weights), down_weight, *state, value_head.reshape(1, D), rewards, old_values, dones, lengths)
    block = pl.BlockSpec((512, 128), lambda i: (i, 0))
    whole = pl.BlockSpec((16, 128), lambda i: (0, 0))
    master_new, moment_new, second_new, loss = pl.pallas_call(
        tail_kernel,
        name="optimizer_state",
        grid=(4,),
        out_shape=(rows, rows, rows, jax.ShapeDtypeStruct((1, 1), F32)),
        in_specs=[block, whole, block, block, block],
        out_specs=(block, block, block, pl.BlockSpec((1, 1), lambda i: (0, 0))),
    )(grad, sums, *state)
    return (from_rows(master_new), from_rows(moment_new), from_rows(second_new), from_rows(work), loss.reshape(()))


def solution(mesh):
    finer = Mesh(mesh.devices.reshape(4, 2, 4, 4), (Z, CORE, X, Y))
    return jax.shard_map(
        per_device,
        mesh=finer,
        in_specs=(
            P(DP, None), P(DP, None), P(DP, None), P(DP, None), P(DP),
            P(None, None, MP), P(MP, None), P(),
            P(DP, None, MP), P(DP, None, MP), P(DP, None, MP),
        ),
        out_specs=(P(DP, None, MP), P(DP, None, MP), P(DP, None, MP), P(None, None, MP), P()),
        check_vma=False,
    )
```

```python
import math

import jax
import jax.numpy as jnp
from jax import lax
from jax.experimental import pallas as pl
from jax.experimental.pallas import tpu as pltpu
from jax.sharding import Mesh
from jax.sharding import PartitionSpec as P

Z, CORE, X, Y = "dp_0", "dp_1", "mp_0", "mp_1"
DP = (Z, CORE)
MP = (X, Y)
GAMMA = 0.99
LAMBDA = 0.95
MAX_NORM = 0.05
D = 2048
TOK = 1024
FFL = 512
ROWS = 256
BF = jnp.bfloat16
LEVELS = 32000.0
F32 = jnp.float32
VMEM_LIMIT = 54 * 1024 * 1024


def mul_of(v, n):
    return pl.multiple_of(v, n)


def ring(v, d):
    return lax.rem(v + (d + 4), 4)


def remote(src, dst, send, recv, device):
    return pltpu.make_async_remote_copy(
        src_ref=src, dst_ref=dst, send_sem=send, recv_sem=recv,
        device_id=device, device_id_type=pl.DeviceIdType.MESH,
    )


def greet(devices):
    barrier = pltpu.get_barrier_semaphore()
    for device in devices:
        pl.semaphore_signal(barrier, inc=1, device_id=device, device_id_type=pl.DeviceIdType.MESH)


def greeted(devices):
    pl.semaphore_wait(pltpu.get_barrier_semaphore(), len(devices))


def own_targets(row, start, rew, old, dones, lengths):
    dn = jnp.broadcast_to(dones[pl.ds(row, 1), :].astype(F32), (8, 256))
    ov = jnp.broadcast_to(old[pl.ds(row, 1), :], (8, 256))
    rw = jnp.broadcast_to(rew[pl.ds(row, 1), :], (8, 256))
    lane = lax.broadcasted_iota(jnp.int32, (8, 256), 1)
    following = jnp.where(lane == 255, 0.0, pltpu.roll(ov, 255, axis=1))
    deltas = (rw + GAMMA * following * (1.0 - dn) - ov)[0:1]
    before = lax.broadcasted_iota(jnp.int32, (256, 256), 0) < lax.broadcasted_iota(jnp.int32, (256, 256), 1)
    counted_s = jnp.dot(dn.astype(BF), before.astype(F32).astype(BF), preferred_element_type=F32)[0:1]
    t = start + lax.broadcasted_iota(jnp.int32, (WT, 256), 0)
    s = lax.broadcasted_iota(jnp.int32, (WT, 256), 1)
    counted_t = jnp.sum(jnp.where(s < t, dn[0:1], 0.0), axis=1, keepdims=True)
    linked = (counted_t == counted_s) & (s >= t)
    powers = jnp.exp(jnp.maximum(s - t, 0).astype(F32) * math.log(GAMMA * LAMBDA))
    advantage = jnp.sum(jnp.where(linked, powers, 0.0) * deltas, axis=1, keepdims=True)
    own_old = jnp.sum(jnp.where(s == t, ov[0:1], 0.0), axis=1, keepdims=True)
    mask = jnp.where(t[:, 0:1] < lengths[row], 1.0, 0.0)
    return advantage + own_old, mask


STREAMS = ((True, 1), (True, -1), (False, 1), (False, -1))
WT = 32
WAVE = 512


def step_kernel(feat_hbm, w_hbm, down_hbm, master_hbm, moment_hbm, second_hbm,
                head_hbm, rew_hbm, old_hbm, dones_hbm, lengths_hbm,
                wk, mo, vo, so, sums_out,
                feat, w4, down, both, hid, part, rv1, rv2, og, mix, bg,
                master, moment, second, gsend, gown, grecv, qs, qr, gv, n1, n2,
                head, rew, old, dones, lengths,
                ins, fs, sent, rx, ry, rfr, rtwo, rg1, rga, rgb, rgc,
                dr, zr0, zr1, nr, wr, wd):
    z, core, x, y = (lax.axis_index(a) for a in (Z, CORE, X, Y))
    other = 1 - core
    me = z * 2 + core
    plane = x * 4 + y
    dp_peers = [{Z: ring(z, i // 2), CORE: lax.rem(core + i % 2, 2)} for i in range(1, 8)]
    mp_peers = [{X: ring(x, i // 4), Y: ring(y, i % 4)} for i in range(1, 16)]

    greet(dp_peers + mp_peers)
    loads = []

    def load(src, dst):
        loads.append(pltpu.make_async_copy(src, dst, ins.at[len(loads)]))
        loads[-1].start()
        return loads[-1]

    load_w = []
    for p in range(4):
        rows = pl.ds(4096 * p, 4096)
        load_w.append(load(w_hbm.at[rows], wk.at[rows]))
    load_f = {}
    for i, dy in enumerate((2, 1, -1, 0)):
        for w in range(2):
            rows = pl.ds(mul_of(ring(y, dy) * 128 + WAVE * w, 128), 128)
            load_f[w, dy] = pltpu.make_async_copy(feat_hbm.at[rows], feat.at[rows], fs.at[w, i])
            load_f[w, dy].start()
        if i == 0:
            load_d = load(down_hbm, down)
    small = [load(a, b) for a, b in ((head_hbm, head), (rew_hbm, rew), (old_hbm, old), (dones_hbm, dones),
                                     (lengths_hbm, lengths))]
    state = [load(a, b) for a, b in ((master_hbm, master), (moment_hbm, moment), (second_hbm, second))]

    out_row = lax.broadcasted_iota(jnp.int32, (256, 256), 0)
    in_row = lax.broadcasted_iota(jnp.int32, (256, 256), 1)
    select = jnp.where(in_row == (out_row % 32) * 8 + out_row // 32, 1.0, 0.0).astype(BF)
    for p in range(4):
        load_w[p].wait()
        for u in range(8):
            base = 4096 * p + 512 * u
            pair = jnp.concatenate([wk[base:base + 256, :], wk[base + 256:base + 512, :]], axis=1)
            moved = jnp.dot(select, pair, preferred_element_type=F32).astype(BF)
            k = 512 * p + 64 * u
            for i in range(8):
                c, g = i // 2, i % 2
                for half in range(2):
                    w4[c, k + 32 * half:k + 32 * half + 32, 128 * g:128 * (g + 1)] = \
                        moved[32 * i:32 * (i + 1), 128 * half:128 * (half + 1)]
    load_d.wait()

    def peer(first, h, delta):
        along_x = STREAMS[h][0] == first
        return {X: ring(x, delta)} if along_x else {Y: ring(y, delta)}

    def tok(w, h, da, db):
        dx, dy = (da, db) if STREAMS[h][0] else (db, da)
        return pl.ds(mul_of(WAVE * w + ring(y, dy) * 128 + ring(x, dx) * WT, WT), WT)

    def offsets(h):
        s = STREAMS[h][1]
        return (2, s, -s, 0)

    def index(h, db):
        return offsets(h).index(db)

    one, two, g1, g2 = {}, {}, {}, {}
    row_at = {2: 0, 1: 1, -1: 2, 0: 3}
    for w in range(2):
        for h in range(4):
            s = STREAMS[h][1]
            for j, db in enumerate(offsets(h)):
                relayed = rx.at[w, row_at[db]] if h < 2 else ry.at[w, h - 2]
                for kind, (da, to) in enumerate(((2, s), (s, s), (-s, -s))):
                    one[w, h, kind, j] = remote(part.at[h, tok(w, h, da, db)], rv1.at[w, h, kind, j],
                                                sent.at[0], relayed if kind == 0 else rfr.at[w, j], peer(True, h, to))
            for kind, (db, to) in enumerate(((2, s), (s, s), (-s, -s))):
                two[w, h, kind] = remote(part.at[h, tok(w, h, 0, db)], rv2.at[w, h, kind],
                                         sent.at[1], rtwo.at[w, min(kind, 1)], peer(False, h, to))
            ahead = 0 if s == 1 else 1
            for kind, (db, to) in enumerate(((0, 1), (0, -1), (-s, s))):
                t = og.at[h, tok(w, h, 0, db)]
                g1[w, h, kind] = remote(t, t, sent.at[2], rg1.at[w, {ahead: 0, 1 - ahead: 1, 2: 2}[kind]],
                                        peer(False, h, to))
            for k, db in enumerate((0, -s, s, 2)):
                for kind, (da, to) in enumerate(((0, 1), (0, -1), (-s, s))):
                    t = og.at[h, tok(w, h, da, db)]
                    if kind == ahead:
                        done = rga.at[w, k]
                    elif h < 2:
                        done = rgb.at[w, row_at[db]]
                    else:
                        done = rgc.at[w, 2 if kind == 2 else 3 - h]
                    g2[w, h, k, kind] = remote(t, t, sent.at[3], done, peer(True, h, to))

    def arrive(count, sem):
        blocks = rv1.at[0, 0, 0, pl.ds(0, count)] if count <= 4 else rv1.at[0, pl.ds(0, count // 4), 0]
        remote(blocks, blocks, sent.at[0], sem, {X: ring(x, 1)}).wait_recv()

    def chunk(dy):
        rows = []
        for w in range(2):
            load_f[w, dy].wait()
            rows.append(pl.ds(mul_of(ring(y, dy) * 128 + WAVE * w, 128), 128))
        f = jnp.concatenate([feat[r, :] for r in rows], axis=0)
        for c in range(4):
            gu = jnp.dot(f, w4[c], preferred_element_type=F32)
            gate, up = gu[:, :128], gu[:, 128:]
            value = (gate * jax.nn.sigmoid(gate) * up).astype(BF)
            hid[:, c * 128:(c + 1) * 128] = value
            for w in range(2):
                both[c, rows[w], :] = gu[128 * w:128 * (w + 1)]
        v = hid[...]
        for h in range(4):
            product = jnp.dot(v, down[:, h * 512:(h + 1) * 512], preferred_element_type=F32).astype(BF)
            for w in range(2):
                part[h, rows[w], :] = product[128 * w:128 * (w + 1)]

    def send(w, dy):
        for h in (0, 1):
            one[w, h, 0, index(h, dy)].start()
            one[w, h, 2, index(h, dy)].start()
        for h in (2, 3):
            s = STREAMS[h][1]
            if dy == 2:
                for j in range(4):
                    one[w, h, 0, j].start()
            elif dy == -s:
                for j in range(4):
                    one[w, h, 2, j].start()

    def pass_on(w, h, j):
        t = tok(w, h, STREAMS[h][1], offsets(h)[j])
        part[h, t, :] = (part[h, t, :].astype(F32) + rv1[w, h, 0, j].astype(F32)).astype(BF)
        one[w, h, 1, j].start()

    def pass_x(w, dy):
        arrive(2, rx.at[w, row_at[dy]])
        for h in (0, 1):
            pass_on(w, h, index(h, dy))

    def pass_y(w, h):
        arrive(4, ry.at[w, h - 2])
        for j in range(4):
            pass_on(w, h, j)

    def finish_one(w, h, j):
        t = tok(w, h, 0, offsets(h)[j])
        total = part[h, t, :].astype(F32) + rv1[w, h, 1, j].astype(F32) + rv1[w, h, 2, j].astype(F32)
        if j == 3:
            mix[w, :, h * 512:(h + 1) * 512] = total + rv2[w, h, 1].astype(F32) + rv2[w, h, 2].astype(F32)
            return
        if j == 1:
            total = total + rv2[w, h, 0].astype(F32)
        part[h, t, :] = total.astype(BF)
        two[w, h, j].start()

    def finish(w, j):
        arrive(8, rfr.at[w, j])
        if j == 1:
            arrive(4, rtwo.at[w, 0])
        if j == 3:
            arrive(8, rtwo.at[w, 1])
        for h in range(4):
            finish_one(w, h, j)

    def own_loss(w, targets, mask):
        mine = pl.ds(mul_of(WAVE * w + y * 128 + x * WT, WT), WT)
        stream = feat[mine, :].astype(F32) + mix[w]
        vh = head[...]
        norm = lax.rsqrt(jnp.sum(stream * stream, axis=1, keepdims=True) / D + 1e-05)
        estimate = norm * jnp.sum(stream * vh, axis=1, keepdims=True)
        errors = estimate - targets
        total_tokens = TOK * 8
        coeff = 2.0 * mask * errors / total_tokens
        inner = coeff * estimate / D
        a = norm * coeff
        b = norm * norm * inner
        for h in range(4):
            cols = slice(h * 512, (h + 1) * 512)
            og[h, mine, :] = (a * vh[:, cols] - b * stream[:, cols]).astype(BF)
        return jnp.sum(mask * errors * errors, axis=0, keepdims=True) / total_tokens

    def spread(w, k):
        for h in range(4):
            g2[w, h, k, 0].start()
            g2[w, h, k, 1].start()

    def relay(w, k):
        arrive(4, rga.at[w, k])
        for h in range(4):
            g2[w, h, k, 2].start()

    def gather_0(w):
        for h in range(4):
            g1[w, h, 0].start()
            g1[w, h, 1].start()
        spread(w, 0)

    def gather_1(w):
        arrive(4, rg1.at[w, 0])
        for h in range(4):
            g1[w, h, 2].start()
        spread(w, 1)

    def gather_2(w):
        relay(w, 0)
        arrive(4, rg1.at[w, 1])
        spread(w, 2)

    def gather_3(w):
        arrive(4, rg1.at[w, 2])
        spread(w, 3)

    def backward(w, dy):
        arrive(4, rgb.at[w, row_at[dy]])
        if dy != 0:
            arrive({-1: 4, 1: 4, 2: 8}[dy], rgc.at[w, {-1: 0, 1: 1, 2: 2}[dy]])
        rows = pl.ds(mul_of(ring(y, dy) * 128 + WAVE * w, 128), 128)
        hg = None
        for h in range(4):
            term = lax.dot_general(og[h, rows, :], down[:, h * 512:(h + 1) * 512],
                                   (((1,), (1,)), ((), ())), preferred_element_type=F32)
            hg = term if hg is None else hg + term
        for c in range(4):
            gate, up = both[c, rows, :128], both[c, rows, 128:]
            d = hg[:, c * 128:(c + 1) * 128]
            sig = jax.nn.sigmoid(gate)
            bg[rows, c * 256:c * 256 + 128] = (d * up * sig * (1.0 + gate * (1.0 - sig))).astype(BF)
            bg[rows, c * 256 + 128:(c + 1) * 256] = (d * gate * sig).astype(BF)

    chunk(2)
    greeted(dp_peers + mp_peers)
    send(0, 2)
    chunk(1)
    send(0, 1)
    chunk(-1)
    send(0, -1)
    pass_x(0, 2)
    pass_y(0, 2)
    chunk(0)
    send(0, 0)
    send(1, 2)
    pass_x(0, 1)
    pass_y(0, 3)
    pass_x(0, -1)
    send(1, 1)
    for c in small:
        c.wait()
    own = [own_targets(2 * w + y // 2, (y % 2) * 128 + x * WT, rew, old, dones, lengths) for w in range(2)]
    finish(0, 0)
    send(1, -1)
    pass_x(0, 0)
    finish(0, 1)
    send(1, 0)
    pass_x(1, 2)
    pass_y(1, 2)
    finish(0, 2)
    finish(0, 3)
    loss = own_loss(0, *own[0])
    pass_x(1, 1)
    pass_y(1, 3)
    pass_x(1, -1)
    gather_0(0)
    finish(1, 0)
    pass_x(1, 0)
    finish(1, 1)
    gather_1(0)
    finish(1, 2)
    gather_2(0)
    finish(1, 3)
    loss = loss + own_loss(1, *own[1])
    gather_0(1)
    gather_3(0)
    relay(0, 1)
    gather_1(1)
    relay(0, 2)
    relay(0, 3)
    gather_2(1)
    backward(0, 0)
    gather_3(1)
    backward(0, -1)
    relay(1, 1)
    backward(0, 1)
    relay(1, 2)
    backward(0, 2)
    relay(1, 3)
    for dy in (0, -1, 1, 2):
        backward(1, dy)

    order = (2, 1, -1, 0)
    halves = (slice(0, 512), slice(512, 1024))
    swap = [[remote(gsend.at[i, :, half], grecv.at[i, :, half], sent.at[4], dr.at[i, h], {CORE: other})
             for h, half in enumerate(halves)] for i in range(4)]

    def grad_rows(dz, c, half):
        cols = pl.ds(mul_of((ring(z, dz) * 2 + c) * ROWS, ROWS), ROWS)
        return lax.dot_general(feat[:, cols], bg[:, half], (((0,), (0,)), ((), ())), preferred_element_type=F32)

    hop = {}
    for h, s in enumerate((1, -1)):
        for kind, to in enumerate((s, s, -s)):
            for j in range(4):
                rows = pl.ds(0, 80) if j == 0 else pl.ds(16 + 64 * j, 64)
                hop[h, kind, j] = remote(qs.at[h, kind, rows], qr.at[h, kind, rows],
                                         sent.at[5], zr0.at[h, j] if kind == 0 else zr1.at[j], {Z: ring(z, to)})

    def exponent_of(bound):
        return jnp.ceil(4.0 * jnp.log2(jnp.maximum(bound, 1e-30)) + 0.02)

    def power(exponent):
        return jnp.exp(exponent * (math.log(2.0) / 4.0))

    def received(h, kind):
        exponent = qr[h, kind, 0:16, :].astype(jnp.int32).astype(F32)[0:1]
        return power(exponent)

    def head_of(h, kind, bound):
        exponent = exponent_of(bound)
        qs[h, kind, 0:16, :] = jnp.broadcast_to(exponent, (16, 512)).astype(jnp.int32).astype(jnp.int16)
        return LEVELS * power(-exponent)

    def both_cores(i, h):
        cols = slice(512 * h, 512 * (h + 1))
        size = jnp.zeros((8, 512), F32)
        for j in range(4):
            rows = slice(64 * j, 64 * (j + 1))
            t = gown[i, rows, cols] + grecv[i, rows, cols]
            gown[i, rows, cols] = t
            size = jnp.maximum(size, jnp.max(jnp.abs(t).reshape(8, 8, 512), axis=0))
        return jnp.max(size, axis=0, keepdims=True)

    def mine_of(i, h, j):
        return gown[i, 64 * j:64 * (j + 1), 512 * h:512 * (h + 1)]

    def code(value, scale):
        return jnp.round(value * scale).astype(jnp.int32).astype(jnp.int16)

    def value_of(h, kind, j, unit):
        return qr[h, kind, 16 + 64 * j:80 + 64 * j, :].astype(jnp.int32).astype(F32) * unit

    def straight(i, h, kind):
        scale = head_of(h, kind, both_cores(i, h))
        for j in range(4):
            qs[h, kind, 16 + 64 * j:80 + 64 * j, :] = code(mine_of(i, h, j), scale)
            hop[h, kind, j].start()

    def pass_sum(i, h):
        size = both_cores(i, h)
        hop[h, 0, 0].wait_recv()
        far_size = received(h, 0)
        scale = head_of(h, 1, size + far_size)
        for j in range(4):
            if j > 0:
                hop[h, 0, j].wait_recv()
            qs[h, 1, 16 + 64 * j:80 + 64 * j, :] = code(mine_of(i, h, j) + value_of(h, 0, j, far_size / LEVELS), scale)
            hop[h, 1, j].start()

    for i, dz in enumerate(order):
        for h, half in enumerate(halves):
            gsend[i, :, half] = grad_rows(dz, other, half)
            swap[i][h].start()
        if i == 1:
            for h in (0, 1):
                swap[0][h].wait_recv()
                straight(0, h, 0)
        if i == 2:
            swap[1][1].wait_recv()
            straight(1, 1, 2)
        if i == 3:
            swap[2][0].wait_recv()
            straight(2, 0, 2)
        for half in halves:
            gown[i, :, half] = grad_rows(dz, core, half)
    swap[1][0].wait_recv()
    pass_sum(1, 0)
    swap[2][1].wait_recv()
    pass_sum(2, 1)
    for h in (0, 1):
        swap[3][h].wait_recv()
    squares = jnp.zeros((8, 128), F32)
    units = {}
    for j in range(4):
        blocks = qr.at[:, pl.ds(1, 2), pl.ds(0, 80) if j == 0 else pl.ds(16 + 64 * j, 64)]
        remote(blocks, blocks, sent.at[5], zr1.at[j], {Z: ring(z, 1)}).wait_recv()
        for h in range(2):
            if j == 0:
                units[h] = [received(h, kind) / LEVELS for kind in (1, 2)]
            owned = gown[3, 64 * j:64 * (j + 1), 512 * h:512 * (h + 1)] + grecv[3, 64 * j:64 * (j + 1), 512 * h:512 * (h + 1)]
            g = owned + value_of(h, 1, j, units[h][0]) + value_of(h, 2, j, units[h][1])
            for c in range(4):
                piece = g[:, c * 128:(c + 1) * 128]
                gv[pl.ds(64 * j * 8 + 4 * h + c, 64, stride=8), :] = piece
                squares = squares + jnp.sum((piece * piece).reshape(8, 8, 128), axis=0)

    n1[me, 0:8, :] = squares
    n1[me, 8:16, :] = jnp.broadcast_to(loss, (8, 128))
    near = [remote(n1.at[me], n1.at[me], sent.at[6], nr.at[0], p) for p in dp_peers]
    for c in near:
        c.start()
    seven, fifteen = n1.at[pl.ds(0, 7)], n2.at[pl.ds(0, 15)]
    remote(seven, seven, sent.at[6], nr.at[0], dp_peers[0]).wait_recv()
    sums = n1[0]
    for i in range(1, 8):
        sums = sums + n1[i]
    n2[plane] = sums
    far = [remote(n2.at[plane], n2.at[plane], sent.at[7], nr.at[1], p) for p in mp_peers]
    for c in far:
        c.start()
    remote(fifteen, fifteen, sent.at[7], nr.at[1], mp_peers[0]).wait_recv()
    sums = n2[0]
    for i in range(1, 16):
        sums = sums + n2[i]
    sums_out[...] = sums
    squared = jnp.sum(jnp.sum(sums[0:8], axis=1, keepdims=True), axis=0, keepdims=True)
    clip = jnp.minimum(1.0, MAX_NORM / (jnp.sqrt(squared) + 1e-06))

    def place(device, q):
        return pl.ds(mul_of(device * 2048 + q * 256, 256), 256)

    def block(device, q):
        return wk.at[place(device, q)]

    spread_dp = {}
    for q in range(8):
        s = 1 if q % 2 == 0 else -1
        src = {0: (me, {Z: ring(z, 1)}), 1: (me, {Z: ring(z, -1)}),
               2: (ring(z, -s) * 2 + core, {Z: ring(z, s)}),
               3: (me, {CORE: other}), 4: (ring(z, -1) * 2 + core, {CORE: other}),
               5: (ring(z, 1) * 2 + core, {CORE: other}), 6: (ring(z, 2) * 2 + core, {CORE: other})}
        for kind, (device, to) in src.items():
            b = block(device, q)
            spread_dp[q, kind] = remote(b, b, sent.at[8], wr.at[q, kind] if kind < 3 else wd.at[0], to)
    for c in state:
        c.wait()
    for q in range(8):
        rows = pl.ds(256 * q, 256)
        g = gv[rows, :] * clip
        new, m, v = updated(g, master[rows, :], moment[rows, :], second[rows, :])
        mo[rows, :] = new
        vo[rows, :] = m
        so[rows, :] = v
        wk[place(me, q), :] = new.astype(BF)
        for kind in (0, 1, 3):
            spread_dp[q, kind].start()
    for q in range(8):
        with_relay, against = (0, 1) if q % 2 == 0 else (1, 0)
        spread_dp[q, with_relay].wait_recv()
        spread_dp[q, 2].start()
        spread_dp[q, 4 + with_relay].start()
        spread_dp[q, against].wait_recv()
        spread_dp[q, 4 + against].start()
    for q in range(8):
        spread_dp[q, 2].wait_recv()
        spread_dp[q, 6].start()
    four, all_but_one = wk.at[pl.ds(0, 4 * 2048)], wk.at[pl.ds(0, 7 * 2048)]
    remote(four, four, sent.at[8], wd.at[0], {CORE: other}).wait_recv()
    for i, (ref, device) in enumerate(((rv1, {X: ring(x, 1)}), (rv2, {X: ring(x, 1)}), (rv2, {X: ring(x, 1)}),
                                       (rv1, {X: ring(x, 1)}), (gsend, {CORE: other}), (qs, {Z: ring(z, 1)}),
                                       (seven, dp_peers[0]), (fifteen, mp_peers[0]), (all_but_one, {CORE: other}))):
        remote(ref, ref, sent.at[i], nr.at[0], device).wait_send()


def tail_kernel(work, master, moment, second, sums, work_out, master_out, moment_out, second_out, loss, sems):
    copies = [pltpu.make_async_copy(a, b, sems.at[i]) for i, (a, b) in enumerate((
        (work, work_out), (master, master_out), (moment, moment_out), (second, second_out)))]
    for c in copies:
        c.start()
    loss[...] = sums[8:9, 0:1]
    for c in copies:
        c.wait()


def updated(g, old, moment, second):
    m = 0.9 * moment + 0.1 * g
    v = 0.999 * second + 0.001 * g * g
    first_hat = m * (1.0 / (1.0 - 0.9 ** 10))
    second_hat = v * (1.0 / (1.0 - 0.999 ** 10))
    return old - 0.001 * (first_hat / (jnp.sqrt(second_hat) + 1e-08) + 0.1 * old), m, v


def rows_of(value):
    r = value.shape[0]
    return value.reshape(r, 2, 4, 128).transpose(0, 2, 1, 3).reshape(r * 8, 128)


def from_rows(value):
    r = value.shape[0] // 8
    return value.reshape(r, 4, 2, 128).transpose(0, 2, 1, 3).reshape(r, 2, 512)


def per_device(features, rewards, old_values, dones, lengths, proj_weights, down_weight, value_head,
               master, moment, second):
    dma = pltpu.SemaphoreType.DMA
    vm = pl.BlockSpec(memory_space=pltpu.VMEM)
    sm = pl.BlockSpec(memory_space=pltpu.SMEM)
    hbm = pl.BlockSpec(memory_space=pl.ANY)
    state = (rows_of(master), rows_of(moment), rows_of(second))
    rows = jax.ShapeDtypeStruct((8 * ROWS, 128), F32)
    row_scratch = pltpu.VMEM((8 * ROWS, 128), F32)
    block_scratch = pltpu.VMEM((4, ROWS, 1024), F32)
    link_scratch = pltpu.VMEM((2, 3, 16 + ROWS, 512), jnp.int16)
    results = pl.pallas_call(
        step_kernel,
        name="critic_step",
        out_shape=(pltpu.VMEM((8 * D, 128), BF), row_scratch, row_scratch, row_scratch,
                   pltpu.VMEM((16, 128), F32)),
        in_specs=[hbm] * 11,
        out_specs=(vm, vm, vm, vm, vm),
        scratch_shapes=[
            pltpu.VMEM((TOK, D), BF), pltpu.VMEM((4, D, 256), BF), pltpu.VMEM((FFL, D), BF),
            pltpu.VMEM((4, TOK, 256), F32), pltpu.VMEM((256, FFL), BF), pltpu.VMEM((4, TOK, 512), BF),
            pltpu.VMEM((2, 4, 3, 4, WT, 512), BF), pltpu.VMEM((2, 4, 3, WT, 512), BF), pltpu.VMEM((4, TOK, 512), BF),
            pltpu.VMEM((2, WT, D), F32), pltpu.VMEM((TOK, 2 * FFL), BF),
            row_scratch, row_scratch, row_scratch, block_scratch, block_scratch, block_scratch,
            link_scratch, link_scratch, row_scratch,
            pltpu.VMEM((8, 16, 128), F32), pltpu.VMEM((16, 16, 128), F32),
            pltpu.VMEM((1, D), F32), pltpu.VMEM((4, 256), F32), pltpu.VMEM((4, 256), F32),
            pltpu.VMEM((4, 256), jnp.int32), pltpu.SMEM((4,), jnp.int32),
            dma((13,)), dma((2, 4)), dma((9,)),
            dma((2, 4)), dma((2, 2)), dma((2, 4)), dma((2, 2)),
            dma((2, 3)), dma((2, 4)), dma((2, 4)), dma((2, 3)),
            dma((4, 2)), dma((2, 4)), dma((4,)), dma((2,)), dma((8, 3)), dma((1,)),
        ],
        compiler_params=pltpu.CompilerParams(collective_id=0, has_side_effects=True, vmem_limit_bytes=VMEM_LIMIT),
    )(features, rows_of(proj_weights), down_weight, *state, value_head.reshape(1, D), rewards, old_values, dones, lengths)
    work, master_new, moment_new, second_new, loss = pl.pallas_call(
        tail_kernel,
        name="results",
        out_shape=(jax.ShapeDtypeStruct((8 * D, 128), BF), rows, rows, rows, jax.ShapeDtypeStruct((1, 1), F32)),
        in_specs=[vm] * 5,
        out_specs=(hbm, hbm, hbm, hbm, vm),
        scratch_shapes=[dma((4,))],
        compiler_params=pltpu.CompilerParams(vmem_limit_bytes=4 * 1024 * 1024),
    )(*(pltpu.with_memory_space_constraint(r, pltpu.VMEM) for r in results))
    return (from_rows(master_new), from_rows(moment_new), from_rows(second_new), from_rows(work), loss.reshape(()))


def solution(mesh):
    finer = Mesh(mesh.devices.reshape(4, 2, 4, 4), (Z, CORE, X, Y))
    return jax.shard_map(
        per_device,
        mesh=finer,
        in_specs=(
            P(DP, None), P(DP, None), P(DP, None), P(DP, None), P(DP),
            P(None, None, MP), P(MP, None), P(),
            P(DP, None, MP), P(DP, None, MP), P(DP, None, MP),
        ),
        out_specs=(P(DP, None, MP), P(DP, None, MP), P(DP, None, MP), P(None, None, MP), P()),
        check_vma=False,
    )
```

```python
import math

import jax
import jax.numpy as jnp
from jax import lax
from jax.experimental import pallas as pl
from jax.experimental.pallas import tpu as pltpu
from jax.sharding import Mesh
from jax.sharding import PartitionSpec as P

Z, CORE, X, Y = "dp_0", "dp_1", "mp_0", "mp_1"
DP = (Z, CORE)
MP = (X, Y)
GAMMA = 0.99
LAMBDA = 0.95
MAX_NORM = 0.05
D = 2048
TOK = 1024
FFL = 512
ROWS = 256
BF = jnp.bfloat16
LEVELS = 32000.0
F32 = jnp.float32
VMEM_LIMIT = 54 * 1024 * 1024


def mul_of(v, n):
    return pl.multiple_of(v, n)


def ring(v, d):
    return lax.rem(v + (d + 4), 4)


def remote(src, dst, send, recv, device):
    return pltpu.make_async_remote_copy(
        src_ref=src, dst_ref=dst, send_sem=send, recv_sem=recv,
        device_id=device, device_id_type=pl.DeviceIdType.MESH,
    )


def greet(devices):
    barrier = pltpu.get_barrier_semaphore()
    for device in devices:
        pl.semaphore_signal(barrier, inc=1, device_id=device, device_id_type=pl.DeviceIdType.MESH)


def greeted(devices):
    pl.semaphore_wait(pltpu.get_barrier_semaphore(), len(devices))


def own_targets(row, start, rew, old, dones, lengths):
    dn = jnp.broadcast_to(dones[pl.ds(row, 1), :].astype(F32), (8, 256))
    ov = jnp.broadcast_to(old[pl.ds(row, 1), :], (8, 256))
    rw = jnp.broadcast_to(rew[pl.ds(row, 1), :], (8, 256))
    lane = lax.broadcasted_iota(jnp.int32, (8, 256), 1)
    following = jnp.where(lane == 255, 0.0, pltpu.roll(ov, 255, axis=1))
    deltas = (rw + GAMMA * following * (1.0 - dn) - ov)[0:1]
    before = lax.broadcasted_iota(jnp.int32, (256, 256), 0) < lax.broadcasted_iota(jnp.int32, (256, 256), 1)
    counted_s = jnp.dot(dn.astype(BF), before.astype(F32).astype(BF), preferred_element_type=F32)[0:1]
    t = start + lax.broadcasted_iota(jnp.int32, (WT, 256), 0)
    s = lax.broadcasted_iota(jnp.int32, (WT, 256), 1)
    counted_t = jnp.sum(jnp.where(s < t, dn[0:1], 0.0), axis=1, keepdims=True)
    linked = (counted_t == counted_s) & (s >= t)
    powers = jnp.exp(jnp.maximum(s - t, 0).astype(F32) * math.log(GAMMA * LAMBDA))
    advantage = jnp.sum(jnp.where(linked, powers, 0.0) * deltas, axis=1, keepdims=True)
    own_old = jnp.sum(jnp.where(s == t, ov[0:1], 0.0), axis=1, keepdims=True)
    mask = jnp.where(t[:, 0:1] < lengths[row], 1.0, 0.0)
    return advantage + own_old, mask


STREAMS = ((True, 1), (True, -1), (False, 1), (False, -1))
WT = 32
WAVE = 512
ORDER = (
    ("C", 2), ("S", 0, 2, 1), ("S", 0, 2, 0), ("S", 1, 2, 1), ("C", 1), ("S", 0, 1, 0), ("C", -1),
    ("S", 0, -1, 0), ("C", 0), ("PX", 0, 2), ("S", 0, 0, 0), ("S", 1, 2, 0), ("S", 1, 1, 1), ("S", 1, -1, 1),
    ("S", 1, -1, 0), ("S", 1, 1, 0), ("PX", 0, 1), ("S", 0, -1, 1), ("S", 0, 1, 1), ("S", 1, 0, 0),
    ("PY", 0, 2), ("PY", 0, 3), ("PX", 0, -1), ("FN", 0, 0, 0), ("PY", 1, 2), ("PX", 0, 0), ("PY", 1, 3),
    ("PX", 1, 2), ("PX", 1, -1), ("PX", 1, 1), ("FN", 0, 0, 1), ("PX", 1, 0), ("FN", 0, 2, 1),
    ("FN", 0, 2, 0), ("FN", 0, 1, 0), ("FN", 1, 0, 0), ("FN", 1, 0, 1), ("FN", 1, 2, 0), ("FN", 1, 2, 1),
    ("FN", 0, 1, 1), ("FN", 0, 3, 0), ("FN", 1, 1, 1), ("FN", 1, 1, 0), ("FN", 0, 3, 1), ("L", 0),
    ("G0", 0, 1), ("G0", 0, 0), ("G0b", 0, 0), ("G0b", 0, 1), ("FN", 1, 3, 1), ("FN", 1, 3, 0), ("L", 1),
    ("G0", 1, 0), ("G0", 1, 1), ("G0b", 1, 0), ("G0b", 1, 1), ("G2", 0, 1), ("G1", 0, 1), ("G1", 0, 0),
    ("G2", 0, 0), ("R", 0, 0, 0), ("R", 0, 0, 1), ("G2", 1, 1), ("G2", 1, 0), ("G1", 1, 0), ("G1", 1, 1),
    ("R", 1, 0, 0), ("R", 1, 0, 1), ("G3", 0, 1), ("R", 0, 2, 1), ("R", 0, 1, 0), ("R", 0, 1, 1),
    ("R", 0, 2, 0), ("G3", 0, 0), ("B", 0, 0), ("R", 1, 2, 0), ("R", 1, 2, 1), ("G3", 1, 0), ("R", 1, 1, 0),
    ("G3", 1, 1), ("R", 1, 1, 1), ("B", 1, 0), ("R", 0, 3, 1), ("B", 0, 1), ("B", 0, -1), ("R", 0, 3, 0),
    ("R", 1, 3, 0), ("R", 1, 3, 1), ("B", 1, -1), ("B", 1, 1), ("B", 0, 2), ("B", 1, 2),
)


def step_kernel(feat_hbm, w_hbm, down_hbm, master_hbm, moment_hbm, second_hbm,
                head_hbm, rew_hbm, old_hbm, dones_hbm, lengths_hbm,
                wk, mo, vo, so, sums_out,
                feat, w4, down, both, hid, part, rv1, rv2, og, mix, bg,
                master, moment, second, gsend, gown, grecv, qs, qr, gv, n1, n2,
                head, rew, old, dones, lengths,
                ins, fs, sent, rx, ry, rfr, rtwo, rg1, rga, rgb, rgc,
                dr, zr0, zr1, nr, wr, wd):
    z, core, x, y = (lax.axis_index(a) for a in (Z, CORE, X, Y))
    other = 1 - core
    me = z * 2 + core
    plane = x * 4 + y
    dp_peers = [{Z: ring(z, i // 2), CORE: lax.rem(core + i % 2, 2)} for i in range(1, 8)]
    mp_peers = [{X: ring(x, i // 4), Y: ring(y, i % 4)} for i in range(1, 16)]

    greet(dp_peers + mp_peers)
    loads = []

    def load(src, dst):
        loads.append(pltpu.make_async_copy(src, dst, ins.at[len(loads)]))
        loads[-1].start()
        return loads[-1]

    load_w = []
    for p in range(4):
        rows = pl.ds(4096 * p, 4096)
        load_w.append(load(w_hbm.at[rows], wk.at[rows]))
    load_f = {}
    for i, dy in enumerate((2, 1, -1, 0)):
        for w in range(2):
            rows = pl.ds(mul_of(ring(y, dy) * 128 + WAVE * w, 128), 128)
            load_f[w, dy] = pltpu.make_async_copy(feat_hbm.at[rows], feat.at[rows], fs.at[w, i])
    load_f[0, 2].start()
    load_f[1, 2].start()
    load_d = load(down_hbm, down)
    small, state = [], []

    out_row = lax.broadcasted_iota(jnp.int32, (256, 256), 0)
    in_row = lax.broadcasted_iota(jnp.int32, (256, 256), 1)
    select = jnp.where(in_row == (out_row % 32) * 8 + out_row // 32, 1.0, 0.0).astype(BF)
    for p in range(4):
        load_w[p].wait()
        if p == 2:
            for dy in (1, -1, 0):
                load_f[0, dy].start()
                load_f[1, dy].start()
        for u in range(8):
            base = 4096 * p + 512 * u
            pair = jnp.concatenate([wk[base:base + 256, :], wk[base + 256:base + 512, :]], axis=1)
            moved = jnp.dot(select, pair, preferred_element_type=F32).astype(BF)
            k = 512 * p + 64 * u
            for i in range(8):
                c, g = i // 2, i % 2
                for half in range(2):
                    w4[c, k + 32 * half:k + 32 * half + 32, 128 * g:128 * (g + 1)] = \
                        moved[32 * i:32 * (i + 1), 128 * half:128 * (half + 1)]
    load_d.wait()

    def peer(first, h, delta):
        along_x = STREAMS[h][0] == first
        return {X: ring(x, delta)} if along_x else {Y: ring(y, delta)}

    def tok(w, h, da, db):
        dx, dy = (da, db) if STREAMS[h][0] else (db, da)
        return pl.ds(mul_of(WAVE * w + ring(y, dy) * 128 + ring(x, dx) * WT, WT), WT)

    def offsets(h):
        s = STREAMS[h][1]
        return (2, s, -s, 0)

    def index(h, db):
        return offsets(h).index(db)

    one, two, g1, g2 = {}, {}, {}, {}
    row_at = {2: 0, 1: 1, -1: 2, 0: 3}
    for w in range(2):
        for h in range(4):
            s = STREAMS[h][1]
            for j, db in enumerate(offsets(h)):
                relayed = rx.at[w, row_at[db]] if h < 2 else ry.at[w, h - 2]
                for kind, (da, to) in enumerate(((2, s), (s, s), (-s, -s))):
                    one[w, h, kind, j] = remote(part.at[h, tok(w, h, da, db)], rv1.at[w, h, kind, j],
                                                sent.at[0], relayed if kind == 0 else rfr.at[w, j, h // 2],
                                                peer(True, h, to))
            for kind, (db, to) in enumerate(((2, s), (s, s), (-s, -s))):
                two[w, h, kind] = remote(part.at[h, tok(w, h, 0, db)], rv2.at[w, h, kind],
                                         sent.at[1], rtwo.at[w, min(kind, 1), h // 2], peer(False, h, to))
            ahead = 0 if s == 1 else 1
            for kind, (db, to) in enumerate(((0, 1), (0, -1), (-s, s))):
                t = og.at[h, tok(w, h, 0, db)]
                g1[w, h, kind] = remote(t, t, sent.at[2], rg1.at[w, {ahead: 0, 1 - ahead: 1, 2: 2}[kind], h // 2],
                                        peer(False, h, to))
            for k, db in enumerate((0, -s, s, 2)):
                for kind, (da, to) in enumerate(((0, 1), (0, -1), (-s, s))):
                    t = og.at[h, tok(w, h, da, db)]
                    if kind == ahead:
                        done = rga.at[w, k, h // 2]
                    elif h < 2:
                        done = rgb.at[w, row_at[db]]
                    else:
                        done = rgc.at[w, 2 if kind == 2 else 3 - h]
                    g2[w, h, k, kind] = remote(t, t, sent.at[3], done, peer(True, h, to))

    def arrive(count, sem):
        blocks = rv1.at[0, 0, 0, pl.ds(0, count)] if count <= 4 else rv1.at[0, pl.ds(0, count // 4), 0]
        remote(blocks, blocks, sent.at[0], sem, {X: ring(x, 1)}).wait_recv()

    def chunk(dy):
        rows = []
        for w in range(2):
            load_f[w, dy].wait()
            rows.append(pl.ds(mul_of(ring(y, dy) * 128 + WAVE * w, 128), 128))
        f = jnp.concatenate([feat[r, :] for r in rows], axis=0)
        for c in range(4):
            gu = jnp.dot(f, w4[c], preferred_element_type=F32)
            gate, up = gu[:, :128], gu[:, 128:]
            value = (gate * jax.nn.sigmoid(gate) * up).astype(BF)
            hid[:, c * 128:(c + 1) * 128] = value
            for w in range(2):
                both[c, rows[w], :] = gu[128 * w:128 * (w + 1)]
        v = hid[...]
        for h in range(4):
            product = jnp.dot(v, down[:, h * 512:(h + 1) * 512], preferred_element_type=F32).astype(BF)
            for w in range(2):
                part[h, rows[w], :] = product[128 * w:128 * (w + 1)]

    def send(w, dy, q):
        if q == 0:
            for kind in (0, 2):
                for h in (0, 1):
                    one[w, h, kind, index(h, dy)].start()
            return
        for j in range(4):
            for h in (2, 3):
                if dy == 2:
                    one[w, h, 0, j].start()
                elif dy == -STREAMS[h][1]:
                    one[w, h, 2, j].start()

    def pass_on(w, h, j):
        t = tok(w, h, STREAMS[h][1], offsets(h)[j])
        part[h, t, :] = (part[h, t, :].astype(F32) + rv1[w, h, 0, j].astype(F32)).astype(BF)
        one[w, h, 1, j].start()

    def pass_x(w, dy):
        arrive(2, rx.at[w, row_at[dy]])
        for h in (0, 1):
            pass_on(w, h, index(h, dy))

    def pass_y(w, h):
        arrive(4, ry.at[w, h - 2])
        for j in range(4):
            pass_on(w, h, j)

    def finish_one(w, h, j):
        t = tok(w, h, 0, offsets(h)[j])
        total = part[h, t, :].astype(F32) + rv1[w, h, 1, j].astype(F32) + rv1[w, h, 2, j].astype(F32)
        if j == 3:
            mix[w, :, h * 512:(h + 1) * 512] = total + rv2[w, h, 1].astype(F32) + rv2[w, h, 2].astype(F32)
            return
        if j == 1:
            total = total + rv2[w, h, 0].astype(F32)
        part[h, t, :] = total.astype(BF)
        two[w, h, j].start()

    def finish(w, j, q):
        arrive(4, rfr.at[w, j, q])
        if j == 1:
            arrive(2, rtwo.at[w, 0, q])
        if j == 3:
            arrive(4, rtwo.at[w, 1, q])
        for h in (2 * q, 2 * q + 1):
            finish_one(w, h, j)

    def own_loss(w, targets, mask):
        mine = pl.ds(mul_of(WAVE * w + y * 128 + x * WT, WT), WT)
        stream = feat[mine, :].astype(F32) + mix[w]
        vh = head[...]
        norm = lax.rsqrt(jnp.sum(stream * stream, axis=1, keepdims=True) / D + 1e-05)
        estimate = norm * jnp.sum(stream * vh, axis=1, keepdims=True)
        errors = estimate - targets
        total_tokens = TOK * 8
        coeff = 2.0 * mask * errors / total_tokens
        inner = coeff * estimate / D
        a = norm * coeff
        b = norm * norm * inner
        for h in range(4):
            cols = slice(h * 512, (h + 1) * 512)
            og[h, mine, :] = (a * vh[:, cols] - b * stream[:, cols]).astype(BF)
        return jnp.sum(mask * errors * errors, axis=0, keepdims=True) / total_tokens

    def spread(w, k, q):
        for kind in (0, 1):
            for h in (2 * q, 2 * q + 1):
                g2[w, h, k, kind].start()

    def relay(w, k, q):
        arrive(2, rga.at[w, k, q])
        for h in (2 * q, 2 * q + 1):
            g2[w, h, k, 2].start()

    def gather_0(w, q):
        for kind in (0, 1):
            for h in (2 * q, 2 * q + 1):
                g1[w, h, kind].start()

    def gather_1(w, q):
        arrive(2, rg1.at[w, 0, q])
        for h in (2 * q, 2 * q + 1):
            g1[w, h, 2].start()
        spread(w, 1, q)

    def gather_2(w, q):
        arrive(2, rg1.at[w, 1, q])
        spread(w, 2, q)

    def gather_3(w, q):
        arrive(2, rg1.at[w, 2, q])
        spread(w, 3, q)

    def backward(w, dy):
        arrive(4, rgb.at[w, row_at[dy]])
        if dy != 0:
            arrive({-1: 4, 1: 4, 2: 8}[dy], rgc.at[w, {-1: 0, 1: 1, 2: 2}[dy]])
        rows = pl.ds(mul_of(ring(y, dy) * 128 + WAVE * w, 128), 128)
        hg = None
        for h in range(4):
            term = lax.dot_general(og[h, rows, :], down[:, h * 512:(h + 1) * 512],
                                   (((1,), (1,)), ((), ())), preferred_element_type=F32)
            hg = term if hg is None else hg + term
        for c in range(4):
            gate, up = both[c, rows, :128], both[c, rows, 128:]
            d = hg[:, c * 128:(c + 1) * 128]
            sig = jax.nn.sigmoid(gate)
            bg[rows, c * 256:c * 256 + 128] = (d * up * sig * (1.0 + gate * (1.0 - sig))).astype(BF)
            bg[rows, c * 256 + 128:(c + 1) * 256] = (d * gate * sig).astype(BF)

    own, losses = [], []

    def loss_of(w):
        losses.append(own_loss(w, *own[w]))

    steps = {"C": chunk, "S": send, "PX": pass_x, "PY": pass_y, "FN": finish, "L": loss_of, "G0": gather_0,
             "G0b": lambda w, q: spread(w, 0, q), "G1": gather_1, "G2": gather_2, "G3": gather_3, "R": relay, "B": backward}
    for at, (name, *args) in enumerate(ORDER):
        if name == "FN" and not own:
            for c in small:
                c.wait()
            own.extend(own_targets(2 * w + y // 2, (y % 2) * 128 + x * WT, rew, old, dones, lengths) for w in range(2))
        steps[name](*args)
        if at == 0:
            greeted(dp_peers + mp_peers)
            small.extend(load(a, b) for a, b in ((head_hbm, head), (rew_hbm, rew), (old_hbm, old), (dones_hbm, dones),
                                                 (lengths_hbm, lengths)))
            state.extend(load(a, b) for a, b in ((master_hbm, master), (moment_hbm, moment), (second_hbm, second)))
    loss = losses[0] + losses[1]

    order = (2, 1, -1, 0)
    halves = (slice(0, 512), slice(512, 1024))
    swap = [[remote(gsend.at[i, :, half], grecv.at[i, :, half], sent.at[4], dr.at[i, h], {CORE: other})
             for h, half in enumerate(halves)] for i in range(4)]

    def grad_rows(dz, c, half):
        cols = pl.ds(mul_of((ring(z, dz) * 2 + c) * ROWS, ROWS), ROWS)
        return lax.dot_general(feat[:, cols], bg[:, half], (((0,), (0,)), ((), ())), preferred_element_type=F32)

    hop = {}
    for h, s in enumerate((1, -1)):
        for kind, to in enumerate((s, s, -s)):
            for j in range(4):
                rows = pl.ds(0, 80) if j == 0 else pl.ds(16 + 64 * j, 64)
                hop[h, kind, j] = remote(qs.at[h, kind, rows], qr.at[h, kind, rows],
                                         sent.at[5], zr0.at[h, j] if kind == 0 else zr1.at[j], {Z: ring(z, to)})

    def exponent_of(bound):
        return jnp.ceil(4.0 * jnp.log2(jnp.maximum(bound, 1e-30)) + 0.02)

    def power(exponent):
        return jnp.exp(exponent * (math.log(2.0) / 4.0))

    def received(h, kind):
        exponent = qr[h, kind, 0:16, :].astype(jnp.int32).astype(F32)[0:1]
        return power(exponent)

    def head_of(h, kind, bound):
        exponent = exponent_of(bound)
        qs[h, kind, 0:16, :] = jnp.broadcast_to(exponent, (16, 512)).astype(jnp.int32).astype(jnp.int16)
        return LEVELS * power(-exponent)

    def both_cores(i, h):
        cols = slice(512 * h, 512 * (h + 1))
        size = jnp.zeros((8, 512), F32)
        for j in range(4):
            rows = slice(64 * j, 64 * (j + 1))
            t = gown[i, rows, cols] + grecv[i, rows, cols]
            gown[i, rows, cols] = t
            size = jnp.maximum(size, jnp.max(jnp.abs(t).reshape(8, 8, 512), axis=0))
        return jnp.max(size, axis=0, keepdims=True)

    def mine_of(i, h, j):
        return gown[i, 64 * j:64 * (j + 1), 512 * h:512 * (h + 1)]

    def code(value, scale):
        return jnp.round(value * scale).astype(jnp.int32).astype(jnp.int16)

    def value_of(h, kind, j, unit):
        return qr[h, kind, 16 + 64 * j:80 + 64 * j, :].astype(jnp.int32).astype(F32) * unit

    def straight(i, h, kind):
        scale = head_of(h, kind, both_cores(i, h))
        for j in range(4):
            qs[h, kind, 16 + 64 * j:80 + 64 * j, :] = code(mine_of(i, h, j), scale)
            hop[h, kind, j].start()

    def pass_sum(i, h):
        size = both_cores(i, h)
        hop[h, 0, 0].wait_recv()
        far_size = received(h, 0)
        scale = head_of(h, 1, size + far_size)
        for j in range(4):
            if j > 0:
                hop[h, 0, j].wait_recv()
            qs[h, 1, 16 + 64 * j:80 + 64 * j, :] = code(mine_of(i, h, j) + value_of(h, 0, j, far_size / LEVELS), scale)
            hop[h, 1, j].start()

    for i, dz in enumerate(order):
        for h, half in enumerate(halves):
            gsend[i, :, half] = grad_rows(dz, other, half)
            swap[i][h].start()
        if i == 1:
            for h in (0, 1):
                swap[0][h].wait_recv()
                straight(0, h, 0)
        if i == 2:
            swap[1][1].wait_recv()
            straight(1, 1, 2)
        if i == 3:
            swap[2][0].wait_recv()
            straight(2, 0, 2)
        for half in halves:
            gown[i, :, half] = grad_rows(dz, core, half)
    swap[1][0].wait_recv()
    pass_sum(1, 0)
    swap[2][1].wait_recv()
    pass_sum(2, 1)
    for h in (0, 1):
        swap[3][h].wait_recv()
    squares = jnp.zeros((8, 128), F32)
    units = {}
    for j in range(4):
        blocks = qr.at[:, pl.ds(1, 2), pl.ds(0, 80) if j == 0 else pl.ds(16 + 64 * j, 64)]
        remote(blocks, blocks, sent.at[5], zr1.at[j], {Z: ring(z, 1)}).wait_recv()
        for h in range(2):
            if j == 0:
                units[h] = [received(h, kind) / LEVELS for kind in (1, 2)]
            owned = gown[3, 64 * j:64 * (j + 1), 512 * h:512 * (h + 1)] + grecv[3, 64 * j:64 * (j + 1), 512 * h:512 * (h + 1)]
            g = owned + value_of(h, 1, j, units[h][0]) + value_of(h, 2, j, units[h][1])
            for c in range(4):
                piece = g[:, c * 128:(c + 1) * 128]
                gv[pl.ds(64 * j * 8 + 4 * h + c, 64, stride=8), :] = piece
                squares = squares + jnp.sum((piece * piece).reshape(8, 8, 128), axis=0)

    line = lax.broadcasted_iota(jnp.int32, (8, 128), 0)
    n1[me] = jnp.where(line == 0, jnp.sum(squares, axis=0, keepdims=True), jnp.where(line == 1, loss, 0.0))
    near = [remote(n1.at[me], n1.at[me], sent.at[6], nr.at[0], p) for p in dp_peers]
    for c in near:
        c.start()
    seven, fifteen = n1.at[pl.ds(0, 7)], n2.at[pl.ds(0, 15)]
    remote(seven, seven, sent.at[6], nr.at[0], dp_peers[0]).wait_recv()
    sums = n1[0]
    for i in range(1, 8):
        sums = sums + n1[i]
    n2[plane] = sums
    far = [remote(n2.at[plane], n2.at[plane], sent.at[7], nr.at[1], p) for p in mp_peers]
    for c in far:
        c.start()
    remote(fifteen, fifteen, sent.at[7], nr.at[1], mp_peers[0]).wait_recv()
    sums = n2[0]
    for i in range(1, 16):
        sums = sums + n2[i]
    sums_out[...] = sums
    squared = jnp.sum(sums[0:1], axis=1, keepdims=True)
    clip = jnp.minimum(1.0, MAX_NORM / (jnp.sqrt(squared) + 1e-06))

    def place(device, q):
        return pl.ds(mul_of(device * 2048 + q * 256, 256), 256)

    def block(device, q):
        return wk.at[place(device, q)]

    spread_dp = {}
    for q in range(8):
        s = 1 if q % 2 == 0 else -1
        src = {0: (me, {Z: ring(z, 1)}), 1: (me, {Z: ring(z, -1)}),
               2: (ring(z, -s) * 2 + core, {Z: ring(z, s)}),
               3: (me, {CORE: other}), 4: (ring(z, -1) * 2 + core, {CORE: other}),
               5: (ring(z, 1) * 2 + core, {CORE: other}), 6: (ring(z, 2) * 2 + core, {CORE: other})}
        for kind, (device, to) in src.items():
            b = block(device, q)
            spread_dp[q, kind] = remote(b, b, sent.at[8], wr.at[q, kind] if kind < 3 else wd.at[0], to)
    for c in state:
        c.wait()
    for q in range(8):
        rows = pl.ds(256 * q, 256)
        g = gv[rows, :] * clip
        new, m, v = updated(g, master[rows, :], moment[rows, :], second[rows, :])
        mo[rows, :] = new
        vo[rows, :] = m
        so[rows, :] = v
        wk[place(me, q), :] = new.astype(BF)
        for kind in (0, 1, 3):
            spread_dp[q, kind].start()
    for q in range(8):
        with_relay, against = (0, 1) if q % 2 == 0 else (1, 0)
        spread_dp[q, with_relay].wait_recv()
        spread_dp[q, 2].start()
        spread_dp[q, 4 + with_relay].start()
        spread_dp[q, against].wait_recv()
        spread_dp[q, 4 + against].start()
    for q in range(8):
        spread_dp[q, 2].wait_recv()
        spread_dp[q, 6].start()
    four, all_but_one = wk.at[pl.ds(0, 4 * 2048)], wk.at[pl.ds(0, 7 * 2048)]
    remote(four, four, sent.at[8], wd.at[0], {CORE: other}).wait_recv()
    for i, (ref, device) in enumerate(((rv1, {X: ring(x, 1)}), (rv2, {X: ring(x, 1)}), (rv2, {X: ring(x, 1)}),
                                       (rv1, {X: ring(x, 1)}), (gsend, {CORE: other}), (qs, {Z: ring(z, 1)}),
                                       (seven, dp_peers[0]), (fifteen, mp_peers[0]), (all_but_one, {CORE: other}))):
        remote(ref, ref, sent.at[i], nr.at[0], device).wait_send()


def tail_kernel(work, master, moment, second, sums, work_out, master_out, moment_out, second_out, loss, sems):
    pieces = [(work.at[pl.ds(2048 * i, 2048)], work_out.at[pl.ds(2048 * i, 2048)]) for i in range(8)]
    pieces += [(master, master_out), (moment, moment_out), (second, second_out)]
    copies = [pltpu.make_async_copy(a, b, sems.at[i]) for i, (a, b) in enumerate(pieces)]
    for c in copies:
        c.start()
    loss[...] = sums[1:2, 0:1]
    for c in copies:
        c.wait()


def updated(g, old, moment, second):
    m = 0.9 * moment + 0.1 * g
    v = 0.999 * second + 0.001 * g * g
    first_hat = m * (1.0 / (1.0 - 0.9 ** 10))
    second_hat = v * (1.0 / (1.0 - 0.999 ** 10))
    return old - 0.001 * (first_hat / (jnp.sqrt(second_hat) + 1e-08) + 0.1 * old), m, v


def rows_of(value):
    r = value.shape[0]
    return value.reshape(r, 2, 4, 128).transpose(0, 2, 1, 3).reshape(r * 8, 128)


def from_rows(value):
    r = value.shape[0] // 8
    return value.reshape(r, 4, 2, 128).transpose(0, 2, 1, 3).reshape(r, 2, 512)


def per_device(features, rewards, old_values, dones, lengths, proj_weights, down_weight, value_head,
               master, moment, second):
    dma = pltpu.SemaphoreType.DMA
    vm = pl.BlockSpec(memory_space=pltpu.VMEM)
    sm = pl.BlockSpec(memory_space=pltpu.SMEM)
    hbm = pl.BlockSpec(memory_space=pl.ANY)
    state = (rows_of(master), rows_of(moment), rows_of(second))
    rows = jax.ShapeDtypeStruct((8 * ROWS, 128), F32)
    row_scratch = pltpu.VMEM((8 * ROWS, 128), F32)
    block_scratch = pltpu.VMEM((4, ROWS, 1024), F32)
    link_scratch = pltpu.VMEM((2, 3, 16 + ROWS, 512), jnp.int16)
    results = pl.pallas_call(
        step_kernel,
        name="critic_step",
        out_shape=(pltpu.VMEM((8 * D, 128), BF), row_scratch, row_scratch, row_scratch,
                   pltpu.VMEM((8, 128), F32)),
        in_specs=[hbm] * 11,
        out_specs=(vm, vm, vm, vm, vm),
        scratch_shapes=[
            pltpu.VMEM((TOK, D), BF), pltpu.VMEM((4, D, 256), BF), pltpu.VMEM((FFL, D), BF),
            pltpu.VMEM((4, TOK, 256), F32), pltpu.VMEM((256, FFL), BF), pltpu.VMEM((4, TOK, 512), BF),
            pltpu.VMEM((2, 4, 3, 4, WT, 512), BF), pltpu.VMEM((2, 4, 3, WT, 512), BF), pltpu.VMEM((4, TOK, 512), BF),
            pltpu.VMEM((2, WT, D), F32), pltpu.VMEM((TOK, 2 * FFL), BF),
            row_scratch, row_scratch, row_scratch, block_scratch, block_scratch, block_scratch,
            link_scratch, link_scratch, row_scratch,
            pltpu.VMEM((8, 8, 128), F32), pltpu.VMEM((16, 8, 128), F32),
            pltpu.VMEM((1, D), F32), pltpu.VMEM((4, 256), F32), pltpu.VMEM((4, 256), F32),
            pltpu.VMEM((4, 256), jnp.int32), pltpu.SMEM((4,), jnp.int32),
            dma((13,)), dma((2, 4)), dma((9,)),
            dma((2, 4)), dma((2, 2)), dma((2, 4, 2)), dma((2, 2, 2)),
            dma((2, 3, 2)), dma((2, 4, 2)), dma((2, 4)), dma((2, 3)),
            dma((4, 2)), dma((2, 4)), dma((4,)), dma((2,)), dma((8, 3)), dma((1,)),
        ],
        compiler_params=pltpu.CompilerParams(collective_id=0, has_side_effects=True, vmem_limit_bytes=VMEM_LIMIT),
    )(features, rows_of(proj_weights), down_weight, *state, value_head.reshape(1, D), rewards, old_values, dones, lengths)
    work, master_new, moment_new, second_new, loss = pl.pallas_call(
        tail_kernel,
        name="results",
        out_shape=(jax.ShapeDtypeStruct((8 * D, 128), BF), rows, rows, rows, jax.ShapeDtypeStruct((1, 1), F32)),
        in_specs=[vm] * 5,
        out_specs=(hbm, hbm, hbm, hbm, vm),
        scratch_shapes=[dma((11,))],
        compiler_params=pltpu.CompilerParams(vmem_limit_bytes=4 * 1024 * 1024),
    )(*(pltpu.with_memory_space_constraint(r, pltpu.VMEM) for r in results))
    return (from_rows(master_new), from_rows(moment_new), from_rows(second_new), from_rows(work), loss.reshape(()))


def solution(mesh):
    finer = Mesh(mesh.devices.reshape(4, 2, 4, 4), (Z, CORE, X, Y))
    return jax.shard_map(
        per_device,
        mesh=finer,
        in_specs=(
            P(DP, None), P(DP, None), P(DP, None), P(DP, None), P(DP),
            P(None, None, MP), P(MP, None), P(),
            P(DP, None, MP), P(DP, None, MP), P(DP, None, MP),
        ),
        out_specs=(P(DP, None, MP), P(DP, None, MP), P(DP, None, MP), P(None, None, MP), P()),
        check_vma=False,
    )
```

```python
import math

import jax
import jax.numpy as jnp
from jax import lax
from jax.experimental import pallas as pl
from jax.experimental.pallas import tpu as pltpu
from jax.sharding import Mesh
from jax.sharding import PartitionSpec as P

Z, CORE, X, Y = "dp_0", "dp_1", "mp_0", "mp_1"
DP = (Z, CORE)
MP = (X, Y)
GAMMA = 0.99
LAMBDA = 0.95
MAX_NORM = 0.05
D = 2048
TOK = 1024
FFL = 512
ROWS = 256
BF = jnp.bfloat16
LEVELS = 32000.0
F32 = jnp.float32
VMEM_LIMIT = 54 * 1024 * 1024


def mul_of(v, n):
    return pl.multiple_of(v, n)


def ring(v, d):
    return lax.rem(v + (d + 4), 4)


def remote(src, dst, send, recv, device):
    return pltpu.make_async_remote_copy(
        src_ref=src, dst_ref=dst, send_sem=send, recv_sem=recv,
        device_id=device, device_id_type=pl.DeviceIdType.MESH,
    )


def greet(devices):
    barrier = pltpu.get_barrier_semaphore()
    for device in devices:
        pl.semaphore_signal(barrier, inc=1, device_id=device, device_id_type=pl.DeviceIdType.MESH)


def greeted(devices):
    pl.semaphore_wait(pltpu.get_barrier_semaphore(), len(devices))


def own_targets(row, start, rew, old, dones, lengths):
    dn = jnp.broadcast_to(dones[pl.ds(row, 1), :].astype(F32), (8, 256))
    ov = jnp.broadcast_to(old[pl.ds(row, 1), :], (8, 256))
    rw = jnp.broadcast_to(rew[pl.ds(row, 1), :], (8, 256))
    lane = lax.broadcasted_iota(jnp.int32, (8, 256), 1)
    following = jnp.where(lane == 255, 0.0, pltpu.roll(ov, 255, axis=1))
    deltas = (rw + GAMMA * following * (1.0 - dn) - ov)[0:1]
    before = lax.broadcasted_iota(jnp.int32, (256, 256), 0) < lax.broadcasted_iota(jnp.int32, (256, 256), 1)
    counted_s = jnp.dot(dn.astype(BF), before.astype(F32).astype(BF), preferred_element_type=F32)[0:1]
    t = start + lax.broadcasted_iota(jnp.int32, (WT, 256), 0)
    s = lax.broadcasted_iota(jnp.int32, (WT, 256), 1)
    counted_t = jnp.sum(jnp.where(s < t, dn[0:1], 0.0), axis=1, keepdims=True)
    linked = (counted_t == counted_s) & (s >= t)
    powers = jnp.exp(jnp.maximum(s - t, 0).astype(F32) * math.log(GAMMA * LAMBDA))
    advantage = jnp.sum(jnp.where(linked, powers, 0.0) * deltas, axis=1, keepdims=True)
    own_old = jnp.sum(jnp.where(s == t, ov[0:1], 0.0), axis=1, keepdims=True)
    mask = jnp.where(t[:, 0:1] < lengths[row], 1.0, 0.0)
    return advantage + own_old, mask


STREAMS = ((True, 1), (True, -1), (False, 1), (False, -1))
WT = 32
WAVE = 512
ORDER = (
    ("C", 2), ("S", 0, 2, 1), ("S", 0, 2, 0), ("C", 1), ("S", 1, 2, 1), ("S", 1, 1, 0), ("S", 0, 1, 1),
    ("S", 1, 2, 0), ("S", 0, 1, 0), ("C", -1), ("S", 0, -1, 1), ("S", 0, -1, 0), ("C", 0), ("PX", 0, 2),
    ("S", 0, 0, 0), ("PX", 1, 1), ("PY", 0, 2), ("PY", 0, 3), ("PX", 1, 2), ("PX", 0, 1), ("PY", 1, 2),
    ("PY", 1, 3), ("PX", 0, -1), ("S", 1, -1, 0), ("FN", 0, 0, 0), ("PX", 0, 0), ("FN", 0, 0, 1),
    ("S", 1, 1, 1), ("S", 1, -1, 1), ("S", 1, 0, 0), ("FN", 0, 2, 1), ("FN", 1, 0, 0), ("FN", 0, 2, 0),
    ("PX", 1, -1), ("FN", 0, 1, 0), ("FN", 0, 1, 1), ("FN", 1, 0, 1), ("PX", 1, 0), ("FN", 1, 2, 1),
    ("FN", 1, 2, 0), ("FN", 1, 1, 0), ("FN", 0, 3, 1), ("FN", 1, 1, 1), ("FN", 0, 3, 0), ("L", 0),
    ("G0", 0, 0), ("G0", 0, 1), ("G0b", 0, 1), ("G0b", 0, 0), ("FN", 1, 3, 0), ("FN", 1, 3, 1), ("L", 1),
    ("G0b", 1, 1), ("G0b", 1, 0), ("G0", 1, 0), ("G0", 1, 1), ("G2", 0, 0), ("G1", 0, 0), ("G1", 0, 1),
    ("G2", 0, 1), ("T", 0), ("R", 0, 0, 1), ("R", 0, 0, 0), ("R", 1, 0, 1), ("R", 1, 0, 0), ("G2", 1, 0),
    ("G2", 1, 1), ("G1", 1, 1), ("G1", 1, 0), ("G3", 0, 0), ("R", 0, 2, 0), ("R", 0, 1, 1), ("R", 0, 1, 0),
    ("R", 0, 2, 1), ("G3", 0, 1), ("B", 0, 0), ("T", 1), ("R", 1, 2, 1), ("R", 1, 2, 0), ("G3", 1, 1),
    ("R", 1, 1, 1), ("G3", 1, 0), ("B", 1, 0), ("R", 1, 1, 0), ("R", 0, 3, 0), ("R", 0, 3, 1), ("B", 0, -1),
    ("B", 0, 1), ("R", 1, 3, 1), ("R", 1, 3, 0), ("B", 1, -1), ("B", 1, 1), ("B", 0, 2), ("B", 1, 2),
)


def step_kernel(feat_hbm, w_hbm, down_hbm, master_hbm, moment_hbm, second_hbm,
                head_hbm, rew_hbm, old_hbm, dones_hbm, lengths_hbm,
                wk, mo, vo, so, sums_out,
                feat, w4, down, both, hid, part, rv1, rv2, og, mix, bg,
                master, moment, second, gsend, gown, grecv, qs, qr, gv, n1, n2,
                head, rew, old, dones, lengths,
                ins, fs, sent, rx, ry, rfr, rtwo, rg1, rga, rgb, rgc,
                dr, zr0, zr1, nr, wr, wd):
    z, core, x, y = (lax.axis_index(a) for a in (Z, CORE, X, Y))
    other = 1 - core
    me = z * 2 + core
    plane = x * 4 + y
    dp_peers = [{Z: ring(z, i // 2), CORE: lax.rem(core + i % 2, 2)} for i in range(1, 8)]
    mp_peers = [{X: ring(x, i // 4), Y: ring(y, i % 4)} for i in range(1, 16)]

    greet(dp_peers + mp_peers)
    loads = []

    def load(src, dst):
        loads.append(pltpu.make_async_copy(src, dst, ins.at[len(loads)]))
        loads[-1].start()
        return loads[-1]

    load_w = []
    for p in range(4):
        rows = pl.ds(4096 * p, 4096)
        load_w.append(load(w_hbm.at[rows], wk.at[rows]))
    load_f = {}
    for i, dy in enumerate((2, 1, -1, 0)):
        for w in range(2):
            rows = pl.ds(mul_of(ring(y, dy) * 128 + WAVE * w, 128), 128)
            load_f[w, dy] = pltpu.make_async_copy(feat_hbm.at[rows], feat.at[rows], fs.at[w, i])
    load_f[0, 2].start()
    load_f[1, 2].start()
    load_d = load(down_hbm, down)
    small, state = [], []

    out_row = lax.broadcasted_iota(jnp.int32, (256, 256), 0)
    in_row = lax.broadcasted_iota(jnp.int32, (256, 256), 1)
    select = jnp.where(in_row == (out_row % 32) * 8 + out_row // 32, 1.0, 0.0).astype(BF)
    for p in range(4):
        load_w[p].wait()
        if p == 2:
            for dy in (1, -1, 0):
                load_f[0, dy].start()
                load_f[1, dy].start()
        for u in range(8):
            base = 4096 * p + 512 * u
            pair = jnp.concatenate([wk[base:base + 256, :], wk[base + 256:base + 512, :]], axis=1)
            moved = jnp.dot(select, pair, preferred_element_type=F32).astype(BF)
            k = 512 * p + 64 * u
            for i in range(8):
                c, g = i // 2, i % 2
                for half in range(2):
                    w4[c, k + 32 * half:k + 32 * half + 32, 128 * g:128 * (g + 1)] = \
                        moved[32 * i:32 * (i + 1), 128 * half:128 * (half + 1)]
    load_d.wait()

    def peer(first, h, delta):
        along_x = STREAMS[h][0] == first
        return {X: ring(x, delta)} if along_x else {Y: ring(y, delta)}

    def tok(w, h, da, db):
        dx, dy = (da, db) if STREAMS[h][0] else (db, da)
        return pl.ds(mul_of(WAVE * w + ring(y, dy) * 128 + ring(x, dx) * WT, WT), WT)

    def offsets(h):
        s = STREAMS[h][1]
        return (2, s, -s, 0)

    def index(h, db):
        return offsets(h).index(db)

    one, two, g1, g2 = {}, {}, {}, {}
    row_at = {2: 0, 1: 1, -1: 2, 0: 3}
    for w in range(2):
        for h in range(4):
            s = STREAMS[h][1]
            for j, db in enumerate(offsets(h)):
                relayed = rx.at[w, row_at[db]] if h < 2 else ry.at[w, h - 2]
                for kind, (da, to) in enumerate(((2, s), (s, s), (-s, -s))):
                    one[w, h, kind, j] = remote(part.at[h, tok(w, h, da, db)], rv1.at[w, h, kind, j],
                                                sent.at[0], relayed if kind == 0 else rfr.at[w, j, h // 2],
                                                peer(True, h, to))
            for kind, (db, to) in enumerate(((2, s), (s, s), (-s, -s))):
                two[w, h, kind] = remote(part.at[h, tok(w, h, 0, db)], rv2.at[w, h, kind],
                                         sent.at[1], rtwo.at[w, min(kind, 1), h // 2], peer(False, h, to))
            ahead = 0 if s == 1 else 1
            for kind, (db, to) in enumerate(((0, 1), (0, -1), (-s, s))):
                t = og.at[h, tok(w, h, 0, db)]
                g1[w, h, kind] = remote(t, t, sent.at[2], rg1.at[w, {ahead: 0, 1 - ahead: 1, 2: 2}[kind], h // 2],
                                        peer(False, h, to))
            for k, db in enumerate((0, -s, s, 2)):
                for kind, (da, to) in enumerate(((0, 1), (0, -1), (-s, s))):
                    t = og.at[h, tok(w, h, da, db)]
                    if kind == ahead:
                        done = rga.at[w, k, h // 2]
                    elif h < 2:
                        done = rgb.at[w, row_at[db]]
                    else:
                        done = rgc.at[w, 2 if kind == 2 else 3 - h]
                    g2[w, h, k, kind] = remote(t, t, sent.at[3], done, peer(True, h, to))

    def arrive(count, sem):
        blocks = rv1.at[0, 0, 0, pl.ds(0, count)] if count <= 4 else rv1.at[0, pl.ds(0, count // 4), 0]
        remote(blocks, blocks, sent.at[0], sem, {X: ring(x, 1)}).wait_recv()

    def chunk(dy):
        rows = []
        for w in range(2):
            load_f[w, dy].wait()
            rows.append(pl.ds(mul_of(ring(y, dy) * 128 + WAVE * w, 128), 128))
        f = jnp.concatenate([feat[r, :] for r in rows], axis=0)
        for c in range(4):
            gu = jnp.dot(f, w4[c], preferred_element_type=F32)
            gate, up = gu[:, :128], gu[:, 128:]
            value = (gate * jax.nn.sigmoid(gate) * up).astype(BF)
            hid[:, c * 128:(c + 1) * 128] = value
            for w in range(2):
                both[c, rows[w], :] = gu[128 * w:128 * (w + 1)]
        v = hid[...]
        for h in range(4):
            product = jnp.dot(v, down[:, h * 512:(h + 1) * 512], preferred_element_type=F32).astype(BF)
            for w in range(2):
                part[h, rows[w], :] = product[128 * w:128 * (w + 1)]

    def send(w, dy, q):
        if q == 0:
            for kind in (0, 2):
                for h in (0, 1):
                    one[w, h, kind, index(h, dy)].start()
            return
        for j in range(4):
            for h in (2, 3):
                if dy == 2:
                    one[w, h, 0, j].start()
                elif dy == -STREAMS[h][1]:
                    one[w, h, 2, j].start()

    def pass_on(w, h, j):
        t = tok(w, h, STREAMS[h][1], offsets(h)[j])
        part[h, t, :] = (part[h, t, :].astype(F32) + rv1[w, h, 0, j].astype(F32)).astype(BF)
        one[w, h, 1, j].start()

    def pass_x(w, dy):
        arrive(2, rx.at[w, row_at[dy]])
        for h in (0, 1):
            pass_on(w, h, index(h, dy))

    def pass_y(w, h):
        arrive(4, ry.at[w, h - 2])
        for j in range(4):
            pass_on(w, h, j)

    def finish_one(w, h, j):
        t = tok(w, h, 0, offsets(h)[j])
        total = part[h, t, :].astype(F32) + rv1[w, h, 1, j].astype(F32) + rv1[w, h, 2, j].astype(F32)
        if j == 3:
            mix[w, :, h * 512:(h + 1) * 512] = total + rv2[w, h, 1].astype(F32) + rv2[w, h, 2].astype(F32)
            return
        if j == 1:
            total = total + rv2[w, h, 0].astype(F32)
        part[h, t, :] = total.astype(BF)
        two[w, h, j].start()

    def finish(w, j, q):
        arrive(4, rfr.at[w, j, q])
        if j == 1:
            arrive(2, rtwo.at[w, 0, q])
        if j == 3:
            arrive(4, rtwo.at[w, 1, q])
        for h in (2 * q, 2 * q + 1):
            finish_one(w, h, j)

    def own_loss(w, targets, mask):
        mine = pl.ds(mul_of(WAVE * w + y * 128 + x * WT, WT), WT)
        stream = feat[mine, :].astype(F32) + mix[w]
        vh = head[...]
        norm = lax.rsqrt(jnp.sum(stream * stream, axis=1, keepdims=True) / D + 1e-05)
        estimate = norm * jnp.sum(stream * vh, axis=1, keepdims=True)
        errors = estimate - targets
        total_tokens = TOK * 8
        coeff = 2.0 * mask * errors / total_tokens
        inner = coeff * estimate / D
        a = norm * coeff
        b = norm * norm * inner
        for h in range(4):
            cols = slice(h * 512, (h + 1) * 512)
            og[h, mine, :] = (a * vh[:, cols] - b * stream[:, cols]).astype(BF)
        return jnp.sum(mask * errors * errors, axis=0, keepdims=True) / total_tokens

    def spread(w, k, q):
        for kind in (0, 1):
            for h in (2 * q, 2 * q + 1):
                g2[w, h, k, kind].start()

    def relay(w, k, q):
        arrive(2, rga.at[w, k, q])
        for h in (2 * q, 2 * q + 1):
            g2[w, h, k, 2].start()

    def gather_0(w, q):
        for kind in (0, 1):
            for h in (2 * q, 2 * q + 1):
                g1[w, h, kind].start()

    def gather_1(w, q):
        arrive(2, rg1.at[w, 0, q])
        for h in (2 * q, 2 * q + 1):
            g1[w, h, 2].start()
        spread(w, 1, q)

    def gather_2(w, q):
        arrive(2, rg1.at[w, 1, q])
        spread(w, 2, q)

    def gather_3(w, q):
        arrive(2, rg1.at[w, 2, q])
        spread(w, 3, q)

    def backward(w, dy):
        arrive(4, rgb.at[w, row_at[dy]])
        if dy != 0:
            arrive({-1: 4, 1: 4, 2: 8}[dy], rgc.at[w, {-1: 0, 1: 1, 2: 2}[dy]])
        rows = pl.ds(mul_of(ring(y, dy) * 128 + WAVE * w, 128), 128)
        hg = None
        for h in range(4):
            term = lax.dot_general(og[h, rows, :], down[:, h * 512:(h + 1) * 512],
                                   (((1,), (1,)), ((), ())), preferred_element_type=F32)
            hg = term if hg is None else hg + term
        for c in range(4):
            gate, up = both[c, rows, :128], both[c, rows, 128:]
            d = hg[:, c * 128:(c + 1) * 128]
            sig = jax.nn.sigmoid(gate)
            bg[rows, c * 256:c * 256 + 128] = (d * up * sig * (1.0 + gate * (1.0 - sig))).astype(BF)
            bg[rows, c * 256 + 128:(c + 1) * 256] = (d * gate * sig).astype(BF)

    own, losses = [], []

    def first_columns(c):
        cols = pl.ds(mul_of((ring(z, 2) * 2 + (other if c == 0 else core)) * ROWS, ROWS), ROWS)
        for m in range(4):
            w4[c, 256 * m:256 * (m + 1), :] = feat[256 * m:256 * (m + 1), cols].T

    def loss_of(w):
        losses.append(own_loss(w, *own[w]))

    steps = {"C": chunk, "S": send, "PX": pass_x, "PY": pass_y, "FN": finish, "L": loss_of, "G0": gather_0,
             "G0b": lambda w, q: spread(w, 0, q), "G1": gather_1, "G2": gather_2, "G3": gather_3, "R": relay, "B": backward,
             "T": first_columns}
    for at, (name, *args) in enumerate(ORDER):
        if name == "FN" and not own:
            for c in small:
                c.wait()
            own.extend(own_targets(2 * w + y // 2, (y % 2) * 128 + x * WT, rew, old, dones, lengths) for w in range(2))
        steps[name](*args)
        if at == 0:
            greeted(dp_peers + mp_peers)
            small.extend(load(a, b) for a, b in ((head_hbm, head), (rew_hbm, rew), (old_hbm, old), (dones_hbm, dones),
                                                 (lengths_hbm, lengths)))
            state.extend(load(a, b) for a, b in ((master_hbm, master), (moment_hbm, moment), (second_hbm, second)))
    loss = losses[0] + losses[1]

    order = (2, 1, -1, 0)
    halves = (slice(0, 512), slice(512, 1024))
    swap = [[remote(gsend.at[i, :, half], grecv.at[i, :, half], sent.at[4], dr.at[i, h], {CORE: other})
             for h, half in enumerate(halves)] for i in range(4)]

    def grad_rows(dz, c, half):
        cols = pl.ds(mul_of((ring(z, dz) * 2 + c) * ROWS, ROWS), ROWS)
        return lax.dot_general(feat[:, cols], bg[:, half], (((0,), (0,)), ((), ())), preferred_element_type=F32)

    hop = {}
    for h, s in enumerate((1, -1)):
        for kind, to in enumerate((s, s, -s)):
            for j in range(4):
                rows = pl.ds(0, 80) if j == 0 else pl.ds(16 + 64 * j, 64)
                hop[h, kind, j] = remote(qs.at[h, kind, rows], qr.at[h, kind, rows],
                                         sent.at[5], zr0.at[h, j] if kind == 0 else zr1.at[j], {Z: ring(z, to)})

    def exponent_of(bound):
        return jnp.ceil(4.0 * jnp.log2(jnp.maximum(bound, 1e-30)) + 0.02)

    def power(exponent):
        return jnp.exp(exponent * (math.log(2.0) / 4.0))

    def received(h, kind):
        exponent = qr[h, kind, 0:16, :].astype(jnp.int32).astype(F32)[0:1]
        return power(exponent)

    def head_of(h, kind, bound):
        exponent = exponent_of(bound)
        qs[h, kind, 0:16, :] = jnp.broadcast_to(exponent, (16, 512)).astype(jnp.int32).astype(jnp.int16)
        return LEVELS * power(-exponent)

    def both_cores(i, h):
        cols = slice(512 * h, 512 * (h + 1))
        size = jnp.zeros((8, 512), F32)
        for j in range(4):
            rows = slice(64 * j, 64 * (j + 1))
            t = gown[i, rows, cols] + grecv[i, rows, cols]
            gown[i, rows, cols] = t
            size = jnp.maximum(size, jnp.max(jnp.abs(t).reshape(8, 8, 512), axis=0))
        return jnp.max(size, axis=0, keepdims=True)

    def mine_of(i, h, j):
        return gown[i, 64 * j:64 * (j + 1), 512 * h:512 * (h + 1)]

    def code(value, scale):
        return jnp.round(value * scale).astype(jnp.int32).astype(jnp.int16)

    def value_of(h, kind, j, unit):
        return qr[h, kind, 16 + 64 * j:80 + 64 * j, :].astype(jnp.int32).astype(F32) * unit

    def straight(i, h, kind):
        scale = head_of(h, kind, both_cores(i, h))
        for j in range(4):
            qs[h, kind, 16 + 64 * j:80 + 64 * j, :] = code(mine_of(i, h, j), scale)
            hop[h, kind, j].start()

    def pass_sum(i, h):
        size = both_cores(i, h)
        hop[h, 0, 0].wait_recv()
        far_size = received(h, 0)
        scale = head_of(h, 1, size + far_size)
        for j in range(4):
            if j > 0:
                hop[h, 0, j].wait_recv()
            qs[h, 1, 16 + 64 * j:80 + 64 * j, :] = code(mine_of(i, h, j) + value_of(h, 0, j, far_size / LEVELS), scale)
            hop[h, 1, j].start()

    def first_rows(c, cols):
        total = None
        for m in range(4):
            term = jnp.dot(w4[c, 256 * m:256 * (m + 1), :], bg[256 * m:256 * (m + 1), cols], preferred_element_type=F32)
            total = term if total is None else total + term
        return total

    for q in range(4):
        quarter = slice(256 * q, 256 * (q + 1))
        gsend[0, :, quarter] = first_rows(0, quarter)
        remote(gsend.at[0, :, quarter], grecv.at[0, :, quarter], sent.at[4], dr.at[0, q // 2], {CORE: other}).start()
    for half in halves:
        gown[0, :, half] = first_rows(1, half)
    for i, dz in enumerate(order):
        if i == 0:
            continue
        for h, half in enumerate(halves):
            gsend[i, :, half] = grad_rows(dz, other, half)
            swap[i][h].start()
        if i == 1:
            for h in (0, 1):
                swap[0][h].wait_recv()
                straight(0, h, 0)
        if i == 2:
            swap[1][1].wait_recv()
            straight(1, 1, 2)
        if i == 3:
            swap[2][0].wait_recv()
            straight(2, 0, 2)
        for half in halves:
            gown[i, :, half] = grad_rows(dz, core, half)
    swap[1][0].wait_recv()
    pass_sum(1, 0)
    swap[2][1].wait_recv()
    pass_sum(2, 1)
    for h in (0, 1):
        swap[3][h].wait_recv()
    squares = jnp.zeros((8, 128), F32)
    units = {}
    for j in range(4):
        blocks = qr.at[:, pl.ds(1, 2), pl.ds(0, 80) if j == 0 else pl.ds(16 + 64 * j, 64)]
        remote(blocks, blocks, sent.at[5], zr1.at[j], {Z: ring(z, 1)}).wait_recv()
        for h in range(2):
            if j == 0:
                units[h] = [received(h, kind) / LEVELS for kind in (1, 2)]
            owned = gown[3, 64 * j:64 * (j + 1), 512 * h:512 * (h + 1)] + grecv[3, 64 * j:64 * (j + 1), 512 * h:512 * (h + 1)]
            g = owned + value_of(h, 1, j, units[h][0]) + value_of(h, 2, j, units[h][1])
            for c in range(4):
                piece = g[:, c * 128:(c + 1) * 128]
                gv[pl.ds(64 * j * 8 + 4 * h + c, 64, stride=8), :] = piece
                squares = squares + jnp.sum((piece * piece).reshape(8, 8, 128), axis=0)

    line = lax.broadcasted_iota(jnp.int32, (8, 128), 0)
    n1[me] = jnp.where(line == 0, jnp.sum(squares, axis=0, keepdims=True), jnp.where(line == 1, loss, 0.0))
    near = [remote(n1.at[me], n1.at[me], sent.at[6], nr.at[0], p) for p in dp_peers]
    for c in near:
        c.start()
    seven, fifteen = n1.at[pl.ds(0, 7)], n2.at[pl.ds(0, 15)]
    remote(seven, seven, sent.at[6], nr.at[0], dp_peers[0]).wait_recv()
    sums = n1[0]
    for i in range(1, 8):
        sums = sums + n1[i]
    n2[plane] = sums
    far = [remote(n2.at[plane], n2.at[plane], sent.at[7], nr.at[1], p) for p in mp_peers]
    for c in far:
        c.start()
    remote(fifteen, fifteen, sent.at[7], nr.at[1], mp_peers[0]).wait_recv()
    sums = n2[0]
    for i in range(1, 16):
        sums = sums + n2[i]
    sums_out[...] = sums
    squared = jnp.sum(sums[0:1], axis=1, keepdims=True)
    clip = jnp.minimum(1.0, MAX_NORM / (jnp.sqrt(squared) + 1e-06))

    def place(device, q):
        return pl.ds(mul_of(device * 2048 + q * 256, 256), 256)

    def block(device, q):
        return wk.at[place(device, q)]

    spread_dp = {}
    for q in range(8):
        s = 1 if q % 2 == 0 else -1
        src = {0: (me, {Z: ring(z, 1)}), 1: (me, {Z: ring(z, -1)}),
               2: (ring(z, -s) * 2 + core, {Z: ring(z, s)}),
               3: (me, {CORE: other}), 4: (ring(z, -1) * 2 + core, {CORE: other}),
               5: (ring(z, 1) * 2 + core, {CORE: other}), 6: (ring(z, 2) * 2 + core, {CORE: other})}
        for kind, (device, to) in src.items():
            b = block(device, q)
            spread_dp[q, kind] = remote(b, b, sent.at[8], wr.at[q, kind] if kind < 3 else wd.at[0], to)
    for c in state:
        c.wait()
    for q in range(8):
        rows = pl.ds(256 * q, 256)
        g = gv[rows, :] * clip
        new, m, v = updated(g, master[rows, :], moment[rows, :], second[rows, :])
        mo[rows, :] = new
        vo[rows, :] = m
        so[rows, :] = v
        wk[place(me, q), :] = new.astype(BF)
        for kind in (0, 1, 3):
            spread_dp[q, kind].start()
    for q in range(8):
        with_relay, against = (0, 1) if q % 2 == 0 else (1, 0)
        spread_dp[q, with_relay].wait_recv()
        spread_dp[q, 2].start()
        spread_dp[q, 4 + with_relay].start()
        spread_dp[q, against].wait_recv()
        spread_dp[q, 4 + against].start()
    for q in range(8):
        spread_dp[q, 2].wait_recv()
        spread_dp[q, 6].start()
    four, all_but_one = wk.at[pl.ds(0, 4 * 2048)], wk.at[pl.ds(0, 7 * 2048)]
    remote(four, four, sent.at[8], wd.at[0], {CORE: other}).wait_recv()
    for i, (ref, device) in enumerate(((rv1, {X: ring(x, 1)}), (rv2, {X: ring(x, 1)}), (rv2, {X: ring(x, 1)}),
                                       (rv1, {X: ring(x, 1)}), (gsend, {CORE: other}), (qs, {Z: ring(z, 1)}),
                                       (seven, dp_peers[0]), (fifteen, mp_peers[0]), (all_but_one, {CORE: other}))):
        remote(ref, ref, sent.at[i], nr.at[0], device).wait_send()


def tail_kernel(work, master, moment, second, sums, work_out, master_out, moment_out, second_out, loss, sems):
    pieces = [(work.at[pl.ds(2048 * i, 2048)], work_out.at[pl.ds(2048 * i, 2048)]) for i in range(8)]
    pieces += [(master, master_out), (moment, moment_out), (second, second_out)]
    copies = [pltpu.make_async_copy(a, b, sems.at[i]) for i, (a, b) in enumerate(pieces)]
    for c in copies:
        c.start()
    loss[...] = sums[1:2, 0:1]
    for c in copies:
        c.wait()


def updated(g, old, moment, second):
    m = 0.9 * moment + 0.1 * g
    v = 0.999 * second + 0.001 * g * g
    first_hat = m * (1.0 / (1.0 - 0.9 ** 10))
    second_hat = v * (1.0 / (1.0 - 0.999 ** 10))
    return old - 0.001 * (first_hat / (jnp.sqrt(second_hat) + 1e-08) + 0.1 * old), m, v


def rows_of(value):
    r = value.shape[0]
    return value.reshape(r, 2, 4, 128).transpose(0, 2, 1, 3).reshape(r * 8, 128)


def from_rows(value):
    r = value.shape[0] // 8
    return value.reshape(r, 4, 2, 128).transpose(0, 2, 1, 3).reshape(r, 2, 512)


def per_device(features, rewards, old_values, dones, lengths, proj_weights, down_weight, value_head,
               master, moment, second):
    dma = pltpu.SemaphoreType.DMA
    vm = pl.BlockSpec(memory_space=pltpu.VMEM)
    sm = pl.BlockSpec(memory_space=pltpu.SMEM)
    hbm = pl.BlockSpec(memory_space=pl.ANY)
    state = (rows_of(master), rows_of(moment), rows_of(second))
    rows = jax.ShapeDtypeStruct((8 * ROWS, 128), F32)
    row_scratch = pltpu.VMEM((8 * ROWS, 128), F32)
    block_scratch = pltpu.VMEM((4, ROWS, 1024), F32)
    link_scratch = pltpu.VMEM((2, 3, 16 + ROWS, 512), jnp.int16)
    results = pl.pallas_call(
        step_kernel,
        name="critic_step",
        out_shape=(pltpu.VMEM((8 * D, 128), BF), row_scratch, row_scratch, row_scratch,
                   pltpu.VMEM((8, 128), F32)),
        in_specs=[hbm] * 11,
        out_specs=(vm, vm, vm, vm, vm),
        scratch_shapes=[
            pltpu.VMEM((TOK, D), BF), pltpu.VMEM((4, D, 256), BF), pltpu.VMEM((FFL, D), BF),
            pltpu.VMEM((4, TOK, 256), F32), pltpu.VMEM((256, FFL), BF), pltpu.VMEM((4, TOK, 512), BF),
            pltpu.VMEM((2, 4, 3, 4, WT, 512), BF), pltpu.VMEM((2, 4, 3, WT, 512), BF), pltpu.VMEM((4, TOK, 512), BF),
            pltpu.VMEM((2, WT, D), F32), pltpu.VMEM((TOK, 2 * FFL), BF),
            row_scratch, row_scratch, row_scratch, block_scratch, block_scratch, block_scratch,
            link_scratch, link_scratch, row_scratch,
            pltpu.VMEM((8, 8, 128), F32), pltpu.VMEM((16, 8, 128), F32),
            pltpu.VMEM((1, D), F32), pltpu.VMEM((4, 256), F32), pltpu.VMEM((4, 256), F32),
            pltpu.VMEM((4, 256), jnp.int32), pltpu.SMEM((4,), jnp.int32),
            dma((13,)), dma((2, 4)), dma((9,)),
            dma((2, 4)), dma((2, 2)), dma((2, 4, 2)), dma((2, 2, 2)),
            dma((2, 3, 2)), dma((2, 4, 2)), dma((2, 4)), dma((2, 3)),
            dma((4, 2)), dma((2, 4)), dma((4,)), dma((2,)), dma((8, 3)), dma((1,)),
        ],
        compiler_params=pltpu.CompilerParams(collective_id=0, has_side_effects=True, vmem_limit_bytes=VMEM_LIMIT),
    )(features, rows_of(proj_weights), down_weight, *state, value_head.reshape(1, D), rewards, old_values, dones, lengths)
    work, master_new, moment_new, second_new, loss = pl.pallas_call(
        tail_kernel,
        name="results",
        out_shape=(jax.ShapeDtypeStruct((8 * D, 128), BF), rows, rows, rows, jax.ShapeDtypeStruct((1, 1), F32)),
        in_specs=[vm] * 5,
        out_specs=(hbm, hbm, hbm, hbm, vm),
        scratch_shapes=[dma((11,))],
        compiler_params=pltpu.CompilerParams(vmem_limit_bytes=4 * 1024 * 1024),
    )(*(pltpu.with_memory_space_constraint(r, pltpu.VMEM) for r in results))
    return (from_rows(master_new), from_rows(moment_new), from_rows(second_new), from_rows(work), loss.reshape(()))


def solution(mesh):
    finer = Mesh(mesh.devices.reshape(4, 2, 4, 4), (Z, CORE, X, Y))
    return jax.shard_map(
        per_device,
        mesh=finer,
        in_specs=(
            P(DP, None), P(DP, None), P(DP, None), P(DP, None), P(DP),
            P(None, None, MP), P(MP, None), P(),
            P(DP, None, MP), P(DP, None, MP), P(DP, None, MP),
        ),
        out_specs=(P(DP, None, MP), P(DP, None, MP), P(DP, None, MP), P(None, None, MP), P()),
        check_vma=False,
    )
```

```python
import math

import jax
import jax.numpy as jnp
from jax import lax
from jax.experimental import pallas as pl
from jax.experimental.pallas import tpu as pltpu
from jax.sharding import Mesh
from jax.sharding import PartitionSpec as P

Z, CORE, X, Y = "dp_0", "dp_1", "mp_0", "mp_1"
DP = (Z, CORE)
MP = (X, Y)
GAMMA = 0.99
LAMBDA = 0.95
MAX_NORM = 0.05
D = 2048
TOK = 1024
FFL = 512
ROWS = 256
BF = jnp.bfloat16
LEVELS = 32000.0
F32 = jnp.float32
VMEM_LIMIT = 54 * 1024 * 1024


def mul_of(v, n):
    return pl.multiple_of(v, n)


def ring(v, d):
    return lax.rem(v + (d + 4), 4)


def remote(src, dst, send, recv, device):
    return pltpu.make_async_remote_copy(
        src_ref=src, dst_ref=dst, send_sem=send, recv_sem=recv,
        device_id=device, device_id_type=pl.DeviceIdType.MESH,
    )


def greet(devices):
    barrier = pltpu.get_barrier_semaphore()
    for device in devices:
        pl.semaphore_signal(barrier, inc=1, device_id=device, device_id_type=pl.DeviceIdType.MESH)


def greeted(devices):
    pl.semaphore_wait(pltpu.get_barrier_semaphore(), len(devices))


def own_targets(row, start, rew, old, dones, lengths):
    dn = jnp.broadcast_to(dones[pl.ds(row, 1), :].astype(F32), (8, 256))
    ov = jnp.broadcast_to(old[pl.ds(row, 1), :], (8, 256))
    rw = jnp.broadcast_to(rew[pl.ds(row, 1), :], (8, 256))
    lane = lax.broadcasted_iota(jnp.int32, (8, 256), 1)
    following = jnp.where(lane == 255, 0.0, pltpu.roll(ov, 255, axis=1))
    deltas = (rw + GAMMA * following * (1.0 - dn) - ov)[0:1]
    before = lax.broadcasted_iota(jnp.int32, (256, 256), 0) < lax.broadcasted_iota(jnp.int32, (256, 256), 1)
    counted_s = jnp.dot(dn.astype(BF), before.astype(F32).astype(BF), preferred_element_type=F32)[0:1]
    t = start + lax.broadcasted_iota(jnp.int32, (WT, 256), 0)
    s = lax.broadcasted_iota(jnp.int32, (WT, 256), 1)
    counted_t = jnp.sum(jnp.where(s < t, dn[0:1], 0.0), axis=1, keepdims=True)
    linked = (counted_t == counted_s) & (s >= t)
    powers = jnp.exp(jnp.maximum(s - t, 0).astype(F32) * math.log(GAMMA * LAMBDA))
    advantage = jnp.sum(jnp.where(linked, powers, 0.0) * deltas, axis=1, keepdims=True)
    own_old = jnp.sum(jnp.where(s == t, ov[0:1], 0.0), axis=1, keepdims=True)
    mask = jnp.where(t[:, 0:1] < lengths[row], 1.0, 0.0)
    return advantage + own_old, mask


STREAMS = ((True, 1), (True, -1), (False, 1), (False, -1))
WT = 32
WAVE = 512
ORDER = (
     ("C", 1), ("S", 1, 2, 1), ("S", 1, 1, 0), ("S", 0, 1, 1),
    ("S", 1, 2, 0), ("S", 0, 1, 0), ("C", -1), ("S", 0, -1, 1), ("S", 0, -1, 0), ("C", 0), ("PX", 0, 2),
    ("S", 0, 0, 0), ("PX", 1, 1), ("PY", 0, 2), ("PY", 0, 3), ("PX", 1, 2), ("PX", 0, 1), ("PY", 1, 2),
    ("PY", 1, 3), ("PX", 0, -1), ("S", 1, -1, 0), ("FN", 0, 0, 0), ("PX", 0, 0), ("FN", 0, 0, 1),
    ("S", 1, 1, 1), ("S", 1, -1, 1), ("S", 1, 0, 0), ("FN", 0, 2, 1), ("FN", 1, 0, 0), ("FN", 0, 2, 0),
    ("PX", 1, -1), ("FN", 0, 1, 0), ("FN", 0, 1, 1), ("FN", 1, 0, 1), ("PX", 1, 0), ("FN", 1, 2, 1),
    ("FN", 1, 2, 0), ("FN", 1, 1, 0), ("FN", 0, 3, 1), ("FN", 1, 1, 1), ("FN", 0, 3, 0), ("L", 0),
    ("G0", 0, 0), ("G0", 0, 1), ("G0b", 0, 1), ("G0b", 0, 0), ("FN", 1, 3, 0), ("FN", 1, 3, 1), ("L", 1),
    ("G0b", 1, 1), ("G0b", 1, 0), ("G0", 1, 0), ("G0", 1, 1), ("G2", 0, 0), ("G1", 0, 0), ("G1", 0, 1),
    ("G2", 0, 1), ("T", 0), ("R", 0, 0, 1), ("R", 0, 0, 0), ("R", 1, 0, 1), ("R", 1, 0, 0), ("G2", 1, 0),
    ("G2", 1, 1), ("G1", 1, 1), ("G1", 1, 0), ("G3", 0, 0), ("R", 0, 2, 0), ("R", 0, 1, 1), ("R", 0, 1, 0),
    ("R", 0, 2, 1), ("G3", 0, 1), ("B", 0, 0), ("T", 1), ("R", 1, 2, 1), ("R", 1, 2, 0), ("G3", 1, 1),
    ("R", 1, 1, 1), ("G3", 1, 0), ("B", 1, 0), ("R", 1, 1, 0), ("R", 0, 3, 0), ("R", 0, 3, 1), ("B", 0, -1),
    ("B", 0, 1), ("R", 1, 3, 1), ("R", 1, 3, 0), ("B", 1, -1), ("B", 1, 1), ("B", 0, 2), ("B", 1, 2),
)


def step_kernel(feat_hbm, w_hbm, down_hbm, master_hbm, moment_hbm, second_hbm,
                head_hbm, rew_hbm, old_hbm, dones_hbm, lengths_hbm,
                wk, mo, vo, so, sums_out,
                feat, w4, down, both, hid, part, rv1, rv2, og, mix, bg,
                master, moment, second, gsend, gown, grecv, qs, qr, gv, n1, n2,
                head, rew, old, dones, lengths,
                ins, fs, sent, rx, ry, rfr, rtwo, rg1, rga, rgb, rgc,
                dr, zr0, zr1, nr, wr, wd):
    z, core, x, y = (lax.axis_index(a) for a in (Z, CORE, X, Y))
    other = 1 - core
    me = z * 2 + core
    plane = x * 4 + y
    dp_peers = [{Z: ring(z, i // 2), CORE: lax.rem(core + i % 2, 2)} for i in range(1, 8)]
    mp_peers = [{X: ring(x, i // 4), Y: ring(y, i % 4)} for i in range(1, 16)]

    greet(dp_peers + mp_peers)
    loads = []

    def load(src, dst):
        loads.append(pltpu.make_async_copy(src, dst, ins.at[len(loads)]))
        loads[-1].start()
        return loads[-1]

    load_w = []
    for p in range(4):
        rows = pl.ds(4096 * p, 4096)
        load_w.append(load(w_hbm.at[rows], wk.at[rows]))
    load_f = {}
    for i, dy in enumerate((2, 1, -1, 0)):
        for w in range(2):
            rows = pl.ds(mul_of(ring(y, dy) * 128 + WAVE * w, 128), 128)
            load_f[w, dy] = pltpu.make_async_copy(feat_hbm.at[rows], feat.at[rows], fs.at[w, i])
    load_f[0, 2].start()
    load_f[1, 2].start()
    load_d = load(down_hbm, down)
    small, state = [], []

    out_row = lax.broadcasted_iota(jnp.int32, (256, 256), 0)
    in_row = lax.broadcasted_iota(jnp.int32, (256, 256), 1)
    select = jnp.where(in_row == (out_row % 32) * 8 + out_row // 32, 1.0, 0.0).astype(BF)
    for p in range(4):
        if p % 2 == 0:
            load_w[p].wait()
            load_w[p + 1].wait()
        if p == 2:
            for dy in (1, -1, 0):
                load_f[0, dy].start()
                load_f[1, dy].start()
        for u in range(8):
            base = 4096 * p + 512 * u
            pair = jnp.concatenate([wk[base:base + 256, :], wk[base + 256:base + 512, :]], axis=1)
            moved = jnp.dot(select, pair, preferred_element_type=F32).astype(BF)
            k = 512 * p + 64 * u
            for i in range(8):
                c, g = i // 2, i % 2
                for half in range(2):
                    w4[c, k + 32 * half:k + 32 * half + 32, 128 * g:128 * (g + 1)] = \
                        moved[32 * i:32 * (i + 1), 128 * half:128 * (half + 1)]
    load_d.wait()

    def peer(first, h, delta):
        along_x = STREAMS[h][0] == first
        return {X: ring(x, delta)} if along_x else {Y: ring(y, delta)}

    def tok(w, h, da, db):
        dx, dy = (da, db) if STREAMS[h][0] else (db, da)
        return pl.ds(mul_of(WAVE * w + ring(y, dy) * 128 + ring(x, dx) * WT, WT), WT)

    def offsets(h):
        s = STREAMS[h][1]
        return (2, s, -s, 0)

    def index(h, db):
        return offsets(h).index(db)

    one, two, g1, g2 = {}, {}, {}, {}
    row_at = {2: 0, 1: 1, -1: 2, 0: 3}
    for w in range(2):
        for h in range(4):
            s = STREAMS[h][1]
            for j, db in enumerate(offsets(h)):
                relayed = rx.at[w, row_at[db]] if h < 2 else ry.at[w, h - 2]
                for kind, (da, to) in enumerate(((2, s), (s, s), (-s, -s))):
                    one[w, h, kind, j] = remote(part.at[h, tok(w, h, da, db)], rv1.at[w, h, kind, j],
                                                sent.at[0], relayed if kind == 0 else rfr.at[w, j, h // 2],
                                                peer(True, h, to))
            for kind, (db, to) in enumerate(((2, s), (s, s), (-s, -s))):
                two[w, h, kind] = remote(part.at[h, tok(w, h, 0, db)], rv2.at[w, h, kind],
                                         sent.at[1], rtwo.at[w, min(kind, 1), h // 2], peer(False, h, to))
            ahead = 0 if s == 1 else 1
            for kind, (db, to) in enumerate(((0, 1), (0, -1), (-s, s))):
                t = og.at[h, tok(w, h, 0, db)]
                g1[w, h, kind] = remote(t, t, sent.at[2], rg1.at[w, {ahead: 0, 1 - ahead: 1, 2: 2}[kind], h // 2],
                                        peer(False, h, to))
            for k, db in enumerate((0, -s, s, 2)):
                for kind, (da, to) in enumerate(((0, 1), (0, -1), (-s, s))):
                    t = og.at[h, tok(w, h, da, db)]
                    if kind == ahead:
                        done = rga.at[w, k, h // 2]
                    elif h < 2:
                        done = rgb.at[w, row_at[db]]
                    else:
                        done = rgc.at[w, 2 if kind == 2 else 3 - h]
                    g2[w, h, k, kind] = remote(t, t, sent.at[3], done, peer(True, h, to))

    def arrive(count, sem):
        blocks = rv1.at[0, 0, 0, pl.ds(0, count)] if count <= 4 else rv1.at[0, pl.ds(0, count // 4), 0]
        remote(blocks, blocks, sent.at[0], sem, {X: ring(x, 1)}).wait_recv()

    def chunk(dy, waves=(0, 1), ready=None):
        rows, n = [], 128 * len(waves)
        for w in waves:
            load_f[w, dy].wait()
            rows.append(pl.ds(mul_of(ring(y, dy) * 128 + WAVE * w, 128), 128))
        f = jnp.concatenate([feat[r, :] for r in rows], axis=0)
        for c in range(4):
            gu = jnp.dot(f, w4[c], preferred_element_type=F32)
            gate, up = gu[:, :128], gu[:, 128:]
            value = (gate * jax.nn.sigmoid(gate) * up).astype(BF)
            hid[0:n, c * 128:(c + 1) * 128] = value
            for i, r in enumerate(rows):
                both[c, r, :] = gu[128 * i:128 * (i + 1)]
        v = hid[0:n, :]
        for h in (2, 3, 0, 1):
            product = jnp.dot(v, down[:, h * 512:(h + 1) * 512], preferred_element_type=F32).astype(BF)
            for i, r in enumerate(rows):
                part[h, r, :] = product[128 * i:128 * (i + 1)]
            if ready is not None and h % 2 == 1:
                ready(h)

    def send(w, dy, q):
        if q == 0:
            for kind in (0, 2):
                for h in (0, 1):
                    one[w, h, kind, index(h, dy)].start()
            return
        for j in range(4):
            for h in (2, 3):
                if dy == 2:
                    one[w, h, 0, j].start()
                elif dy == -STREAMS[h][1]:
                    one[w, h, 2, j].start()

    def pass_on(w, h, j):
        t = tok(w, h, STREAMS[h][1], offsets(h)[j])
        part[h, t, :] = (part[h, t, :].astype(F32) + rv1[w, h, 0, j].astype(F32)).astype(BF)
        one[w, h, 1, j].start()

    def pass_x(w, dy):
        arrive(2, rx.at[w, row_at[dy]])
        for h in (0, 1):
            pass_on(w, h, index(h, dy))

    def pass_y(w, h):
        arrive(4, ry.at[w, h - 2])
        for j in range(4):
            pass_on(w, h, j)

    def finish_one(w, h, j):
        t = tok(w, h, 0, offsets(h)[j])
        total = part[h, t, :].astype(F32) + rv1[w, h, 1, j].astype(F32) + rv1[w, h, 2, j].astype(F32)
        if j == 3:
            mix[w, :, h * 512:(h + 1) * 512] = total + rv2[w, h, 1].astype(F32) + rv2[w, h, 2].astype(F32)
            return
        if j == 1:
            total = total + rv2[w, h, 0].astype(F32)
        part[h, t, :] = total.astype(BF)
        two[w, h, j].start()

    def finish(w, j, q):
        arrive(4, rfr.at[w, j, q])
        if j == 1:
            arrive(2, rtwo.at[w, 0, q])
        if j == 3:
            arrive(4, rtwo.at[w, 1, q])
        for h in (2 * q, 2 * q + 1):
            finish_one(w, h, j)

    def own_loss(w, targets, mask):
        mine = pl.ds(mul_of(WAVE * w + y * 128 + x * WT, WT), WT)
        stream = feat[mine, :].astype(F32) + mix[w]
        vh = head[...]
        norm = lax.rsqrt(jnp.sum(stream * stream, axis=1, keepdims=True) / D + 1e-05)
        estimate = norm * jnp.sum(stream * vh, axis=1, keepdims=True)
        errors = estimate - targets
        total_tokens = TOK * 8
        coeff = 2.0 * mask * errors / total_tokens
        inner = coeff * estimate / D
        a = norm * coeff
        b = norm * norm * inner
        for h in range(4):
            cols = slice(h * 512, (h + 1) * 512)
            og[h, mine, :] = (a * vh[:, cols] - b * stream[:, cols]).astype(BF)
        return jnp.sum(mask * errors * errors, axis=0, keepdims=True) / total_tokens

    def spread(w, k, q):
        for kind in (0, 1):
            for h in (2 * q, 2 * q + 1):
                g2[w, h, k, kind].start()

    def relay(w, k, q):
        arrive(2, rga.at[w, k, q])
        for h in (2 * q, 2 * q + 1):
            g2[w, h, k, 2].start()

    def gather_0(w, q):
        for kind in (0, 1):
            for h in (2 * q, 2 * q + 1):
                g1[w, h, kind].start()

    def gather_1(w, q):
        arrive(2, rg1.at[w, 0, q])
        for h in (2 * q, 2 * q + 1):
            g1[w, h, 2].start()
        spread(w, 1, q)

    def gather_2(w, q):
        arrive(2, rg1.at[w, 1, q])
        spread(w, 2, q)

    def gather_3(w, q):
        arrive(2, rg1.at[w, 2, q])
        spread(w, 3, q)

    def backward(w, dy):
        arrive(4, rgb.at[w, row_at[dy]])
        if dy != 0:
            arrive({-1: 4, 1: 4, 2: 8}[dy], rgc.at[w, {-1: 0, 1: 1, 2: 2}[dy]])
        rows = pl.ds(mul_of(ring(y, dy) * 128 + WAVE * w, 128), 128)
        hg = None
        for h in range(4):
            term = lax.dot_general(og[h, rows, :], down[:, h * 512:(h + 1) * 512],
                                   (((1,), (1,)), ((), ())), preferred_element_type=F32)
            hg = term if hg is None else hg + term
        for c in range(4):
            gate, up = both[c, rows, :128], both[c, rows, 128:]
            d = hg[:, c * 128:(c + 1) * 128]
            sig = jax.nn.sigmoid(gate)
            bg[rows, c * 256:c * 256 + 128] = (d * up * sig * (1.0 + gate * (1.0 - sig))).astype(BF)
            bg[rows, c * 256 + 128:(c + 1) * 256] = (d * gate * sig).astype(BF)

    own, losses = [], []

    def first_columns(c):
        cols = pl.ds(mul_of((ring(z, 2) * 2 + (other if c == 0 else core)) * ROWS, ROWS), ROWS)
        for m in range(4):
            w4[c, 256 * m:256 * (m + 1), :] = feat[256 * m:256 * (m + 1), cols].T

    def loss_of(w):
        losses.append(own_loss(w, *own[w]))

    steps = {"C": chunk, "S": send, "PX": pass_x, "PY": pass_y, "FN": finish, "L": loss_of, "G0": gather_0,
             "G0b": lambda w, q: spread(w, 0, q), "G1": gather_1, "G2": gather_2, "G3": gather_3, "R": relay, "B": backward,
             "T": first_columns}

    def first_sends(h):
        if h == 3:
            greeted(dp_peers + mp_peers)
        send(0, 2, h // 2)

    chunk(2, (0,), first_sends)
    chunk(2, (1,))
    for at, (name, *args) in enumerate(ORDER):
        if name == "FN" and not own:
            for c in small:
                c.wait()
            own.extend(own_targets(2 * w + y // 2, (y % 2) * 128 + x * WT, rew, old, dones, lengths) for w in range(2))
        steps[name](*args)
        if at == 0:
            small.extend(load(a, b) for a, b in ((head_hbm, head), (rew_hbm, rew), (old_hbm, old), (dones_hbm, dones),
                                                 (lengths_hbm, lengths)))
            state.extend(load(a, b) for a, b in ((master_hbm, master), (moment_hbm, moment), (second_hbm, second)))
    loss = losses[0] + losses[1]

    order = (2, 1, -1, 0)
    halves = (slice(0, 512), slice(512, 1024))
    swap = [[remote(gsend.at[i, :, half], grecv.at[i, :, half], sent.at[4], dr.at[i, h], {CORE: other})
             for h, half in enumerate(halves)] for i in range(4)]

    def grad_rows(dz, c, half):
        cols = pl.ds(mul_of((ring(z, dz) * 2 + c) * ROWS, ROWS), ROWS)
        return lax.dot_general(feat[:, cols], bg[:, half], (((0,), (0,)), ((), ())), preferred_element_type=F32)

    hop = {}
    for h, s in enumerate((1, -1)):
        for kind, to in enumerate((s, s, -s)):
            for j in range(4):
                rows = pl.ds(0, 80) if j == 0 else pl.ds(16 + 64 * j, 64)
                hop[h, kind, j] = remote(qs.at[h, kind, rows], qr.at[h, kind, rows],
                                         sent.at[5], zr0.at[h, j] if kind == 0 else zr1.at[j], {Z: ring(z, to)})

    def exponent_of(bound):
        return jnp.ceil(4.0 * jnp.log2(jnp.maximum(bound, 1e-30)) + 0.02)

    def power(exponent):
        return jnp.exp(exponent * (math.log(2.0) / 4.0))

    def received(h, kind):
        exponent = qr[h, kind, 0:16, :].astype(jnp.int32).astype(F32)[0:1]
        return power(exponent)

    def head_of(h, kind, bound):
        exponent = exponent_of(bound)
        qs[h, kind, 0:16, :] = jnp.broadcast_to(exponent, (16, 512)).astype(jnp.int32).astype(jnp.int16)
        return LEVELS * power(-exponent)

    def both_cores(i, h):
        cols = slice(512 * h, 512 * (h + 1))
        size = jnp.zeros((8, 512), F32)
        for j in range(4):
            rows = slice(64 * j, 64 * (j + 1))
            t = gown[i, rows, cols] + grecv[i, rows, cols]
            gown[i, rows, cols] = t
            size = jnp.maximum(size, jnp.max(jnp.abs(t).reshape(8, 8, 512), axis=0))
        return jnp.max(size, axis=0, keepdims=True)

    def mine_of(i, h, j):
        return gown[i, 64 * j:64 * (j + 1), 512 * h:512 * (h + 1)]

    def code(value, scale):
        return jnp.round(value * scale).astype(jnp.int32).astype(jnp.int16)

    def value_of(h, kind, j, unit):
        return qr[h, kind, 16 + 64 * j:80 + 64 * j, :].astype(jnp.int32).astype(F32) * unit

    def straight(i, h, kind):
        scale = head_of(h, kind, both_cores(i, h))
        for j in range(4):
            qs[h, kind, 16 + 64 * j:80 + 64 * j, :] = code(mine_of(i, h, j), scale)
            hop[h, kind, j].start()

    def pass_sum(i, h):
        size = both_cores(i, h)
        hop[h, 0, 0].wait_recv()
        far_size = received(h, 0)
        scale = head_of(h, 1, size + far_size)
        for j in range(4):
            if j > 0:
                hop[h, 0, j].wait_recv()
            qs[h, 1, 16 + 64 * j:80 + 64 * j, :] = code(mine_of(i, h, j) + value_of(h, 0, j, far_size / LEVELS), scale)
            hop[h, 1, j].start()

    def first_rows(c, cols):
        total = None
        for m in range(4):
            term = jnp.dot(w4[c, 256 * m:256 * (m + 1), :], bg[256 * m:256 * (m + 1), cols], preferred_element_type=F32)
            total = term if total is None else total + term
        return total

    for q in range(4):
        quarter = slice(256 * q, 256 * (q + 1))
        gsend[0, :, quarter] = first_rows(0, quarter)
        remote(gsend.at[0, :, quarter], grecv.at[0, :, quarter], sent.at[4], dr.at[0, q // 2], {CORE: other}).start()
    for half in halves:
        gown[0, :, half] = first_rows(1, half)
    for i, dz in enumerate(order):
        if i == 0:
            continue
        for h, half in enumerate(halves):
            gsend[i, :, half] = grad_rows(dz, other, half)
            swap[i][h].start()
        if i == 1:
            for h in (0, 1):
                swap[0][h].wait_recv()
                straight(0, h, 0)
        if i == 2:
            swap[1][1].wait_recv()
            straight(1, 1, 2)
        if i == 3:
            swap[2][0].wait_recv()
            straight(2, 0, 2)
        for half in halves:
            gown[i, :, half] = grad_rows(dz, core, half)
    swap[1][0].wait_recv()
    pass_sum(1, 0)
    swap[2][1].wait_recv()
    pass_sum(2, 1)
    for h in (0, 1):
        swap[3][h].wait_recv()
    squares = jnp.zeros((8, 128), F32)
    units = {}
    for j in range(4):
        blocks = qr.at[:, pl.ds(1, 2), pl.ds(0, 80) if j == 0 else pl.ds(16 + 64 * j, 64)]
        remote(blocks, blocks, sent.at[5], zr1.at[j], {Z: ring(z, 1)}).wait_recv()
        for h in range(2):
            if j == 0:
                units[h] = [received(h, kind) / LEVELS for kind in (1, 2)]
            owned = gown[3, 64 * j:64 * (j + 1), 512 * h:512 * (h + 1)] + grecv[3, 64 * j:64 * (j + 1), 512 * h:512 * (h + 1)]
            g = owned + value_of(h, 1, j, units[h][0]) + value_of(h, 2, j, units[h][1])
            for c in range(4):
                piece = g[:, c * 128:(c + 1) * 128]
                gv[pl.ds(64 * j * 8 + 4 * h + c, 64, stride=8), :] = piece
                squares = squares + jnp.sum((piece * piece).reshape(8, 8, 128), axis=0)

    line = lax.broadcasted_iota(jnp.int32, (8, 128), 0)
    n1[me] = jnp.where(line == 0, jnp.sum(squares, axis=0, keepdims=True), jnp.where(line == 1, loss, 0.0))
    near = [remote(n1.at[me], n1.at[me], sent.at[6], nr.at[0], p) for p in dp_peers]
    for c in near:
        c.start()
    seven, fifteen = n1.at[pl.ds(0, 7)], n2.at[pl.ds(0, 15)]
    remote(seven, seven, sent.at[6], nr.at[0], dp_peers[0]).wait_recv()
    sums = n1[0]
    for i in range(1, 8):
        sums = sums + n1[i]
    n2[plane] = sums
    far = [remote(n2.at[plane], n2.at[plane], sent.at[7], nr.at[1], p) for p in mp_peers]
    for c in far:
        c.start()
    remote(fifteen, fifteen, sent.at[7], nr.at[1], mp_peers[0]).wait_recv()
    sums = n2[0]
    for i in range(1, 16):
        sums = sums + n2[i]
    sums_out[...] = sums
    squared = jnp.sum(sums[0:1], axis=1, keepdims=True)
    clip = jnp.minimum(1.0, MAX_NORM / (jnp.sqrt(squared) + 1e-06))

    def place(device, q):
        return pl.ds(mul_of(device * 2048 + q * 256, 256), 256)

    def block(device, q):
        return wk.at[place(device, q)]

    spread_dp = {}
    for q in range(8):
        s = 1 if q % 2 == 0 else -1
        src = {0: (me, {Z: ring(z, 1)}), 1: (me, {Z: ring(z, -1)}),
               2: (ring(z, -s) * 2 + core, {Z: ring(z, s)}),
               3: (me, {CORE: other}), 4: (ring(z, -1) * 2 + core, {CORE: other}),
               5: (ring(z, 1) * 2 + core, {CORE: other}), 6: (ring(z, 2) * 2 + core, {CORE: other})}
        for kind, (device, to) in src.items():
            b = block(device, q)
            spread_dp[q, kind] = remote(b, b, sent.at[8], wr.at[q, kind] if kind < 3 else wd.at[0], to)
    for c in state:
        c.wait()
    for q in range(8):
        rows = pl.ds(256 * q, 256)
        g = gv[rows, :] * clip
        new, m, v = updated(g, master[rows, :], moment[rows, :], second[rows, :])
        mo[rows, :] = new
        vo[rows, :] = m
        so[rows, :] = v
        wk[place(me, q), :] = new.astype(BF)
        for kind in (0, 1, 3):
            spread_dp[q, kind].start()
    for q in range(8):
        with_relay, against = (0, 1) if q % 2 == 0 else (1, 0)
        spread_dp[q, with_relay].wait_recv()
        spread_dp[q, 2].start()
        spread_dp[q, 4 + with_relay].start()
        spread_dp[q, against].wait_recv()
        spread_dp[q, 4 + against].start()
    for q in range(8):
        spread_dp[q, 2].wait_recv()
        spread_dp[q, 6].start()
    four, all_but_one = wk.at[pl.ds(0, 4 * 2048)], wk.at[pl.ds(0, 7 * 2048)]
    remote(four, four, sent.at[8], wd.at[0], {CORE: other}).wait_recv()
    for i, (ref, device) in enumerate(((rv1, {X: ring(x, 1)}), (rv2, {X: ring(x, 1)}), (rv2, {X: ring(x, 1)}),
                                       (rv1, {X: ring(x, 1)}), (gsend, {CORE: other}), (qs, {Z: ring(z, 1)}),
                                       (seven, dp_peers[0]), (fifteen, mp_peers[0]), (all_but_one, {CORE: other}))):
        remote(ref, ref, sent.at[i], nr.at[0], device).wait_send()


def tail_kernel(work, master, moment, second, sums, work_out, master_out, moment_out, second_out, loss, sems):
    pieces = [(work.at[pl.ds(2048 * i, 2048)], work_out.at[pl.ds(2048 * i, 2048)]) for i in range(8)]
    pieces += [(master, master_out), (moment, moment_out), (second, second_out)]
    copies = [pltpu.make_async_copy(a, b, sems.at[i]) for i, (a, b) in enumerate(pieces)]
    for c in copies:
        c.start()
    loss[...] = sums[1:2, 0:1]
    for c in copies:
        c.wait()


def updated(g, old, moment, second):
    m = 0.9 * moment + 0.1 * g
    v = 0.999 * second + 0.001 * g * g
    first_hat = m * (1.0 / (1.0 - 0.9 ** 10))
    second_hat = v * (1.0 / (1.0 - 0.999 ** 10))
    return old - 0.001 * (first_hat / (jnp.sqrt(second_hat) + 1e-08) + 0.1 * old), m, v


def rows_of(value):
    r = value.shape[0]
    return value.reshape(r, 2, 4, 128).transpose(0, 2, 1, 3).reshape(r * 8, 128)


def from_rows(value):
    r = value.shape[0] // 8
    return value.reshape(r, 4, 2, 128).transpose(0, 2, 1, 3).reshape(r, 2, 512)


def per_device(features, rewards, old_values, dones, lengths, proj_weights, down_weight, value_head,
               master, moment, second):
    dma = pltpu.SemaphoreType.DMA
    vm = pl.BlockSpec(memory_space=pltpu.VMEM)
    sm = pl.BlockSpec(memory_space=pltpu.SMEM)
    hbm = pl.BlockSpec(memory_space=pl.ANY)
    state = (rows_of(master), rows_of(moment), rows_of(second))
    rows = jax.ShapeDtypeStruct((8 * ROWS, 128), F32)
    row_scratch = pltpu.VMEM((8 * ROWS, 128), F32)
    block_scratch = pltpu.VMEM((4, ROWS, 1024), F32)
    link_scratch = pltpu.VMEM((2, 3, 16 + ROWS, 512), jnp.int16)
    results = pl.pallas_call(
        step_kernel,
        name="critic_step",
        out_shape=(pltpu.VMEM((8 * D, 128), BF), row_scratch, row_scratch, row_scratch,
                   pltpu.VMEM((8, 128), F32)),
        in_specs=[hbm] * 11,
        out_specs=(vm, vm, vm, vm, vm),
        scratch_shapes=[
            pltpu.VMEM((TOK, D), BF), pltpu.VMEM((4, D, 256), BF), pltpu.VMEM((FFL, D), BF),
            pltpu.VMEM((4, TOK, 256), F32), pltpu.VMEM((256, FFL), BF), pltpu.VMEM((4, TOK, 512), BF),
            pltpu.VMEM((2, 4, 3, 4, WT, 512), BF), pltpu.VMEM((2, 4, 3, WT, 512), BF), pltpu.VMEM((4, TOK, 512), BF),
            pltpu.VMEM((2, WT, D), F32), pltpu.VMEM((TOK, 2 * FFL), BF),
            row_scratch, row_scratch, row_scratch, block_scratch, block_scratch, block_scratch,
            link_scratch, link_scratch, row_scratch,
            pltpu.VMEM((8, 8, 128), F32), pltpu.VMEM((16, 8, 128), F32),
            pltpu.VMEM((1, D), F32), pltpu.VMEM((4, 256), F32), pltpu.VMEM((4, 256), F32),
            pltpu.VMEM((4, 256), jnp.int32), pltpu.SMEM((4,), jnp.int32),
            dma((13,)), dma((2, 4)), dma((9,)),
            dma((2, 4)), dma((2, 2)), dma((2, 4, 2)), dma((2, 2, 2)),
            dma((2, 3, 2)), dma((2, 4, 2)), dma((2, 4)), dma((2, 3)),
            dma((4, 2)), dma((2, 4)), dma((4,)), dma((2,)), dma((8, 3)), dma((1,)),
        ],
        compiler_params=pltpu.CompilerParams(collective_id=0, has_side_effects=True, vmem_limit_bytes=VMEM_LIMIT),
    )(features, rows_of(proj_weights), down_weight, *state, value_head.reshape(1, D), rewards, old_values, dones, lengths)
    work, master_new, moment_new, second_new, loss = pl.pallas_call(
        tail_kernel,
        name="results",
        out_shape=(jax.ShapeDtypeStruct((8 * D, 128), BF), rows, rows, rows, jax.ShapeDtypeStruct((1, 1), F32)),
        in_specs=[vm] * 5,
        out_specs=(hbm, hbm, hbm, hbm, vm),
        scratch_shapes=[dma((11,))],
        compiler_params=pltpu.CompilerParams(vmem_limit_bytes=4 * 1024 * 1024),
    )(*(pltpu.with_memory_space_constraint(r, pltpu.VMEM) for r in results))
    return (from_rows(master_new), from_rows(moment_new), from_rows(second_new), from_rows(work), loss.reshape(()))


def solution(mesh):
    finer = Mesh(mesh.devices.reshape(4, 2, 4, 4), (Z, CORE, X, Y))
    return jax.shard_map(
        per_device,
        mesh=finer,
        in_specs=(
            P(DP, None), P(DP, None), P(DP, None), P(DP, None), P(DP),
            P(None, None, MP), P(MP, None), P(),
            P(DP, None, MP), P(DP, None, MP), P(DP, None, MP),
        ),
        out_specs=(P(DP, None, MP), P(DP, None, MP), P(DP, None, MP), P(None, None, MP), P()),
        check_vma=False,
    )
```

```python
import math

import jax
import jax.numpy as jnp
from jax import lax
from jax.experimental import pallas as pl
from jax.experimental.pallas import tpu as pltpu
from jax.sharding import Mesh
from jax.sharding import PartitionSpec as P

Z, CORE, X, Y = "dp_0", "dp_1", "mp_0", "mp_1"
DP = (Z, CORE)
MP = (X, Y)
GAMMA = 0.99
LAMBDA = 0.95
MAX_NORM = 0.05
D = 2048
TOK = 1024
FFL = 512
ROWS = 256
BF = jnp.bfloat16
LEVELS = 32000.0
F32 = jnp.float32
VMEM_LIMIT = 54 * 1024 * 1024


def mul_of(v, n):
    return pl.multiple_of(v, n)


def ring(v, d):
    return lax.rem(v + (d + 4), 4)


def remote(src, dst, send, recv, device):
    return pltpu.make_async_remote_copy(
        src_ref=src, dst_ref=dst, send_sem=send, recv_sem=recv,
        device_id=device, device_id_type=pl.DeviceIdType.MESH,
    )


def greet(devices):
    barrier = pltpu.get_barrier_semaphore()
    for device in devices:
        pl.semaphore_signal(barrier, inc=1, device_id=device, device_id_type=pl.DeviceIdType.MESH)


def greeted(devices):
    pl.semaphore_wait(pltpu.get_barrier_semaphore(), len(devices))


def own_targets(row, start, rew, old, dones, lengths):
    dn = jnp.broadcast_to(dones[pl.ds(row, 1), :].astype(F32), (8, 256))
    ov = jnp.broadcast_to(old[pl.ds(row, 1), :], (8, 256))
    rw = jnp.broadcast_to(rew[pl.ds(row, 1), :], (8, 256))
    lane = lax.broadcasted_iota(jnp.int32, (8, 256), 1)
    following = jnp.where(lane == 255, 0.0, pltpu.roll(ov, 255, axis=1))
    deltas = (rw + GAMMA * following * (1.0 - dn) - ov)[0:1]
    before = lax.broadcasted_iota(jnp.int32, (256, 256), 0) < lax.broadcasted_iota(jnp.int32, (256, 256), 1)
    counted_s = jnp.dot(dn.astype(BF), before.astype(F32).astype(BF), preferred_element_type=F32)[0:1]
    t = start + lax.broadcasted_iota(jnp.int32, (WT, 256), 0)
    s = lax.broadcasted_iota(jnp.int32, (WT, 256), 1)
    counted_t = jnp.sum(jnp.where(s < t, dn[0:1], 0.0), axis=1, keepdims=True)
    linked = (counted_t == counted_s) & (s >= t)
    powers = jnp.exp(jnp.maximum(s - t, 0).astype(F32) * math.log(GAMMA * LAMBDA))
    advantage = jnp.sum(jnp.where(linked, powers, 0.0) * deltas, axis=1, keepdims=True)
    own_old = jnp.sum(jnp.where(s == t, ov[0:1], 0.0), axis=1, keepdims=True)
    mask = jnp.where(t[:, 0:1] < lengths[row], 1.0, 0.0)
    return advantage + own_old, mask


STREAMS = ((True, 1), (True, -1), (False, 1), (False, -1))
WT = 32
WAVE = 512
ORDER = (
     ("C", 1), ("S", 1, 2, 1), ("S", 1, 1, 0), ("S", 0, 1, 1),
    ("S", 1, 2, 0), ("S", 0, 1, 0), ("C", -1), ("S", 0, -1, 1), ("S", 0, -1, 0), ("C", 0), ("PX", 0, 2),
    ("S", 0, 0, 0), ("PX", 1, 1), ("PY", 0, 2), ("PY", 0, 3), ("PX", 1, 2), ("PX", 0, 1), ("PY", 1, 2),
    ("PY", 1, 3), ("PX", 0, -1), ("S", 1, -1, 0), ("FN", 0, 0, 0), ("PX", 0, 0), ("FN", 0, 0, 1),
    ("S", 1, 1, 1), ("S", 1, -1, 1), ("S", 1, 0, 0), ("FN", 0, 2, 1), ("FN", 1, 0, 0), ("FN", 0, 2, 0),
    ("PX", 1, -1), ("FN", 0, 1, 0), ("FN", 0, 1, 1), ("FN", 1, 0, 1), ("PX", 1, 0), ("FN", 1, 2, 1),
    ("FN", 1, 2, 0), ("FN", 1, 1, 0), ("FN", 0, 3, 1), ("FN", 1, 1, 1), ("FN", 0, 3, 0), ("L", 0),
    ("G0", 0, 0), ("G0", 0, 1), ("G0b", 0, 1), ("G0b", 0, 0), ("FN", 1, 3, 0), ("FN", 1, 3, 1), ("L", 1),
    ("G0b", 1, 1), ("G0b", 1, 0), ("G0", 1, 0), ("G0", 1, 1), ("G2", 0, 0), ("G1", 0, 0), ("G1", 0, 1),
    ("G2", 0, 1), ("T", 0), ("R", 0, 0, 1), ("R", 0, 0, 0), ("R", 1, 0, 1), ("R", 1, 0, 0), ("G2", 1, 0),
    ("G2", 1, 1), ("G1", 1, 1), ("G1", 1, 0), ("G3", 0, 0), ("R", 0, 2, 0), ("R", 0, 1, 1), ("R", 0, 1, 0),
    ("R", 0, 2, 1), ("G3", 0, 1), ("B", 0, 0), ("T", 1), ("R", 1, 2, 1), ("R", 1, 2, 0), ("G3", 1, 1),
    ("R", 1, 1, 1), ("G3", 1, 0), ("B", 1, 0), ("R", 1, 1, 0), ("R", 0, 3, 0), ("R", 0, 3, 1), ("B", 0, -1),
    ("B", 0, 1), ("R", 1, 3, 1), ("R", 1, 3, 0), ("B", 1, -1), ("B", 1, 1), ("B", 0, 2), ("B", 1, 2),
)


def step_kernel(feat_hbm, w_hbm, down_hbm, master_hbm, moment_hbm, second_hbm,
                head_hbm, rew_hbm, old_hbm, dones_hbm, lengths_hbm,
                wk, mo, vo, so, sums_out,
                feat, w4, down, both, hid, part, rv1, rv2, og, mix, bg,
                master, moment, second, gsend, gown, grecv, qs, qr, gv, n1, n2,
                head, rew, old, dones, lengths,
                ins, fs, sent, rx, ry, rfr, rtwo, rg1, rga, rgb, rgc,
                dr, zr0, zr1, nr, wr, wd):
    z, core, x, y = (lax.axis_index(a) for a in (Z, CORE, X, Y))
    other = 1 - core
    me = z * 2 + core
    plane = x * 4 + y
    dp_peers = [{Z: ring(z, i // 2), CORE: lax.rem(core + i % 2, 2)} for i in range(1, 8)]
    mp_peers = [{X: ring(x, i // 4), Y: ring(y, i % 4)} for i in range(1, 16)]

    greet(dp_peers + mp_peers)
    loads = []

    def load(src, dst):
        loads.append(pltpu.make_async_copy(src, dst, ins.at[len(loads)]))
        loads[-1].start()
        return loads[-1]

    load_w = []
    for p in range(4):
        rows = pl.ds(4096 * p, 4096)
        load_w.append(load(w_hbm.at[rows], wk.at[rows]))
    load_f = {}
    for i, dy in enumerate((2, 1, -1, 0)):
        for w in range(2):
            rows = pl.ds(mul_of(ring(y, dy) * 128 + WAVE * w, 128), 128)
            load_f[w, dy] = pltpu.make_async_copy(feat_hbm.at[rows], feat.at[rows], fs.at[w, i])
    load_f[0, 2].start()
    load_f[1, 2].start()
    load_d = load(down_hbm, down)
    small, state = [], []

    out_row = lax.broadcasted_iota(jnp.int32, (256, 256), 0)
    in_row = lax.broadcasted_iota(jnp.int32, (256, 256), 1)
    select = jnp.where(in_row == (out_row % 32) * 8 + out_row // 32, 1.0, 0.0).astype(BF)
    for p in range(4):
        load_w[p].wait()
        if p == 2:
            for dy in (1, -1, 0):
                load_f[0, dy].start()
                load_f[1, dy].start()
        for u in range(8):
            base = 4096 * p + 512 * u
            pair = jnp.concatenate([wk[base:base + 256, :], wk[base + 256:base + 512, :]], axis=1)
            moved = jnp.dot(select, pair, preferred_element_type=F32).astype(BF)
            k = 512 * p + 64 * u
            for i in range(8):
                c, g = i // 2, i % 2
                for half in range(2):
                    w4[c, k + 32 * half:k + 32 * half + 32, 128 * g:128 * (g + 1)] = \
                        moved[32 * i:32 * (i + 1), 128 * half:128 * (half + 1)]
    load_d.wait()

    def peer(first, h, delta):
        along_x = STREAMS[h][0] == first
        return {X: ring(x, delta)} if along_x else {Y: ring(y, delta)}

    def tok(w, h, da, db):
        dx, dy = (da, db) if STREAMS[h][0] else (db, da)
        return pl.ds(mul_of(WAVE * w + ring(y, dy) * 128 + ring(x, dx) * WT, WT), WT)

    def offsets(h):
        s = STREAMS[h][1]
        return (2, s, -s, 0)

    def index(h, db):
        return offsets(h).index(db)

    one, two, g1, g2 = {}, {}, {}, {}
    row_at = {2: 0, 1: 1, -1: 2, 0: 3}
    for w in range(2):
        for h in range(4):
            s = STREAMS[h][1]
            for j, db in enumerate(offsets(h)):
                relayed = rx.at[w, row_at[db]] if h < 2 else ry.at[w, h - 2]
                for kind, (da, to) in enumerate(((2, s), (s, s), (-s, -s))):
                    one[w, h, kind, j] = remote(part.at[h, tok(w, h, da, db)], rv1.at[w, h, kind, j],
                                                sent.at[0], relayed if kind == 0 else rfr.at[w, j, h // 2],
                                                peer(True, h, to))
            for kind, (db, to) in enumerate(((2, s), (s, s), (-s, -s))):
                two[w, h, kind] = remote(part.at[h, tok(w, h, 0, db)], rv2.at[w, h, kind],
                                         sent.at[1], rtwo.at[w, min(kind, 1), h // 2], peer(False, h, to))
            ahead = 0 if s == 1 else 1
            for kind, (db, to) in enumerate(((0, 1), (0, -1), (-s, s))):
                t = og.at[h, tok(w, h, 0, db)]
                g1[w, h, kind] = remote(t, t, sent.at[2], rg1.at[w, {ahead: 0, 1 - ahead: 1, 2: 2}[kind], h // 2],
                                        peer(False, h, to))
            for k, db in enumerate((0, -s, s, 2)):
                for kind, (da, to) in enumerate(((0, 1), (0, -1), (-s, s))):
                    t = og.at[h, tok(w, h, da, db)]
                    if kind == ahead:
                        done = rga.at[w, k, h // 2]
                    elif h < 2:
                        done = rgb.at[w, row_at[db]]
                    else:
                        done = rgc.at[w, 2 if kind == 2 else 3 - h]
                    g2[w, h, k, kind] = remote(t, t, sent.at[3], done, peer(True, h, to))

    def arrive(count, sem):
        blocks = rv1.at[0, 0, 0, pl.ds(0, count)] if count <= 4 else rv1.at[0, pl.ds(0, count // 4), 0]
        remote(blocks, blocks, sent.at[0], sem, {X: ring(x, 1)}).wait_recv()

    def chunk(dy, waves=(0, 1), ready=None):
        rows, n = [], 128 * len(waves)
        for w in waves:
            load_f[w, dy].wait()
            rows.append(pl.ds(mul_of(ring(y, dy) * 128 + WAVE * w, 128), 128))
        f = jnp.concatenate([feat[r, :] for r in rows], axis=0)
        for c in range(4):
            gu = jnp.dot(f, w4[c], preferred_element_type=F32)
            gate, up = gu[:, :128], gu[:, 128:]
            value = (gate * jax.nn.sigmoid(gate) * up).astype(BF)
            hid[0:n, c * 128:(c + 1) * 128] = value
            for i, r in enumerate(rows):
                both[c, r, :] = gu[128 * i:128 * (i + 1)]
        v = hid[0:n, :]
        for h in (2, 3, 0, 1):
            product = jnp.dot(v, down[:, h * 512:(h + 1) * 512], preferred_element_type=F32).astype(BF)
            for i, r in enumerate(rows):
                part[h, r, :] = product[128 * i:128 * (i + 1)]
            if ready is not None and h % 2 == 1:
                ready(h)

    def send(w, dy, q):
        if q == 0:
            for kind in (0, 2):
                for h in (0, 1):
                    one[w, h, kind, index(h, dy)].start()
            return
        for j in range(4):
            for h in (2, 3):
                if dy == 2:
                    one[w, h, 0, j].start()
                elif dy == -STREAMS[h][1]:
                    one[w, h, 2, j].start()

    def pass_on(w, h, j):
        t = tok(w, h, STREAMS[h][1], offsets(h)[j])
        part[h, t, :] = (part[h, t, :].astype(F32) + rv1[w, h, 0, j].astype(F32)).astype(BF)
        one[w, h, 1, j].start()

    def pass_x(w, dy):
        arrive(2, rx.at[w, row_at[dy]])
        for h in (0, 1):
            pass_on(w, h, index(h, dy))

    def pass_y(w, h):
        arrive(4, ry.at[w, h - 2])
        for j in range(4):
            pass_on(w, h, j)

    def finish_one(w, h, j):
        t = tok(w, h, 0, offsets(h)[j])
        total = part[h, t, :].astype(F32) + rv1[w, h, 1, j].astype(F32) + rv1[w, h, 2, j].astype(F32)
        if j == 3:
            mix[w, :, h * 512:(h + 1) * 512] = total + rv2[w, h, 1].astype(F32) + rv2[w, h, 2].astype(F32)
            return
        if j == 1:
            total = total + rv2[w, h, 0].astype(F32)
        part[h, t, :] = total.astype(BF)
        two[w, h, j].start()

    def finish(w, j, q):
        arrive(4, rfr.at[w, j, q])
        if j == 1:
            arrive(2, rtwo.at[w, 0, q])
        if j == 3:
            arrive(4, rtwo.at[w, 1, q])
        for h in (2 * q, 2 * q + 1):
            finish_one(w, h, j)

    def own_loss(w, targets, mask):
        mine = pl.ds(mul_of(WAVE * w + y * 128 + x * WT, WT), WT)
        stream = feat[mine, :].astype(F32) + mix[w]
        vh = head[...]
        norm = lax.rsqrt(jnp.sum(stream * stream, axis=1, keepdims=True) / D + 1e-05)
        estimate = norm * jnp.sum(stream * vh, axis=1, keepdims=True)
        errors = estimate - targets
        total_tokens = TOK * 8
        coeff = 2.0 * mask * errors / total_tokens
        inner = coeff * estimate / D
        a = norm * coeff
        b = norm * norm * inner
        for h in range(4):
            cols = slice(h * 512, (h + 1) * 512)
            og[h, mine, :] = (a * vh[:, cols] - b * stream[:, cols]).astype(BF)
        return jnp.sum(mask * errors * errors, axis=0, keepdims=True) / total_tokens

    def spread(w, k, q):
        for kind in (0, 1):
            for h in (2 * q, 2 * q + 1):
                g2[w, h, k, kind].start()

    def relay(w, k, q):
        arrive(2, rga.at[w, k, q])
        for h in (2 * q, 2 * q + 1):
            g2[w, h, k, 2].start()

    def gather_0(w, q):
        for kind in (0, 1):
            for h in (2 * q, 2 * q + 1):
                g1[w, h, kind].start()

    def gather_1(w, q):
        arrive(2, rg1.at[w, 0, q])
        for h in (2 * q, 2 * q + 1):
            g1[w, h, 2].start()
        spread(w, 1, q)

    def gather_2(w, q):
        arrive(2, rg1.at[w, 1, q])
        spread(w, 2, q)

    def gather_3(w, q):
        arrive(2, rg1.at[w, 2, q])
        spread(w, 3, q)

    def backward(w, dy):
        arrive(4, rgb.at[w, row_at[dy]])
        if dy != 0:
            arrive({-1: 4, 1: 4, 2: 8}[dy], rgc.at[w, {-1: 0, 1: 1, 2: 2}[dy]])
        rows = pl.ds(mul_of(ring(y, dy) * 128 + WAVE * w, 128), 128)
        hg = None
        for h in range(4):
            term = lax.dot_general(og[h, rows, :], down[:, h * 512:(h + 1) * 512],
                                   (((1,), (1,)), ((), ())), preferred_element_type=F32)
            hg = term if hg is None else hg + term
        for c in range(4):
            gate, up = both[c, rows, :128], both[c, rows, 128:]
            d = hg[:, c * 128:(c + 1) * 128]
            sig = jax.nn.sigmoid(gate)
            bg[rows, c * 256:c * 256 + 128] = (d * up * sig * (1.0 + gate * (1.0 - sig))).astype(BF)
            bg[rows, c * 256 + 128:(c + 1) * 256] = (d * gate * sig).astype(BF)

    own, losses = [], []

    def first_columns(c):
        cols = pl.ds(mul_of((ring(z, 2) * 2 + (other if c == 0 else core)) * ROWS, ROWS), ROWS)
        for m in range(4):
            w4[c, 256 * m:256 * (m + 1), :] = feat[256 * m:256 * (m + 1), cols].T

    def loss_of(w):
        losses.append(own_loss(w, *own[w]))

    steps = {"C": chunk, "S": send, "PX": pass_x, "PY": pass_y, "FN": finish, "L": loss_of, "G0": gather_0,
             "G0b": lambda w, q: spread(w, 0, q), "G1": gather_1, "G2": gather_2, "G3": gather_3, "R": relay, "B": backward,
             "T": first_columns}

    def first_sends(h):
        if h == 3:
            greeted(dp_peers + mp_peers)
        send(0, 2, h // 2)

    chunk(2, (0,), first_sends)
    chunk(2, (1,))
    for at, (name, *args) in enumerate(ORDER):
        if name == "FN" and not own:
            for c in small:
                c.wait()
            own.extend(own_targets(2 * w + y // 2, (y % 2) * 128 + x * WT, rew, old, dones, lengths) for w in range(2))
        steps[name](*args)
        if at == 0:
            small.extend(load(a, b) for a, b in ((head_hbm, head), (rew_hbm, rew), (old_hbm, old), (dones_hbm, dones),
                                                 (lengths_hbm, lengths)))
            state.extend(load(a, b) for a, b in ((master_hbm, master), (moment_hbm, moment), (second_hbm, second)))
    loss = losses[0] + losses[1]

    order = (2, 1, -1, 0)
    halves = (slice(0, 512), slice(512, 1024))
    swap = [[remote(gsend.at[i, :, half], grecv.at[i, :, half], sent.at[4], dr.at[i, h], {CORE: other})
             for h, half in enumerate(halves)] for i in range(4)]

    def grad_rows(dz, c, half):
        cols = pl.ds(mul_of((ring(z, dz) * 2 + c) * ROWS, ROWS), ROWS)
        return lax.dot_general(feat[:, cols], bg[:, half], (((0,), (0,)), ((), ())), preferred_element_type=F32)

    hop = {}
    for h, s in enumerate((1, -1)):
        for kind, to in enumerate((s, s, -s)):
            for j in range(4):
                rows = pl.ds(0, 80) if j == 0 else pl.ds(16 + 64 * j, 64)
                hop[h, kind, j] = remote(qs.at[h, kind, rows], qr.at[h, kind, rows],
                                         sent.at[5], zr0.at[h, j] if kind == 0 else zr1.at[j], {Z: ring(z, to)})

    def exponent_of(bound):
        return jnp.ceil(4.0 * jnp.log2(jnp.maximum(bound, 1e-30)) + 0.02)

    def power(exponent):
        return jnp.exp(exponent * (math.log(2.0) / 4.0))

    def received(h, kind):
        exponent = qr[h, kind, 0:16, :].astype(jnp.int32).astype(F32)[0:1]
        return power(exponent)

    def head_of(h, kind, bound):
        exponent = exponent_of(bound)
        qs[h, kind, 0:16, :] = jnp.broadcast_to(exponent, (16, 512)).astype(jnp.int32).astype(jnp.int16)
        return LEVELS * power(-exponent)

    def both_cores(i, h):
        cols = slice(512 * h, 512 * (h + 1))
        size = jnp.zeros((8, 512), F32)
        for j in range(4):
            rows = slice(64 * j, 64 * (j + 1))
            t = gown[i, rows, cols] + grecv[i, rows, cols]
            gown[i, rows, cols] = t
            size = jnp.maximum(size, jnp.max(jnp.abs(t).reshape(8, 8, 512), axis=0))
        return jnp.max(size, axis=0, keepdims=True)

    def mine_of(i, h, j):
        return gown[i, 64 * j:64 * (j + 1), 512 * h:512 * (h + 1)]

    def code(value, scale):
        return jnp.round(value * scale).astype(jnp.int32).astype(jnp.int16)

    def value_of(h, kind, j, unit):
        return qr[h, kind, 16 + 64 * j:80 + 64 * j, :].astype(jnp.int32).astype(F32) * unit

    def straight(i, h, kind):
        scale = head_of(h, kind, both_cores(i, h))
        for j in range(4):
            qs[h, kind, 16 + 64 * j:80 + 64 * j, :] = code(mine_of(i, h, j), scale)
            hop[h, kind, j].start()

    def pass_sum(i, h):
        size = both_cores(i, h)
        hop[h, 0, 0].wait_recv()
        far_size = received(h, 0)
        scale = head_of(h, 1, size + far_size)
        for j in range(4):
            if j > 0:
                hop[h, 0, j].wait_recv()
            qs[h, 1, 16 + 64 * j:80 + 64 * j, :] = code(mine_of(i, h, j) + value_of(h, 0, j, far_size / LEVELS), scale)
            hop[h, 1, j].start()

    def first_rows(c, cols):
        total = None
        for m in range(4):
            term = jnp.dot(w4[c, 256 * m:256 * (m + 1), :], bg[256 * m:256 * (m + 1), cols], preferred_element_type=F32)
            total = term if total is None else total + term
        return total

    for q in range(4):
        quarter = slice(256 * q, 256 * (q + 1))
        gsend[0, :, quarter] = first_rows(0, quarter)
        remote(gsend.at[0, :, quarter], grecv.at[0, :, quarter], sent.at[4], dr.at[0, q // 2], {CORE: other}).start()
    for half in halves:
        gown[0, :, half] = first_rows(1, half)
    for i, dz in enumerate(order):
        if i == 0:
            continue
        for h, half in enumerate(halves):
            gsend[i, :, half] = grad_rows(dz, other, half)
            swap[i][h].start()
        if i == 1:
            for h in (0, 1):
                swap[0][h].wait_recv()
                straight(0, h, 0)
        if i == 2:
            swap[1][1].wait_recv()
            straight(1, 1, 2)
        if i == 3:
            swap[2][0].wait_recv()
            straight(2, 0, 2)
        for half in halves:
            gown[i, :, half] = grad_rows(dz, core, half)
    swap[1][0].wait_recv()
    pass_sum(1, 0)
    swap[2][1].wait_recv()
    pass_sum(2, 1)
    for h in (0, 1):
        swap[3][h].wait_recv()
    squares = jnp.zeros((8, 128), F32)
    units = {}
    for j in range(4):
        blocks = qr.at[:, pl.ds(1, 2), pl.ds(0, 80) if j == 0 else pl.ds(16 + 64 * j, 64)]
        remote(blocks, blocks, sent.at[5], zr1.at[j], {Z: ring(z, 1)}).wait_recv()
        for h in range(2):
            if j == 0:
                units[h] = [received(h, kind) / LEVELS for kind in (1, 2)]
            owned = gown[3, 64 * j:64 * (j + 1), 512 * h:512 * (h + 1)] + grecv[3, 64 * j:64 * (j + 1), 512 * h:512 * (h + 1)]
            g = owned + value_of(h, 1, j, units[h][0]) + value_of(h, 2, j, units[h][1])
            for c in range(4):
                piece = g[:, c * 128:(c + 1) * 128]
                gv[pl.ds(64 * j * 8 + 4 * h + c, 64, stride=8), :] = piece
                squares = squares + jnp.sum((piece * piece).reshape(8, 8, 128), axis=0)

    line = lax.broadcasted_iota(jnp.int32, (8, 128), 0)
    n1[me] = jnp.where(line == 0, jnp.sum(squares, axis=0, keepdims=True), jnp.where(line == 1, loss, 0.0))
    near = [remote(n1.at[me], n1.at[me], sent.at[6], nr.at[0], p) for p in dp_peers]
    for c in near:
        c.start()
    seven, fifteen = n1.at[pl.ds(0, 7)], n2.at[pl.ds(0, 15)]
    remote(seven, seven, sent.at[6], nr.at[0], dp_peers[0]).wait_recv()
    sums = n1[0]
    for i in range(1, 8):
        sums = sums + n1[i]
    n2[plane] = sums
    far = [remote(n2.at[plane], n2.at[plane], sent.at[7], nr.at[1], p) for p in mp_peers]
    for c in far:
        c.start()
    remote(fifteen, fifteen, sent.at[7], nr.at[1], mp_peers[0]).wait_recv()
    sums = n2[0]
    for i in range(1, 16):
        sums = sums + n2[i]
    sums_out[...] = sums
    squared = jnp.sum(sums[0:1], axis=1, keepdims=True)
    clip = jnp.minimum(1.0, MAX_NORM / (jnp.sqrt(squared) + 1e-06))

    def place(device, q):
        return pl.ds(mul_of(device * 2048 + q * 256, 256), 256)

    def block(device, q):
        return wk.at[place(device, q)]

    spread_dp = {}
    for q in range(8):
        s = 1 if q % 2 == 0 else -1
        src = {0: (me, {Z: ring(z, 1)}), 1: (me, {Z: ring(z, -1)}),
               2: (ring(z, -s) * 2 + core, {Z: ring(z, s)}),
               3: (me, {CORE: other}), 4: (ring(z, -1) * 2 + core, {CORE: other}),
               5: (ring(z, 1) * 2 + core, {CORE: other}), 6: (ring(z, 2) * 2 + core, {CORE: other})}
        for kind, (device, to) in src.items():
            b = block(device, q)
            spread_dp[q, kind] = remote(b, b, sent.at[8], wr.at[q, kind] if kind < 3 else wd.at[0], to)
    for c in state:
        c.wait()
    for q in range(8):
        rows = pl.ds(256 * q, 256)
        g = gv[rows, :] * clip
        new, m, v = updated(g, master[rows, :], moment[rows, :], second[rows, :])
        mo[rows, :] = new
        vo[rows, :] = m
        so[rows, :] = v
        wk[place(me, q), :] = new.astype(BF)
        for kind in (0, 1, 3):
            spread_dp[q, kind].start()
    for q in range(8):
        with_relay, against = (0, 1) if q % 2 == 0 else (1, 0)
        spread_dp[q, with_relay].wait_recv()
        spread_dp[q, 2].start()
        spread_dp[q, 4 + with_relay].start()
        spread_dp[q, against].wait_recv()
        spread_dp[q, 4 + against].start()
    for q in range(8):
        spread_dp[q, 2].wait_recv()
        spread_dp[q, 6].start()
    four, all_but_one = wk.at[pl.ds(0, 4 * 2048)], wk.at[pl.ds(0, 7 * 2048)]
    remote(four, four, sent.at[8], wd.at[0], {CORE: other}).wait_recv()
    for i, (ref, device) in enumerate(((rv1, {X: ring(x, 1)}), (rv2, {X: ring(x, 1)}), (rv2, {X: ring(x, 1)}),
                                       (rv1, {X: ring(x, 1)}), (gsend, {CORE: other}), (qs, {Z: ring(z, 1)}),
                                       (seven, dp_peers[0]), (fifteen, mp_peers[0]), (all_but_one, {CORE: other}))):
        remote(ref, ref, sent.at[i], nr.at[0], device).wait_send()


def tail_kernel(work, master, moment, second, sums, work_out, master_out, moment_out, second_out, loss, sems):
    pieces = [(work.at[pl.ds(2048 * i, 2048)], work_out.at[pl.ds(2048 * i, 2048)]) for i in range(8)]
    pieces += [(master, master_out), (moment, moment_out), (second, second_out)]
    copies = [pltpu.make_async_copy(a, b, sems.at[i]) for i, (a, b) in enumerate(pieces)]
    for c in copies:
        c.start()
    loss[...] = sums[1:2, 0:1]
    for c in copies:
        c.wait()


def updated(g, old, moment, second):
    m = 0.9 * moment + 0.1 * g
    v = 0.999 * second + 0.001 * g * g
    first_hat = m * (1.0 / (1.0 - 0.9 ** 10))
    second_hat = v * (1.0 / (1.0 - 0.999 ** 10))
    return old - 0.001 * (first_hat / (jnp.sqrt(second_hat) + 1e-08) + 0.1 * old), m, v


def rows_of(value):
    r = value.shape[0]
    return value.reshape(r, 2, 4, 128).transpose(0, 2, 1, 3).reshape(r * 8, 128)


def from_rows(value):
    r = value.shape[0] // 8
    return value.reshape(r, 4, 2, 128).transpose(0, 2, 1, 3).reshape(r, 2, 512)


def per_device(features, rewards, old_values, dones, lengths, proj_weights, down_weight, value_head,
               master, moment, second):
    dma = pltpu.SemaphoreType.DMA
    vm = pl.BlockSpec(memory_space=pltpu.VMEM)
    sm = pl.BlockSpec(memory_space=pltpu.SMEM)
    hbm = pl.BlockSpec(memory_space=pl.ANY)
    state = (rows_of(master), rows_of(moment), rows_of(second))
    rows = jax.ShapeDtypeStruct((8 * ROWS, 128), F32)
    row_scratch = pltpu.VMEM((8 * ROWS, 128), F32)
    block_scratch = pltpu.VMEM((4, ROWS, 1024), F32)
    link_scratch = pltpu.VMEM((2, 3, 16 + ROWS, 512), jnp.int16)
    results = pl.pallas_call(
        step_kernel,
        name="critic_step",
        out_shape=(pltpu.VMEM((8 * D, 128), BF), row_scratch, row_scratch, row_scratch,
                   pltpu.VMEM((8, 128), F32)),
        in_specs=[hbm] * 11,
        out_specs=(vm, vm, vm, vm, vm),
        scratch_shapes=[
            pltpu.VMEM((TOK, D), BF), pltpu.VMEM((4, D, 256), BF), pltpu.VMEM((FFL, D), BF),
            pltpu.VMEM((4, TOK, 256), F32), pltpu.VMEM((256, FFL), BF), pltpu.VMEM((4, TOK, 512), BF),
            pltpu.VMEM((2, 4, 3, 4, WT, 512), BF), pltpu.VMEM((2, 4, 3, WT, 512), BF), pltpu.VMEM((4, TOK, 512), BF),
            pltpu.VMEM((2, WT, D), F32), pltpu.VMEM((TOK, 2 * FFL), BF),
            row_scratch, row_scratch, row_scratch, block_scratch, block_scratch, block_scratch,
            link_scratch, link_scratch, row_scratch,
            pltpu.VMEM((8, 8, 128), F32), pltpu.VMEM((16, 8, 128), F32),
            pltpu.VMEM((1, D), F32), pltpu.VMEM((4, 256), F32), pltpu.VMEM((4, 256), F32),
            pltpu.VMEM((4, 256), jnp.int32), pltpu.SMEM((4,), jnp.int32),
            dma((13,)), dma((2, 4)), dma((9,)),
            dma((2, 4)), dma((2, 2)), dma((2, 4, 2)), dma((2, 2, 2)),
            dma((2, 3, 2)), dma((2, 4, 2)), dma((2, 4)), dma((2, 3)),
            dma((4, 2)), dma((2, 4)), dma((4,)), dma((2,)), dma((8, 3)), dma((1,)),
        ],
        compiler_params=pltpu.CompilerParams(collective_id=0, has_side_effects=True, vmem_limit_bytes=VMEM_LIMIT),
    )(features, rows_of(proj_weights), down_weight, *state, value_head.reshape(1, D), rewards, old_values, dones, lengths)
    work, master_new, moment_new, second_new, loss = pl.pallas_call(
        tail_kernel,
        name="results",
        out_shape=(jax.ShapeDtypeStruct((8 * D, 128), BF), rows, rows, rows, jax.ShapeDtypeStruct((1, 1), F32)),
        in_specs=[vm] * 5,
        out_specs=(hbm, hbm, hbm, hbm, vm),
        scratch_shapes=[dma((11,))],
        compiler_params=pltpu.CompilerParams(vmem_limit_bytes=4 * 1024 * 1024),
    )(*(pltpu.with_memory_space_constraint(r, pltpu.VMEM) for r in results))
    return (from_rows(master_new), from_rows(moment_new), from_rows(second_new), from_rows(work), loss.reshape(()))


def solution(mesh):
    finer = Mesh(mesh.devices.reshape(4, 2, 4, 4), (Z, CORE, X, Y))
    return jax.shard_map(
        per_device,
        mesh=finer,
        in_specs=(
            P(DP, None), P(DP, None), P(DP, None), P(DP, None), P(DP),
            P(None, None, MP), P(MP, None), P(),
            P(DP, None, MP), P(DP, None, MP), P(DP, None, MP),
        ),
        out_specs=(P(DP, None, MP), P(DP, None, MP), P(DP, None, MP), P(None, None, MP), P()),
        check_vma=False,
    )
```
